128 devices in a mesh: tile: 16 (over z, y), obs: 8 (over x, core).
Axes of the slice: x: 4, y: 4, z: 4, core: 2. Of those that a mesh axis runs over, the one named last changes fastest.
Arguments:
- control: float32 [128, 1024, 1024], P(None, 'tile', 'obs'), may hold values from -6 to 6
- background: bfloat16 [128, 1024, 1024], P(None, 'tile', 'obs'), may hold values from -6 to 6
- spread: float32 [1024, 1024], P('tile', 'obs'), may hold values from 0.03 to 0.24
- obs_holder: int32 [32768, 1], P(('tile', 'obs')), may hold values from 0 to 127; in each aligned block of 256 rows (0 to 255, 256 to 511, ...) at most 6 rows name the same one
- obs_anchor: int32 [32768], P(('tile', 'obs')), may hold values from 0 to 8000
- obs_frac: float32 [2, 32768], P(None, ('tile', 'obs')), may hold values from 0 to 1
- innovation: float32 [32768, 616], P(('tile', 'obs')), may hold values from -6 to 6
- inverse_var: float32 [616], replicated, may hold values from 0.5 to 2
- w_first: bfloat16 [128, 512], replicated, may hold values from -0.5 to 0.5
- b_first: float32 [512], replicated, may hold values from -3 to 3
- w_second: bfloat16 [512, 512], replicated, may hold values from -0.25 to 0.25
- b_second: float32 [512], replicated, may hold values from -3 to 3
- w_third: bfloat16 [512, 616], replicated, may hold values from -0.25 to 0.25
Outputs:
- departures: float32 [32768, 616], P(('tile', 'obs'))
- gradient: float32 [128, 1024, 1024], P(None, 'tile', 'obs')
The draws below stay inside these ranges and needn't reach their ends.
Inputs may be any that keep to these rules, and one draw needn't show every extreme that they name: `obs_holder`: among the observations of one device (aligned blocks of 256 rows) at most 6 name the same holder.
All inputs are finite; a program needn't handle non-finite values.
Results may differ from the reference program's by a relative error of at most 0.0011.
Values may be sent and summed in bfloat16 or wider, within the bound.
No kernel may reach another device: no remote copies, remote signals or barrier semaphores. Data moves between devices by JAX's collectives and lax.ppermute only.
A program may use at most 64 MiB of HBM per device.

```python
import math
import jax
import jax.numpy as jnp
import numpy as np
from jax import lax

LEV = 128
HID = 512
CH = 616
SWEEPS = 2
CX = 64
CY = 128
OBS_DEV = 256
CAP = 6
NX = 1024
NY = 1024
OBS = 32768
N_OBS = 8
DEVICES = 128


def with_ends(drawn, rng, least, top_value):
    dims = drawn.shape
    index_at = [jax.random.randint(jax.random.fold_in(rng, axis), (), 0, dims[axis]) for axis in range(len(dims))]
    drawn = drawn.at[tuple(index_at)].set(least)
    longest = dims.index(max(dims))
    index_at[longest] = (index_at[longest] + 1) % dims[longest]
    return drawn.at[tuple(index_at)].set(top_value)


def levels(key, extent, pieces, least, top_value):
    def one(dim, parts):
        draws = jax.random.uniform(jax.random.fold_in(jax.random.fold_in(key, 6), dim), (parts,), jnp.float32, least / len(pieces), top_value / len(pieces))
        return jnp.repeat(jnp.exp(draws), extent[dim] // parts).reshape((-1,) + (1,) * (len(extent) - dim - 1))

    factor_of = one(*pieces[0])
    for cut in pieces[1:]:
        factor_of = factor_of * one(*cut)
    return factor_of


def routed_block(rng, own, number, rows, number_of, top, reach, lean):
    ranking = jax.random.permutation(rng, number_of)
    heavy_load, common = shares(number_of, rows * top, reach, lean, True), shares(number_of, rows * top, reach, lean, False)
    places = jnp.arange(number_of)

    def named(sizes, turn):
        used = int((sizes > 0).sum())
        fixed = max(1, used // 4)
        passed = fixed + (places - fixed + turn * (used - fixed)) % max(1, number_of - fixed)
        return jnp.zeros((number_of,), jnp.int32).at[ranking[jnp.where(places < fixed, places, passed)]].set(jnp.asarray(sizes, jnp.int32))

    sizes = jnp.where(number % 4 == 0, named(heavy_load, number // 4), named(common, number - number // 4 - 1))
    mixed = jax.random.permutation(jax.random.fold_in(own, 3), number_of)
    source_of, taker = mixed[0:number_of // 2 * 2:2], mixed[1:number_of // 2 * 2:2]
    room = jnp.minimum(sizes[source_of] - 1, reach - sizes[taker]) // 2
    room = jnp.where((source_of == ranking[0]) | (taker == ranking[0]) | (sizes[taker] == 0), 0, jnp.maximum(room, 0))
    passed = jax.random.randint(jax.random.fold_in(own, 4), (number_of // 2,), 0, 1 << 20) % (room + 1)
    sizes = sizes.at[source_of].add(-passed).at[taker].add(passed)
    items = jnp.searchsorted(jnp.cumsum(sizes), jnp.arange(rows * top), side="right").astype(jnp.int32)
    grid = items.reshape(top, rows).T
    grid = grid[jax.random.permutation(jax.random.fold_in(own, 1), rows)]
    turn = jax.random.randint(jax.random.fold_in(own, 2), (rows, 1), 0, top)
    return jnp.take_along_axis(grid, (jnp.arange(top)[None, :] + turn) % top, axis=1)


def shares(count, total, reach, skew, full):
    loads = [(1 << 20) // math.isqrt(rank ** skew) + 1 for rank in range(1, count + 1)]
    largest = reach if full else min(reach, max(-(-total // count), total * loads[0] // sum(loads)))
    least = 1 if total - largest >= count - 1 else 0
    holding, surplus = [largest] + [least] * (count - 1), total - largest - least * (count - 1)
    while surplus > 0:
        free = [i for i in range(1, count) if holding[i] < largest] or [i for i in range(1, count) if holding[i] < reach]
        mass, left = sum([loads[i] for i in free]), surplus
        for i in free:
            more = min(reach - holding[i], max(1, left * loads[i] // mass), surplus)
            holding[i] = holding[i] + more
            surplus = surplus - more
    return np.array(holding)


def bell_draw(rng, extent, scale, reach, cuts=(), kind=jnp.bfloat16):
    loudness = levels(rng, extent, cuts, -0.22, 0.18) if cuts else 1.0
    entries = jax.random.normal(rng, extent, jnp.float32) * scale * loudness
    return jnp.minimum(jnp.maximum(entries, -reach), reach).astype(kind)


def setup_inputs(seed: int = 0) -> dict:
    keys = jax.random.split(jax.random.key(seed), 14)
    control = bell_draw(keys[0], (LEV, NX, NY), 1.0, 6.0, ((1, 16), (2, 8)), jnp.float32)
    background = bell_draw(keys[1], (LEV, NX, NY), 1.0, 6.0, ((1, 16), (2, 8)))
    spread = jnp.clip(jnp.exp(math.log(0.24) - 2.0794415 * jax.random.uniform(keys[2], (NX, NY), jnp.float32) ** levels(keys[2], (NX, NY), ((0, 16), (1, 8)), -0.2, 0.2)), 0.03, 0.24)
    obs_holder_keys = jax.random.split(jax.random.fold_in(keys[3], 1), OBS // OBS_DEV)
    obs_holder_turns = jax.random.permutation(jax.random.fold_in(keys[3], 3), OBS // OBS_DEV)
    obs_holder = jax.vmap(lambda own, number: routed_block(jax.random.fold_in(keys[3], 2), own, number, OBS_DEV, DEVICES, 1, CAP, 2))(obs_holder_keys, obs_holder_turns).reshape((OBS, 1))
    obs_anchor = with_ends(jax.random.randint(keys[4], (OBS,), 0, (CX - 1) * (CY - 1)), jax.random.fold_in(keys[4], 1), 0, ((CX - 1) * (CY - 1)) - 1).astype(jnp.int32)
    obs_frac = jnp.clip(1.0 * jax.random.uniform(keys[5], (2, OBS), jnp.float32) ** levels(keys[5], (2, OBS), ((1, 128),), -0.2, 0.2), 0.0, 1.0)
    innovation = bell_draw(keys[6], (OBS, CH), 1.0, 6.0, ((0, 128),), jnp.float32)
    inverse_var = jnp.clip(jnp.exp(jax.random.uniform(keys[7], (CH,), jnp.float32, math.log(0.5), math.log(2.0))), 0.5, 2.0)
    w_first = bell_draw(keys[8], (LEV, HID), LEV ** -0.5, 0.5)
    b_first = bell_draw(keys[9], (HID,), 1.0, 3.0, (), jnp.float32)
    w_second = bell_draw(keys[10], (HID, HID), HID ** -0.5, 0.25)
    b_second = bell_draw(keys[11], (HID,), 1.0, 3.0, (), jnp.float32)
    w_third = bell_draw(keys[12], (HID, CH), HID ** -0.5, 0.25)
    return {"control": control, "background": background, "spread": spread, "obs_holder": obs_holder, "obs_anchor": obs_anchor, "obs_frac": obs_frac, "innovation": innovation, "inverse_var": inverse_var, "w_first": w_first, "b_first": b_first, "w_second": w_second, "b_second": b_second, "w_third": w_third}


def laplace(field):
    total = jnp.roll(field, -1, 1) + jnp.roll(field, 1, 1)
    total = total + jnp.roll(field, -1, 2) + jnp.roll(field, 1, 2)
    return total - 4.0 * field


def radiances(base, delta, innov, inverse_var, w_first, b_first, w_second, b_second, w_third):
    h_one = jnp.tanh(jnp.dot(base, w_first, preferred_element_type=jnp.float32) + b_first)
    d_one = 1.0 - h_one * h_one
    h_two = jnp.tanh(jnp.dot(h_one.astype(jnp.bfloat16), w_second, preferred_element_type=jnp.float32) + b_second)
    d_two = 1.0 - h_two * h_two
    t_one = (d_one * jnp.dot(delta, w_first, preferred_element_type=jnp.float32)).astype(jnp.bfloat16)
    t_two = (d_two * jnp.dot(t_one, w_second, preferred_element_type=jnp.float32)).astype(jnp.bfloat16)
    change = jnp.dot(t_two, w_third, preferred_element_type=jnp.float32)
    departures = (change - innov) * inverse_var
    s_two = (d_two * jnp.dot(departures.astype(jnp.bfloat16), w_third.T, preferred_element_type=jnp.float32)).astype(jnp.bfloat16)
    s_one = (d_one * jnp.dot(s_two, w_second.T, preferred_element_type=jnp.float32)).astype(jnp.bfloat16)
    return departures, jnp.dot(s_one, w_first.T, preferred_element_type=jnp.float32)


def reference(control, background, spread, obs_holder, obs_anchor, obs_frac, innovation, inverse_var, w_first, b_first, w_second, b_second, w_third):
    increment = control
    for step in range(SWEEPS):
        increment = increment + spread[None] * laplace(increment)
    inc_cols = increment.astype(jnp.bfloat16).reshape(LEV, NX * NY).T
    bg_cols = background.reshape(LEV, NX * NY).T
    holder = obs_holder[:, 0].astype(jnp.int32)
    anchor = obs_anchor.astype(jnp.int32)
    ix = (holder // N_OBS) * CX + anchor // (CY - 1)
    iy = (holder % N_OBS) * CY + anchor % (CY - 1)
    corner = (ix * NY + iy).astype(jnp.int32)
    sources = [corner, corner + NY, corner + 1, corner + NY + 1]
    frac_x = obs_frac[0]
    frac_y = obs_frac[1]
    weights = [(1.0 - frac_x) * (1.0 - frac_y), frac_x * (1.0 - frac_y), (1.0 - frac_x) * frac_y, frac_x * frac_y]
    base = sum(weights[j][:, None] * bg_cols[sources[j]].astype(jnp.float32) for j in range(4)).astype(jnp.bfloat16)
    delta = sum(weights[j][:, None] * inc_cols[sources[j]].astype(jnp.float32) for j in range(4)).astype(jnp.bfloat16)
    blocks = OBS // OBS_DEV

    def one_block(items):
        return radiances(items[0], items[1], items[2], inverse_var, w_first, b_first, w_second, b_second, w_third)

    departures, profile_grad = lax.map(one_block, (base.reshape(blocks, OBS_DEV, LEV), delta.reshape(blocks, OBS_DEV, LEV), innovation.reshape(blocks, OBS_DEV, CH)))
    departures = departures.reshape(OBS, CH)
    profile_grad = profile_grad.reshape(OBS, LEV)
    gathered = jnp.zeros((NX * NY, LEV), jnp.float32)
    for j in range(4):
        gathered = gathered.at[sources[j]].add(weights[j][:, None] * profile_grad)
    adjoint = gathered.T.reshape(LEV, NX, NY)
    for step in range(SWEEPS):
        adjoint = adjoint + laplace(spread[None] * adjoint)
    return departures, control + adjoint
```

```python
import jax
import jax.numpy as jnp
from jax import lax
from jax.experimental import pallas as pl
from jax.experimental.pallas import tpu as pltpu
from jax.sharding import PartitionSpec as P

F32 = jnp.float32
BF16 = jnp.bfloat16
LEV = 128
BX = 64
BY = 128
CELLS = BX * BY
OWN = 256
DEV = 128
CAP = 6
ROWS = 8
SLOTS = CAP * DEV
HID = 512
CH = 616
PX = BX + 4
PY = BY + 16
CHUNK = 8
VMEM_LIMIT = 56 * 1024 * 1024


def params(**extra):
    return pltpu.CompilerParams(vmem_limit_bytes=VMEM_LIMIT, **extra)


def nn(a, b):
    return jnp.dot(a, b, preferred_element_type=F32)


def nt(a, b):
    return lax.dot_general(a, b, (((1,), (1,)), ((), ())), preferred_element_type=F32)


def iota(shape, dim):
    return lax.broadcasted_iota(jnp.int32, shape, dim)


def split_two(a):
    high = a.astype(BF16)
    return high, (a - high.astype(F32)).astype(BF16)


def eye_pair():
    row = iota((LEV, 2 * LEV), 0)
    col = iota((LEV, 2 * LEV), 1)
    return ((col == row) | (col == row + LEV)).astype(BF16)


def request_kernel(holder, anchor, frac, innov, ivar, w_third, out):
    held = holder[...]
    marks = (iota((DEV, OWN), 0) == held).astype(BF16)
    before = (iota((OWN, OWN), 0) < iota((OWN, OWN), 1)).astype(BF16)
    rank = jnp.sum(marks.astype(F32) * nn(marks, before), axis=0, keepdims=True).astype(jnp.int32)
    at = anchor[...].astype(F32)
    x = jnp.floor((at + 0.5) * (1.0 / (BY - 1)))
    y = at - (BY - 1) * x
    fields = [x + 1.0, y]
    for dim in range(2):
        value = frac[dim : dim + 1, :]
        for _ in range(3):
            piece = value.astype(BF16).astype(F32)
            fields.append(piece)
            value = value - piece
    fields = jnp.concatenate(fields, axis=0)
    fields = jnp.concatenate([fields] * (LEV // 8), axis=0)
    fields = jnp.where((iota((LEV, OWN), 0) >> 3) == rank, fields, 0.0).astype(BF16)
    scaled = (innov[...] * ivar[...]).astype(BF16)
    pulled = nt(scaled, w_third[...]).astype(BF16)
    row = iota((DEV * ROWS, OWN), 0)
    to_slot = (row == held * ROWS + rank).astype(BF16)
    to_fields = (row == held * ROWS + CAP).astype(BF16)
    out[:, :LEV] = (nn(to_slot, pulled[:, :LEV]) + nt(to_fields, fields)).astype(BF16)
    out[:, LEV:] = nn(to_slot, pulled[:, LEV:]).astype(BF16)


def requests(holder, anchor, frac, innov, ivar, w_third):
    return pl.pallas_call(
        request_kernel,
        out_shape=jax.ShapeDtypeStruct((DEV * ROWS, HID), BF16),
        compiler_params=params(),
        name="requests",
    )(holder, anchor, frac, innov, ivar, w_third)


def columns_kernel(control, background, spread, ct, bgt, x_up, x_down, y_up, y_down, wide, planes):
    step = pl.program_id(0)
    pair = eye_pair()
    wide[...] = background[...].astype(F32).reshape(LEV * CHUNK, BY)
    flat = control.reshape(LEV * CHUNK, BY)
    for i in range(CHUNK):
        here = pl.ds(i, LEV, stride=CHUNK)
        high, low = split_two(flat[here, :])
        back = wide[here, :].astype(BF16)
        both = jnp.concatenate(
            [
                jnp.concatenate([high, low], axis=1),
                jnp.concatenate([back, jnp.zeros_like(back)], axis=1),
            ],
            axis=0,
        )
        turned = nt(pair, both)
        ct[i] = turned[:, :LEV]
        bgt[i] = turned[:, LEV:]
        for n, y in enumerate((0, 1, BY - 2, BY - 1)):
            planes[n, pl.ds(step * CHUNK + i, 1), :] = turned[y : y + 1, :LEV]

    @pl.when(step == 0)
    def _():
        x_down[:BY, :] = ct[0].astype(BF16)
        x_down[BY : 2 * BY, :] = ct[1].astype(BF16)

    @pl.when(step == pl.num_programs(0) - 1)
    def _():
        x_up[:BY, :] = ct[CHUNK - 2].astype(BF16)
        x_up[BY : 2 * BY, :] = ct[CHUNK - 1].astype(BF16)
        s = spread[...]
        turned = jnp.transpose(jnp.concatenate([s, s], axis=0))

        def rows(two):
            high, low = split_two(two)
            zero = jnp.zeros((12, BY), F32)
            return jnp.concatenate([high.astype(F32), low.astype(F32), zero], axis=0).astype(BF16)

        x_down[2 * BY :, :] = rows(s[0:2, :])
        x_up[2 * BY :, :] = rows(s[BX - 2 : BX, :])
        y_down[: 2 * BX, :] = planes[0:2].reshape(2 * BX, LEV).astype(BF16)
        y_up[: 2 * BX, :] = planes[2:4].reshape(2 * BX, LEV).astype(BF16)
        y_down[2 * BX :, :] = rows(turned[0:2, :])
        y_up[2 * BX :, :] = rows(turned[BY - 2 : BY, :])


def to_columns(control, background, spread):
    keep = lambda i: (0, 0)
    return pl.pallas_call(
        columns_kernel,
        grid=(BX // CHUNK,),
        in_specs=[
            pl.BlockSpec((LEV, CHUNK, BY), lambda i: (0, i, 0)),
            pl.BlockSpec((LEV, CHUNK, BY), lambda i: (0, i, 0)),
            pl.BlockSpec((BX, BY), keep),
        ],
        out_specs=[
            pl.BlockSpec((CHUNK, BY, LEV), lambda i: (i, 0, 0)),
            pl.BlockSpec((CHUNK, BY, LEV), lambda i: (i, 0, 0)),
            pl.BlockSpec((2 * BY + 16, LEV), keep),
            pl.BlockSpec((2 * BY + 16, LEV), keep),
            pl.BlockSpec((2 * BX + 16, LEV), keep),
            pl.BlockSpec((2 * BX + 16, LEV), keep),
        ],
        out_shape=[
            jax.ShapeDtypeStruct((BX, BY, LEV), F32),
            jax.ShapeDtypeStruct((BX, BY, LEV), F32),
            jax.ShapeDtypeStruct((2 * BY + 16, LEV), BF16),
            jax.ShapeDtypeStruct((2 * BY + 16, LEV), BF16),
            jax.ShapeDtypeStruct((2 * BX + 16, LEV), BF16),
            jax.ShapeDtypeStruct((2 * BX + 16, LEV), BF16),
        ],
        scratch_shapes=[
            pltpu.VMEM((LEV * CHUNK, BY), F32),
            pltpu.VMEM((4, BX, LEV), F32),
        ],
        compiler_params=params(dimension_semantics=("arbitrary",)),
        name="columns",
    )(control, background, spread)


def shift(array, axis, by):
    count = lax.axis_size(axis)
    return lax.ppermute(array, axis, [(i, (i + by) % count) for i in range(count)])


def rims_around(x_up, x_down, y_up, y_down):
    y_low = shift(y_up, "obs", 1)
    y_high = shift(y_down, "obs", -1)
    x_low = shift(x_up, "tile", 1)
    x_high = shift(x_down, "tile", -1)

    def corner(row):
        low, high = BX + row, row
        return jnp.concatenate(
            [y_low[low : low + 1], y_high[high : high + 1], y_low[2 * BX :], y_high[2 * BX :]], axis=0
        )

    low = shift(corner(BX - 1), "tile", 1)
    high = shift(corner(0), "tile", -1)
    return x_low, x_high, y_low, y_high, low, high


def laplace(field, x, first, count):
    total = field[x + 1, pl.ds(first, count), :] + field[x - 1, pl.ds(first, count), :]
    total = total + field[x, pl.ds(first + 1, count), :]
    total = total + field[x, pl.ds(first - 1, count), :]
    return total - 4.0 * field[x, pl.ds(first, count), :]


def plane(field, x, y, count):
    flat = field.reshape(PX * PY, LEV)
    return flat[pl.ds(x * PY + y, count, stride=PY), :]


def set_plane(field, x, y, count, value):
    flat = field.reshape(PX * PY, LEV)
    flat[pl.ds(x * PY + y, count, stride=PY), :] = value


def plane_laplace(field, y):
    total = plane(field, 3, y, BX) + plane(field, 1, y, BX)
    total = total + plane(field, 2, y + 1, BX) + plane(field, 2, y - 1, BX)
    return total - 4.0 * plane(field, 2, y, BX)


def lanes(column):
    return jnp.broadcast_to(column, (column.shape[0], LEV))


def fill_rims(field, x_low, x_high, y_low, y_high, low, high):
    for n in range(2):
        field[n, 8 : 8 + BY, :] = x_low[n * BY : (n + 1) * BY, :].astype(F32)
        field[BX + 2 + n, 8 : 8 + BY, :] = x_high[n * BY : (n + 1) * BY, :].astype(F32)
        set_plane(field, 2, 6 + n, BX, y_low[n * BX : (n + 1) * BX, :].astype(F32))
        set_plane(field, 2, 8 + BY + n, BX, y_high[n * BX : (n + 1) * BX, :].astype(F32))
    low_rows = low[...].astype(F32)
    high_rows = high[...].astype(F32)
    field[1, 7:8, :] = low_rows[0:1]
    field[1, 8 + BY : 9 + BY, :] = low_rows[1:2]
    field[BX + 2, 7:8, :] = high_rows[0:1]
    field[BX + 2, 8 + BY : 9 + BY, :] = high_rows[1:2]


def joined(rows, at):
    block = rows[at : at + 16, :].astype(F32)
    return block[0:2] + block[2:4]


def increment_kernel(ct, spread, x_low, x_high, y_low, y_high, low, high, inc, coef, field, first):
    square = jnp.concatenate(
        [joined(x_low, 2 * BY), spread[...], joined(x_high, 2 * BY), jnp.zeros((BY - PX, BY), F32)],
        axis=0,
    )
    turned = jnp.transpose(square)

    def broadcast(x, carry):
        moved = pltpu.roll(turned, (LEV - x) % LEV, 1)
        coef[x, 8 : 8 + BY, :] = lanes(moved[:, 0:1])
        return carry

    lax.fori_loop(0, PX, broadcast, 0)
    sides = jnp.concatenate(
        [joined(y_low, 2 * BX), joined(y_high, 2 * BX), jnp.zeros((BY - 4, BY), F32)], axis=0
    )
    sides = jnp.transpose(sides)[:BX, :]
    for n in range(2):
        set_plane(coef, 2, 6 + n, BX, lanes(sides[:, n : n + 1]))
        set_plane(coef, 2, 8 + BY + n, BX, lanes(sides[:, 2 + n : 3 + n]))
    for rows, x, lane in ((low, 1, BX - 1), (high, BX + 2, 0)):
        block = rows[...].astype(F32)
        left = block[2:4] + block[4:6]
        right = block[18:20] + block[20:22]
        coef[x, 7:8, :] = lanes(left[1:2, lane : lane + 1])
        coef[x, 8 + BY : 9 + BY, :] = lanes(right[0:1, lane : lane + 1])
    field[2 : 2 + BX, 8 : 8 + BY, :] = ct[...]
    fill_rims(field, x_low, x_high, y_low, y_high, low, high)

    def sweep_one(x, carry):
        middle = field[x, 8 : 8 + BY, :]
        first[x, 8 : 8 + BY, :] = middle + coef[x, 8 : 8 + BY, :] * laplace(field, x, 8, BY)
        return carry

    lax.fori_loop(1, PX - 1, sweep_one, 0)
    for y in (7, 8 + BY):
        moved = plane(field, 2, y, BX) + plane(coef, 2, y, BX) * plane_laplace(field, y)
        set_plane(first, 2, y, BX, moved)

    def sweep_two(x, carry):
        middle = first[x, 8 : 8 + BY, :]
        result = middle + coef[x, 8 : 8 + BY, :] * laplace(first, x, 8, BY)
        inc[x - 2] = result.astype(BF16).astype(F32)
        return carry

    lax.fori_loop(2, PX - 2, sweep_two, 0)


def increments(ct, spread, rims):
    return pl.pallas_call(
        increment_kernel,
        out_shape=[
            jax.ShapeDtypeStruct((BX, BY, LEV), F32),
            jax.ShapeDtypeStruct((PX, PY, LEV), F32),
        ],
        scratch_shapes=[pltpu.VMEM((PX, PY, LEV), F32), pltpu.VMEM((PX, PY, LEV), F32)],
        compiler_params=params(),
        name="increment",
    )(ct, spread, *rims)


def decode(rows):
    back = lambda n: pltpu.roll(rows, LEV - n, 1)
    frac_x = back(2) + back(3) + back(4)
    frac_y = back(5) + back(6) + back(7)
    valid = rows > 0.5
    cell = jnp.where(valid, (rows - 1.0) * BY + back(1), 0.0).astype(jnp.int32)
    off = lambda w: jnp.where(valid, w, 0.0)
    return cell, (
        off((1.0 - frac_x) * (1.0 - frac_y)),
        off(frac_x * (1.0 - frac_y)),
        off((1.0 - frac_x) * frac_y),
        off(frac_x * frac_y),
    )


def gather_kernel(got, bgt, inct, reply, slots, wide, cells, table, ga, gb, gc, gd, spaced):
    wide[...] = got[...].astype(F32).reshape(DEV * ROWS, LEV)
    cell, weights = decode(wide[pl.ds(CAP, DEV, stride=ROWS), :])
    cells[...] = cell
    pltpu.sync_copy(cells, table)
    for k in range(CAP):

        def fetch(step, carry):
            for n in range(8):
                owner = step * 8 + n
                at = table[owner, 8 * k]
                to = pl.ds(2 * (k * DEV + owner), 2)
                ga[to, :] = bgt[pl.ds(at, 2), :]
                gb[to, :] = bgt[pl.ds(at + BY, 2), :]
                gc[to, :] = inct[pl.ds(at, 2), :]
                gd[to, :] = inct[pl.ds(at + BY, 2), :]
            return carry

        lax.fori_loop(0, DEV // 8, fetch, 0)
    spaced[...] = jnp.zeros_like(spaced)
    for k in range(CAP):
        w = [lanes(weight[:, 8 * k : 8 * k + 1]) for weight in weights]
        even = pl.ds(2 * DEV * k, DEV, stride=2)
        odd = pl.ds(2 * DEV * k + 1, DEV, stride=2)
        for n, (one, two) in enumerate(((ga, gb), (gc, gd))):
            mixed = w[0] * one[even, :] + w[1] * two[even, :]
            mixed = mixed + w[2] * one[odd, :]
            mixed = mixed + w[3] * two[odd, :]
            slots[k * DEV : (k + 1) * DEV, n * LEV : (n + 1) * LEV] = mixed.astype(BF16)
            spaced[n, pl.ds(k, DEV, stride=ROWS), :] = mixed
    reply[:, :LEV] = spaced[0].astype(BF16)
    reply[:, LEV:] = spaced[1].astype(BF16)


def gathered(got, bgt, inct):
    rows = pltpu.VMEM((2 * SLOTS, LEV), F32)
    whole = pl.BlockSpec(memory_space=pltpu.VMEM)
    return pl.pallas_call(
        gather_kernel,
        grid=(1,),
        in_specs=[pl.BlockSpec((DEV, ROWS, LEV), lambda i: (0, 0, 0)), whole, whole],
        out_specs=[whole, whole],
        out_shape=[
            jax.ShapeDtypeStruct((DEV * ROWS, 2 * LEV), BF16),
            jax.ShapeDtypeStruct((SLOTS, 2 * LEV), BF16),
        ],
        scratch_shapes=[
            pltpu.VMEM((DEV * ROWS, LEV), F32),
            pltpu.VMEM((DEV, LEV), jnp.int32),
            pltpu.SMEM((DEV, LEV), jnp.int32),
            rows,
            rows,
            rows,
            rows,
            pltpu.VMEM((2, DEV * ROWS, LEV), F32),
        ],
        compiler_params=params(),
        name="gather",
    )(got, bgt, inct)


def tangent(base, delta, w_first, b_first, w_second, b_second):
    h_one = jnp.tanh(nn(base, w_first) + b_first)
    d_one = 1.0 - h_one * h_one
    h_two = jnp.tanh(nn(h_one.astype(BF16), w_second) + b_second)
    d_two = 1.0 - h_two * h_two
    t_one = (d_one * nn(delta, w_first)).astype(BF16)
    t_two = (d_two * nn(t_one, w_second)).astype(BF16)
    return d_one, d_two, t_two


BLOCK = 256


def adjoint_kernel(
    got, slots, w_first, b_first, w_second, b_second, w_third, ivar,
    acc, x_up, x_down, y_up, y_down,
    wide, pulled, profile, cells, table, ca, cb,
):
    for n in range(HID // LEV):
        at = slice(n * LEV, (n + 1) * LEV)
        wide[...] = got[:, :, at].astype(F32).reshape(DEV * ROWS, LEV)
        for k in range(CAP):
            pulled[k * DEV : (k + 1) * DEV, at] = wide[pl.ds(k, DEV, stride=ROWS), :]
        if n == 0:
            cell, weights = decode(wide[pl.ds(CAP, DEV, stride=ROWS), :])
    cells[...] = cell
    pltpu.sync_copy(cells, table)

    def block(i, carry):
        here = pl.ds(pl.multiple_of(i * BLOCK, BLOCK), BLOCK)
        d_one, d_two, t_two = tangent(
            slots[here, :LEV], slots[here, LEV:],
            w_first[...], b_first[...], w_second[...], b_second[...],
        )
        change = nn(t_two, w_third[...]) * ivar[...]
        s_two = (d_two * (nt(change.astype(BF16), w_third[...]) - pulled[here, :])).astype(BF16)
        s_one = (d_one * nt(s_two, w_second[...])).astype(BF16)
        profile[here, :] = nt(s_one, w_first[...])
        return carry

    lax.fori_loop(0, SLOTS // BLOCK, block, 0)
    acc[...] = jnp.zeros_like(acc)
    for k in range(CAP):
        grad = profile[k * DEV : (k + 1) * DEV, :]
        w = [lanes(weight[:, 8 * k : 8 * k + 1]) for weight in weights]
        even = pl.ds(2 * DEV * k, DEV, stride=2)
        odd = pl.ds(2 * DEV * k + 1, DEV, stride=2)
        ca[even, :] = w[0] * grad
        cb[even, :] = w[1] * grad
        ca[odd, :] = w[2] * grad
        cb[odd, :] = w[3] * grad
    for k in range(CAP):

        def add(step, carry):
            for n in range(8):
                owner = step * 8 + n
                at = table[owner, 8 * k]
                there = pl.ds(2 * (k * DEV + owner), 2)
                one = acc[pl.ds(at, 2), :] + ca[there, :]
                two = acc[pl.ds(at + BY, 2), :] + cb[there, :]
                acc[pl.ds(at, 2), :] = one
                acc[pl.ds(at + BY, 2), :] = two
            return carry

        lax.fori_loop(0, DEV // 8, add, 0)
    x_down[...] = acc[: 2 * BY, :].astype(BF16)
    x_up[...] = acc[CELLS - 2 * BY :, :].astype(BF16)
    for n in range(2):
        y_down[n * BX : (n + 1) * BX, :] = acc[pl.ds(n, BX, stride=BY), :].astype(BF16)
        y_up[n * BX : (n + 1) * BX, :] = acc[pl.ds(BY - 2 + n, BX, stride=BY), :].astype(BF16)


def adjoint(got, slots, w_first, b_first, w_second, b_second, w_third, ivar):
    return pl.pallas_call(
        adjoint_kernel,
        out_shape=[
            jax.ShapeDtypeStruct((CELLS, LEV), F32),
            jax.ShapeDtypeStruct((2 * BY, LEV), BF16),
            jax.ShapeDtypeStruct((2 * BY, LEV), BF16),
            jax.ShapeDtypeStruct((2 * BX, LEV), BF16),
            jax.ShapeDtypeStruct((2 * BX, LEV), BF16),
        ],
        scratch_shapes=[
            pltpu.VMEM((DEV * ROWS, LEV), F32),
            pltpu.VMEM((SLOTS, HID), F32),
            pltpu.VMEM((SLOTS, LEV), F32),
            pltpu.VMEM((DEV, LEV), jnp.int32),
            pltpu.SMEM((DEV, LEV), jnp.int32),
            pltpu.VMEM((2 * SLOTS, LEV), F32),
            pltpu.VMEM((2 * SLOTS, LEV), F32),
        ],
        compiler_params=params(),
        name="adjoint",
    )(got, slots, w_first, b_first, w_second, b_second, w_third, ivar)


def departure_kernel(
    reply, holder, innov, w_first, b_first, w_second, b_second, w_third, ivar, out
):
    held = holder[...]
    marks = (iota((OWN, DEV), 1) == held).astype(BF16)
    before = (iota((OWN, OWN), 1) < iota((OWN, OWN), 0)).astype(BF16)
    rank = jnp.sum(marks.astype(F32) * nn(before, marks), axis=1, keepdims=True).astype(jnp.int32)
    pick = (iota((OWN, DEV * ROWS), 1) == held * ROWS + rank).astype(BF16)
    own = nn(pick, reply[...]).astype(BF16)
    _, _, t_two = tangent(
        own[:, :LEV], own[:, LEV:], w_first[...], b_first[...], w_second[...], b_second[...]
    )
    out[...] = (nn(t_two, w_third[...]) - innov[...]) * ivar[...]


def departures_of(reply, holder, innov, w_first, b_first, w_second, b_second, w_third, ivar):
    return pl.pallas_call(
        departure_kernel,
        out_shape=jax.ShapeDtypeStruct((OWN, CH), F32),
        compiler_params=params(),
        name="departures",
    )(reply, holder, innov, w_first, b_first, w_second, b_second, w_third, ivar)


def gradient_kernel(
    acc, coef, x_low, x_high, y_low, y_high, low, high, control, out, field, grown, second
):
    step = pl.program_id(0)

    @pl.when(step == 0)
    def _():
        fill_rims(field, x_low, x_high, y_low, y_high, low, high)

        def fill(x, carry):
            field[x, 8 : 8 + BY, :] = acc[pl.ds(pl.multiple_of((x - 2) * BY, BY), BY), :]
            return carry

        lax.fori_loop(2, PX - 2, fill, 0)
        grown[...] = field[...]

        def scale(x, carry):
            field[x] = field[x] * coef[x]
            return carry

        lax.fori_loop(0, PX, scale, 0)

        def sweep_one(x, carry):
            value = grown[x, 8 : 8 + BY, :] + laplace(field, x, 8, BY)
            grown[x, 8 : 8 + BY, :] = value
            second[x, 8 : 8 + BY, :] = coef[x, 8 : 8 + BY, :] * value
            return carry

        lax.fori_loop(1, PX - 1, sweep_one, 0)
        for y in (7, 8 + BY):
            value = plane(grown, 2, y, BX) + plane_laplace(field, y)
            set_plane(second, 2, y, BX, plane(coef, 2, y, BX) * value)

    pair = eye_pair()
    flat_out = out.reshape(LEV * CHUNK, BY)
    flat_control = control.reshape(LEV * CHUNK, BY)
    for i in range(CHUNK):
        x = step * CHUNK + i + 2
        value = grown[x, 8 : 8 + BY, :] + laplace(second, x, 8, BY)
        high_part, low_part = split_two(value)
        turned = nt(pair, jnp.concatenate([high_part, low_part], axis=1))
        here = pl.ds(i, LEV, stride=CHUNK)
        flat_out[here, :] = turned + flat_control[here, :]


def gradient_of(acc, coef, rims, control):
    whole = pl.BlockSpec(memory_space=pltpu.VMEM)
    block = pl.BlockSpec((LEV, CHUNK, BY), lambda i: (0, i, 0))
    return pl.pallas_call(
        gradient_kernel,
        grid=(BX // CHUNK,),
        in_specs=[whole] * 8 + [block],
        out_specs=block,
        out_shape=jax.ShapeDtypeStruct((LEV, BX, BY), F32),
        scratch_shapes=[pltpu.VMEM((PX, PY, LEV), F32)] * 3,
        compiler_params=params(dimension_semantics=("arbitrary",)),
        name="gradient",
    )(acc, coef, *rims, control)


def exchange(array):
    return lax.all_to_all(array, ("tile", "obs"), split_axis=0, concat_axis=0, tiled=True)


def per_device(
    control,
    background,
    spread,
    obs_holder,
    obs_anchor,
    obs_frac,
    innovation,
    inverse_var,
    w_first,
    b_first,
    w_second,
    b_second,
    w_third,
):
    ivar = inverse_var.reshape(1, CH)
    b_one = b_first.reshape(1, HID)
    b_two = b_second.reshape(1, HID)
    asked = requests(
        obs_holder.reshape(1, OWN), obs_anchor.reshape(1, OWN), obs_frac, innovation, ivar, w_third
    )
    got = exchange(asked.reshape(DEV, ROWS, HID))
    ct, bgt, *send = to_columns(control, background, spread)
    inct, coef = increments(ct, spread, rims_around(*send))
    reply, slots = gathered(got, bgt.reshape(CELLS, LEV), inct.reshape(CELLS, LEV))
    reply = exchange(reply.reshape(DEV, ROWS, 2 * LEV))
    acc, *send = adjoint(got, slots, w_first, b_one, w_second, b_two, w_third, ivar)
    departures = departures_of(
        reply.reshape(DEV * ROWS, 2 * LEV), obs_holder, innovation,
        w_first, b_one, w_second, b_two, w_third, ivar,
    )
    gradient = gradient_of(acc, coef, rims_around(*send), control)
    return departures, gradient


def solution(mesh):
    return jax.shard_map(
        per_device,
        mesh=mesh,
        in_specs=(
            P(None, "tile", "obs"),
            P(None, "tile", "obs"),
            P("tile", "obs"),
            P(("tile", "obs"), None),
            P(("tile", "obs")),
            P(None, ("tile", "obs")),
            P(("tile", "obs"), None),
            P(),
            P(),
            P(),
            P(),
            P(),
            P(),
        ),
        out_specs=(P(("tile", "obs"), None), P(None, "tile", "obs")),
        check_vma=False,
    )
```

```python
import jax
import jax.numpy as jnp
from jax import lax
from jax.experimental import pallas as pl
from jax.experimental.pallas import tpu as pltpu
from jax.sharding import PartitionSpec as P

F32 = jnp.float32
BF16 = jnp.bfloat16
LEV = 128
BX = 64
BY = 128
CELLS = BX * BY
OWN = 256
DEV = 128
CAP = 6
ROWS = 8
SLOTS = CAP * DEV
HID = 512
CH = 616
PX = BX + 4
PY = BY + 16
CHUNK = 8


def params(mib, **extra):
    return pltpu.CompilerParams(vmem_limit_bytes=mib * 1024 * 1024, **extra)


def cost(us):
    return pl.CostEstimate(flops=int(us * 1.0e9), bytes_accessed=0, transcendentals=0)


def tn(a, b):
    return lax.dot_general(a, b, (((0,), (0,)), ((), ())), preferred_element_type=F32)


def down(row):
    return jnp.transpose(jnp.broadcast_to(row, (LEV, row.shape[1])))


def nn(a, b):
    return jnp.dot(a, b, preferred_element_type=F32)


def nt(a, b):
    return lax.dot_general(a, b, (((1,), (1,)), ((), ())), preferred_element_type=F32)


def iota(shape, dim):
    return lax.broadcasted_iota(jnp.int32, shape, dim)


def split_two(a):
    high = a.astype(BF16)
    return high, (a - high.astype(F32)).astype(BF16)


def eye_pair():
    row = iota((LEV, 2 * LEV), 0)
    col = iota((LEV, 2 * LEV), 1)
    return ((col == row) | (col == row + LEV)).astype(BF16)


def ranks(held):
    marks = (iota((DEV, OWN), 0) == held).astype(BF16)
    before = (iota((OWN, OWN), 0) < iota((OWN, OWN), 1)).astype(BF16)
    return jnp.sum(marks.astype(F32) * nn(marks, before), axis=0, keepdims=True).astype(jnp.int32)


def request_kernel(holder, anchor, frac, innov, ivar, w_third, out):
    held = holder[...]
    rank = ranks(held)
    at = anchor[...].astype(F32)
    x = jnp.floor((at + 0.5) * (1.0 / (BY - 1)))
    y = at - (BY - 1) * x
    fields = [x + 1.0, y]
    for dim in range(2):
        value = frac[dim : dim + 1, :]
        for _ in range(3):
            piece = value.astype(BF16).astype(F32)
            fields.append(piece)
            value = value - piece
    fields = jnp.concatenate(fields, axis=0)
    fields = jnp.concatenate([fields] * (LEV // 8), axis=0)
    fields = jnp.where((iota((LEV, OWN), 0) >> 3) == rank, fields, 0.0).astype(BF16)
    each = down(ivar[...].reshape(1, CH))
    scaled = (innov[...] * jnp.concatenate([each, each], axis=1)).astype(BF16)
    pulled = tn(scaled, w_third[...]).astype(BF16)
    row = iota((DEV * ROWS, OWN), 0)
    to_slot = (row == held * ROWS + rank).astype(BF16)
    to_fields = (row == held * ROWS + CAP).astype(BF16)
    out[:, :LEV] = (nn(to_slot, pulled[:, :LEV]) + nt(to_fields, fields)).astype(BF16)
    out[:, LEV:] = nn(to_slot, pulled[:, LEV:]).astype(BF16)


def requests(holder, anchor, frac, innov, ivar, w_third):
    return pl.pallas_call(
        request_kernel,
        out_shape=jax.ShapeDtypeStruct((DEV * ROWS, HID), BF16),
        compiler_params=params(12),
        cost_estimate=cost(4),
        name="requests",
    )(holder, anchor, frac, innov, ivar, w_third)


def columns_kernel(control, background, spread, ct, bgt, x_up, x_down, y_up, y_down, wide, planes):
    step = pl.program_id(0)
    pair = eye_pair()
    wide[...] = background[...].astype(F32).reshape(LEV * CHUNK, BY)
    flat = control.reshape(LEV * CHUNK, BY)
    for i in range(CHUNK):
        here = pl.ds(i, LEV, stride=CHUNK)
        high, low = split_two(flat[here, :])
        back = wide[here, :].astype(BF16)
        both = jnp.concatenate(
            [
                jnp.concatenate([high, low], axis=1),
                jnp.concatenate([back, jnp.zeros_like(back)], axis=1),
            ],
            axis=0,
        )
        turned = nt(pair, both)
        ct[i] = turned[:, :LEV]
        bgt[i] = turned[:, LEV:]
        for n, y in enumerate((0, 1, BY - 2, BY - 1)):
            planes[n, pl.ds(step * CHUNK + i, 1), :] = turned[y : y + 1, :LEV]

    @pl.when(step == 0)
    def _():
        x_down[:BY, :] = ct[0].astype(BF16)
        x_down[BY : 2 * BY, :] = ct[1].astype(BF16)

    @pl.when(step == pl.num_programs(0) - 1)
    def _():
        x_up[:BY, :] = ct[CHUNK - 2].astype(BF16)
        x_up[BY : 2 * BY, :] = ct[CHUNK - 1].astype(BF16)
        s = spread[...]
        turned = jnp.transpose(jnp.concatenate([s, s], axis=0))

        def rows(two):
            high, low = split_two(two)
            zero = jnp.zeros((12, BY), F32)
            return jnp.concatenate([high.astype(F32), low.astype(F32), zero], axis=0).astype(BF16)

        x_down[2 * BY :, :] = rows(s[0:2, :])
        x_up[2 * BY :, :] = rows(s[BX - 2 : BX, :])
        y_down[: 2 * BX, :] = planes[0:2].reshape(2 * BX, LEV).astype(BF16)
        y_up[: 2 * BX, :] = planes[2:4].reshape(2 * BX, LEV).astype(BF16)
        y_down[2 * BX :, :] = rows(turned[0:2, :])
        y_up[2 * BX :, :] = rows(turned[BY - 2 : BY, :])


def to_columns(control, background, spread):
    keep = lambda i: (0, 0)
    return pl.pallas_call(
        columns_kernel,
        grid=(BX // CHUNK,),
        in_specs=[
            pl.BlockSpec((LEV, CHUNK, BY), lambda i: (0, i, 0)),
            pl.BlockSpec((LEV, CHUNK, BY), lambda i: (0, i, 0)),
            pl.BlockSpec((BX, BY), keep),
        ],
        out_specs=[
            pl.BlockSpec((CHUNK, BY, LEV), lambda i: (i, 0, 0)),
            pl.BlockSpec((CHUNK, BY, LEV), lambda i: (i, 0, 0)),
            pl.BlockSpec((2 * BY + 16, LEV), keep),
            pl.BlockSpec((2 * BY + 16, LEV), keep),
            pl.BlockSpec((2 * BX + 16, LEV), keep),
            pl.BlockSpec((2 * BX + 16, LEV), keep),
        ],
        out_shape=[
            jax.ShapeDtypeStruct((BX, BY, LEV), F32),
            jax.ShapeDtypeStruct((BX, BY, LEV), F32),
            jax.ShapeDtypeStruct((2 * BY + 16, LEV), BF16),
            jax.ShapeDtypeStruct((2 * BY + 16, LEV), BF16),
            jax.ShapeDtypeStruct((2 * BX + 16, LEV), BF16),
            jax.ShapeDtypeStruct((2 * BX + 16, LEV), BF16),
        ],
        scratch_shapes=[
            pltpu.VMEM((LEV * CHUNK, BY), F32),
            pltpu.VMEM((4, BX, LEV), F32),
        ],
        compiler_params=params(10, dimension_semantics=("arbitrary",)),
        cost_estimate=cost(6),
        name="columns",
    )(control, background, spread)


def shift(array, axis, by):
    count = lax.axis_size(axis)
    return lax.ppermute(array, axis, [(i, (i + by) % count) for i in range(count)])


def rims_around(x_up, x_down, y_up, y_down):
    y_low = shift(y_up, "obs", 1)
    y_high = shift(y_down, "obs", -1)
    x_low = shift(x_up, "tile", 1)
    x_high = shift(x_down, "tile", -1)

    def corner(row):
        low, high = BX + row, row
        return jnp.concatenate(
            [y_low[low : low + 1], y_high[high : high + 1], y_low[2 * BX :], y_high[2 * BX :]], axis=0
        )

    low = shift(corner(BX - 1), "tile", 1)
    high = shift(corner(0), "tile", -1)
    return x_low, x_high, y_low, y_high, low, high


def laplace(field, x, first, count):
    total = field[x + 1, pl.ds(first, count), :] + field[x - 1, pl.ds(first, count), :]
    total = total + field[x, pl.ds(first + 1, count), :]
    total = total + field[x, pl.ds(first - 1, count), :]
    return total - 4.0 * field[x, pl.ds(first, count), :]


def plane(field, x, y, count):
    flat = field.reshape(PX * PY, LEV)
    return flat[pl.ds(x * PY + y, count, stride=PY), :]


def set_plane(field, x, y, count, value):
    flat = field.reshape(PX * PY, LEV)
    flat[pl.ds(x * PY + y, count, stride=PY), :] = value


def plane_laplace(field, y):
    total = plane(field, 3, y, BX) + plane(field, 1, y, BX)
    total = total + plane(field, 2, y + 1, BX) + plane(field, 2, y - 1, BX)
    return total - 4.0 * plane(field, 2, y, BX)


def lanes(column):
    return jnp.broadcast_to(column, (column.shape[0], LEV))


def fill_rims(field, x_low, x_high, y_low, y_high, low, high):
    for n in range(2):
        field[n, 8 : 8 + BY, :] = x_low[n * BY : (n + 1) * BY, :].astype(F32)
        field[BX + 2 + n, 8 : 8 + BY, :] = x_high[n * BY : (n + 1) * BY, :].astype(F32)
        set_plane(field, 2, 6 + n, BX, y_low[n * BX : (n + 1) * BX, :].astype(F32))
        set_plane(field, 2, 8 + BY + n, BX, y_high[n * BX : (n + 1) * BX, :].astype(F32))
    low_rows = low[...].astype(F32)
    high_rows = high[...].astype(F32)
    field[1, 7:8, :] = low_rows[0:1]
    field[1, 8 + BY : 9 + BY, :] = low_rows[1:2]
    field[BX + 2, 7:8, :] = high_rows[0:1]
    field[BX + 2, 8 + BY : 9 + BY, :] = high_rows[1:2]


def joined(rows, at):
    block = rows[at : at + 16, :].astype(F32)
    return block[0:2] + block[2:4]


def increment_kernel(ct, spread, x_low, x_high, y_low, y_high, low, high, inc, coef, field, first):
    square = jnp.concatenate(
        [joined(x_low, 2 * BY), spread[...], joined(x_high, 2 * BY), jnp.zeros((BY - PX, BY), F32)],
        axis=0,
    )
    turned = jnp.transpose(square)

    for x in range(PX):
        coef[x, 8 : 8 + BY, :] = lanes(turned[:, x : x + 1])
    sides = jnp.concatenate(
        [joined(y_low, 2 * BX), joined(y_high, 2 * BX), jnp.zeros((BY - 4, BY), F32)], axis=0
    )
    sides = jnp.transpose(sides)[:BX, :]
    for n in range(2):
        set_plane(coef, 2, 6 + n, BX, lanes(sides[:, n : n + 1]))
        set_plane(coef, 2, 8 + BY + n, BX, lanes(sides[:, 2 + n : 3 + n]))
    for rows, x, lane in ((low, 1, BX - 1), (high, BX + 2, 0)):
        block = rows[...].astype(F32)
        left = block[2:4] + block[4:6]
        right = block[18:20] + block[20:22]
        coef[x, 7:8, :] = lanes(left[1:2, lane : lane + 1])
        coef[x, 8 + BY : 9 + BY, :] = lanes(right[0:1, lane : lane + 1])
    field[2 : 2 + BX, 8 : 8 + BY, :] = ct[...]
    fill_rims(field, x_low, x_high, y_low, y_high, low, high)

    def sweep_one(x, carry):
        middle = field[x, 8 : 8 + BY, :]
        first[x, 8 : 8 + BY, :] = middle + coef[x, 8 : 8 + BY, :] * laplace(field, x, 8, BY)
        return carry

    lax.fori_loop(1, PX - 1, sweep_one, 0)
    for y in (7, 8 + BY):
        moved = plane(field, 2, y, BX) + plane(coef, 2, y, BX) * plane_laplace(field, y)
        set_plane(first, 2, y, BX, moved)

    def sweep_two(x, carry):
        middle = first[x, 8 : 8 + BY, :]
        result = middle + coef[x, 8 : 8 + BY, :] * laplace(first, x, 8, BY)
        inc[x - 2] = result.astype(BF16).astype(F32)
        return carry

    lax.fori_loop(2, PX - 2, sweep_two, 0)


def increments(ct, spread, rims):
    return pl.pallas_call(
        increment_kernel,
        out_shape=[
            jax.ShapeDtypeStruct((BX, BY, LEV), F32),
            jax.ShapeDtypeStruct((PX, PY, LEV), F32),
        ],
        scratch_shapes=[pltpu.VMEM((PX, PY, LEV), F32), pltpu.VMEM((PX, PY, LEV), F32)],
        compiler_params=params(27),
        cost_estimate=cost(6),
        name="increment",
    )(ct, spread, *rims)


def decode(rows):
    back = lambda n: pltpu.roll(rows, LEV - n, 1)
    frac_x = back(2) + back(3) + back(4)
    frac_y = back(5) + back(6) + back(7)
    valid = rows > 0.5
    cell = jnp.where(valid, (rows - 1.0) * BY + back(1), 0.0).astype(jnp.int32)
    off = lambda w: jnp.where(valid, w, 0.0)
    return cell, (
        off((1.0 - frac_x) * (1.0 - frac_y)),
        off(frac_x * (1.0 - frac_y)),
        off((1.0 - frac_x) * frac_y),
        off(frac_x * frac_y),
    )


def gather_kernel(got, bgt, inct, reply, slots, wide, cells, table, ga, gb, gc, gd, spaced):
    wide[...] = got[...].astype(F32).reshape(DEV * ROWS, LEV)
    cell, weights = decode(wide[pl.ds(CAP, DEV, stride=ROWS), :])
    cells[...] = cell
    pltpu.sync_copy(cells, table)
    for k in range(CAP):

        def fetch(step, carry):
            for n in range(8):
                owner = step * 8 + n
                at = table[owner, 8 * k]
                to = pl.ds(2 * (k * DEV + owner), 2)
                ga[to, :] = bgt[pl.ds(at, 2), :]
                gb[to, :] = bgt[pl.ds(at + BY, 2), :]
                gc[to, :] = inct[pl.ds(at, 2), :]
                gd[to, :] = inct[pl.ds(at + BY, 2), :]
            return carry

        lax.fori_loop(0, DEV // 8, fetch, 0)
    spaced[...] = jnp.zeros_like(spaced)
    for k in range(CAP):
        w = [lanes(weight[:, 8 * k : 8 * k + 1]) for weight in weights]
        even = pl.ds(2 * DEV * k, DEV, stride=2)
        odd = pl.ds(2 * DEV * k + 1, DEV, stride=2)
        for n, (one, two) in enumerate(((ga, gb), (gc, gd))):
            mixed = w[0] * one[even, :] + w[1] * two[even, :]
            mixed = mixed + w[2] * one[odd, :]
            mixed = mixed + w[3] * two[odd, :]
            slots[k * DEV : (k + 1) * DEV, n * LEV : (n + 1) * LEV] = mixed.astype(BF16)
            spaced[n, pl.ds(k, DEV, stride=ROWS), :] = mixed
    reply[:, :LEV] = spaced[0].astype(BF16)
    reply[:, LEV:] = spaced[1].astype(BF16)


def gathered(got, bgt, inct):
    rows = pltpu.VMEM((2 * SLOTS, LEV), F32)
    whole = pl.BlockSpec(memory_space=pltpu.VMEM)
    return pl.pallas_call(
        gather_kernel,
        grid=(1,),
        in_specs=[pl.BlockSpec((DEV, ROWS, LEV), lambda i: (0, 0, 0)), whole, whole],
        out_specs=[whole, whole],
        out_shape=[
            jax.ShapeDtypeStruct((DEV * ROWS, 2 * LEV), BF16),
            jax.ShapeDtypeStruct((SLOTS, 2 * LEV), BF16),
        ],
        scratch_shapes=[
            pltpu.VMEM((DEV * ROWS, LEV), F32),
            pltpu.VMEM((DEV, LEV), jnp.int32),
            pltpu.SMEM((DEV, LEV), jnp.int32),
            rows,
            rows,
            rows,
            rows,
            pltpu.VMEM((2, DEV * ROWS, LEV), F32),
        ],
        compiler_params=params(18),
        cost_estimate=cost(5),
        name="gather",
    )(got, bgt, inct)


def tangent(base, delta, w_first, b_first, w_second, b_second):
    h_one = jnp.tanh(nn(base, w_first) + b_first)
    d_one = 1.0 - h_one * h_one
    h_two = jnp.tanh(nn(h_one.astype(BF16), w_second) + b_second)
    d_two = 1.0 - h_two * h_two
    t_one = (d_one * nn(delta, w_first)).astype(BF16)
    t_two = (d_two * nn(t_one, w_second)).astype(BF16)
    return d_one, d_two, t_two


BLOCK = 256


def adjoint_kernel(
    got, slots, w_first, b_first, w_second, b_second, w_third, ivar,
    acc, x_up, x_down, y_up, y_down,
    wide, pulled, profile, cells, table, ca, cb,
):
    for n in range(HID // LEV):
        at = slice(n * LEV, (n + 1) * LEV)
        wide[...] = got[:, :, at].astype(F32).reshape(DEV * ROWS, LEV)
        for k in range(CAP):
            pulled[k * DEV : (k + 1) * DEV, at] = wide[pl.ds(k, DEV, stride=ROWS), :]
        if n == 0:
            cell, weights = decode(wide[pl.ds(CAP, DEV, stride=ROWS), :])
    cells[...] = cell
    pltpu.sync_copy(cells, table)

    def block(i, carry):
        here = pl.ds(pl.multiple_of(i * BLOCK, BLOCK), BLOCK)
        d_one, d_two, t_two = tangent(
            slots[here, :LEV], slots[here, LEV:],
            w_first[...], b_first[...], w_second[...], b_second[...],
        )
        change = nt(t_two, w_third[...]) * ivar[...].reshape(1, CH)
        s_two = (d_two * (nn(change.astype(BF16), w_third[...]) - pulled[here, :])).astype(BF16)
        s_one = (d_one * nt(s_two, w_second[...])).astype(BF16)
        profile[here, :] = nt(s_one, w_first[...])
        return carry

    lax.fori_loop(0, SLOTS // BLOCK, block, 0)
    acc[...] = jnp.zeros_like(acc)
    for k in range(CAP):
        grad = profile[k * DEV : (k + 1) * DEV, :]
        w = [lanes(weight[:, 8 * k : 8 * k + 1]) for weight in weights]
        even = pl.ds(2 * DEV * k, DEV, stride=2)
        odd = pl.ds(2 * DEV * k + 1, DEV, stride=2)
        ca[even, :] = w[0] * grad
        cb[even, :] = w[1] * grad
        ca[odd, :] = w[2] * grad
        cb[odd, :] = w[3] * grad
    for k in range(CAP):

        def add(step, carry):
            for n in range(8):
                owner = step * 8 + n
                at = table[owner, 8 * k]
                there = pl.ds(2 * (k * DEV + owner), 2)
                one = acc[pl.ds(at, 2), :] + ca[there, :]
                two = acc[pl.ds(at + BY, 2), :] + cb[there, :]
                acc[pl.ds(at, 2), :] = one
                acc[pl.ds(at + BY, 2), :] = two
            return carry

        lax.fori_loop(0, DEV // 8, add, 0)
    x_down[...] = acc[: 2 * BY, :].astype(BF16)
    x_up[...] = acc[CELLS - 2 * BY :, :].astype(BF16)
    for n in range(2):
        y_down[n * BX : (n + 1) * BX, :] = acc[pl.ds(n, BX, stride=BY), :].astype(BF16)
        y_up[n * BX : (n + 1) * BX, :] = acc[pl.ds(BY - 2 + n, BX, stride=BY), :].astype(BF16)


def adjoint(got, slots, w_first, b_first, w_second, b_second, w_third, ivar):
    return pl.pallas_call(
        adjoint_kernel,
        out_shape=[
            jax.ShapeDtypeStruct((CELLS, LEV), F32),
            jax.ShapeDtypeStruct((2 * BY, LEV), BF16),
            jax.ShapeDtypeStruct((2 * BY, LEV), BF16),
            jax.ShapeDtypeStruct((2 * BX, LEV), BF16),
            jax.ShapeDtypeStruct((2 * BX, LEV), BF16),
        ],
        scratch_shapes=[
            pltpu.VMEM((DEV * ROWS, LEV), F32),
            pltpu.VMEM((SLOTS, HID), F32),
            pltpu.VMEM((SLOTS, LEV), F32),
            pltpu.VMEM((DEV, LEV), jnp.int32),
            pltpu.SMEM((DEV, LEV), jnp.int32),
            pltpu.VMEM((2 * SLOTS, LEV), F32),
            pltpu.VMEM((2 * SLOTS, LEV), F32),
        ],
        compiler_params=params(24),
        cost_estimate=cost(10),
        name="adjoint",
    )(got, slots, w_first, b_first, w_second, b_second, w_third, ivar)


def departure_kernel(
    reply, holder, innov, w_first, b_first, w_second, b_second, w_third, ivar, out
):
    held = holder[...]
    pick = (iota((OWN, DEV * ROWS), 1) == down(held * ROWS + ranks(held)).astype(jnp.int32)[:, 0:1]).astype(BF16)
    own = nn(pick, reply[...]).astype(BF16)
    _, _, t_two = tangent(
        own[:, :LEV], own[:, LEV:], w_first[...], b_first[...], w_second[...], b_second[...]
    )
    each = down(ivar[...].reshape(1, CH))
    out[...] = (nt(w_third[...], t_two) - innov[...]) * jnp.concatenate([each, each], axis=1)


def departures_of(reply, holder, innov, w_first, b_first, w_second, b_second, w_third, ivar):
    return pl.pallas_call(
        departure_kernel,
        out_shape=jax.ShapeDtypeStruct((CH, OWN), F32),
        compiler_params=params(12),
        cost_estimate=cost(4),
        name="departures",
    )(reply, holder, innov, w_first, b_first, w_second, b_second, w_third, ivar)


def gradient_kernel(
    acc, coef, x_low, x_high, y_low, y_high, low, high, control, out, field, grown, second
):
    step = pl.program_id(0)

    @pl.when(step == 0)
    def _():
        fill_rims(field, x_low, x_high, y_low, y_high, low, high)

        def fill(x, carry):
            field[x, 8 : 8 + BY, :] = acc[pl.ds(pl.multiple_of((x - 2) * BY, BY), BY), :]
            return carry

        lax.fori_loop(2, PX - 2, fill, 0)
        grown[...] = field[...]

        def scale(x, carry):
            field[x] = field[x] * coef[x]
            return carry

        lax.fori_loop(0, PX, scale, 0)

        def sweep_one(x, carry):
            value = grown[x, 8 : 8 + BY, :] + laplace(field, x, 8, BY)
            grown[x, 8 : 8 + BY, :] = value
            second[x, 8 : 8 + BY, :] = coef[x, 8 : 8 + BY, :] * value
            return carry

        lax.fori_loop(1, PX - 1, sweep_one, 0)
        for y in (7, 8 + BY):
            value = plane(grown, 2, y, BX) + plane_laplace(field, y)
            set_plane(second, 2, y, BX, plane(coef, 2, y, BX) * value)

    pair = eye_pair()
    flat_out = out.reshape(LEV * CHUNK, BY)
    flat_control = control.reshape(LEV * CHUNK, BY)
    for i in range(CHUNK):
        x = step * CHUNK + i + 2
        value = grown[x, 8 : 8 + BY, :] + laplace(second, x, 8, BY)
        high_part, low_part = split_two(value)
        turned = nt(pair, jnp.concatenate([high_part, low_part], axis=1))
        here = pl.ds(i, LEV, stride=CHUNK)
        flat_out[here, :] = turned + flat_control[here, :]


def gradient_of(acc, coef, rims, control):
    whole = pl.BlockSpec(memory_space=pltpu.VMEM)
    block = pl.BlockSpec((LEV, CHUNK, BY), lambda i: (0, i, 0))
    return pl.pallas_call(
        gradient_kernel,
        grid=(BX // CHUNK,),
        in_specs=[whole] * 8 + [block],
        out_specs=block,
        out_shape=jax.ShapeDtypeStruct((LEV, BX, BY), F32),
        scratch_shapes=[pltpu.VMEM((PX, PY, LEV), F32)] * 3,
        compiler_params=params(30, dimension_semantics=("arbitrary",)),
        cost_estimate=cost(8),
        name="gradient",
    )(acc, coef, *rims, control)


def exchange(array):
    return lax.all_to_all(array, ("tile", "obs"), split_axis=0, concat_axis=0, tiled=True)


def per_device(
    control,
    background,
    spread,
    obs_holder,
    obs_anchor,
    obs_frac,
    innovation,
    inverse_var,
    w_first,
    b_first,
    w_second,
    b_second,
    w_third,
):
    b_one = b_first.reshape(1, HID)
    b_two = b_second.reshape(1, HID)
    holder = obs_holder.reshape(1, OWN)
    innov = innovation.T
    w_last = w_third.T
    asked = requests(holder, obs_anchor.reshape(1, OWN), obs_frac, innov, inverse_var, w_last)
    got = exchange(asked.reshape(DEV, ROWS, HID))
    ct, bgt, *send = to_columns(control, background, spread)
    inct, coef = increments(ct, spread, rims_around(*send))
    reply, slots = gathered(got, bgt.reshape(CELLS, LEV), inct.reshape(CELLS, LEV))
    reply = exchange(reply.reshape(DEV, ROWS, 2 * LEV))
    acc, *send = adjoint(got, slots, w_first, b_one, w_second, b_two, w_last, inverse_var)
    departures = departures_of(
        reply.reshape(DEV * ROWS, 2 * LEV), holder, innov,
        w_first, b_one, w_second, b_two, w_last, inverse_var,
    ).T
    gradient = gradient_of(acc, coef, rims_around(*send), control)
    return departures, gradient


def solution(mesh):
    return jax.shard_map(
        per_device,
        mesh=mesh,
        in_specs=(
            P(None, "tile", "obs"),
            P(None, "tile", "obs"),
            P("tile", "obs"),
            P(("tile", "obs"), None),
            P(("tile", "obs")),
            P(None, ("tile", "obs")),
            P(("tile", "obs"), None),
            P(),
            P(),
            P(),
            P(),
            P(),
            P(),
        ),
        out_specs=(P(("tile", "obs"), None), P(None, "tile", "obs")),
        check_vma=False,
    )
```

```python
import functools

import jax
import jax.numpy as jnp
from jax import lax
from jax.experimental import pallas as pl
from jax.experimental.pallas import tpu as pltpu
from jax.sharding import PartitionSpec as P


F32 = jnp.float32
BF16 = jnp.bfloat16
LEV = 128
BX = 64
BY = 128
CELLS = BX * BY
OWN = 256
DEV = 128
CAP = 6
ROWS = 8
SLOTS = CAP * DEV
HID = 512
CH = 616
PX = BX + 4
PY = BY + 16
CHUNK = 8


def params(mib, **extra):
    return pltpu.CompilerParams(vmem_limit_bytes=mib * 1024 * 1024, **extra)


def cost(us):
    return pl.CostEstimate(flops=int(us * 1.0e9), bytes_accessed=0, transcendentals=0)


def tn(a, b):
    return lax.dot_general(a, b, (((0,), (0,)), ((), ())), preferred_element_type=F32)


def down(row):
    return jnp.transpose(jnp.broadcast_to(row, (LEV, row.shape[1])))


def in_vmem(array):
    return pltpu.with_memory_space_constraint(array, pltpu.VMEM)


def in_hbm(array):
    return pltpu.with_memory_space_constraint(array, pltpu.HBM)


def nn(a, b):
    return jnp.dot(a, b, preferred_element_type=F32)


def nt(a, b):
    return lax.dot_general(a, b, (((1,), (1,)), ((), ())), preferred_element_type=F32)


def iota(shape, dim):
    return lax.broadcasted_iota(jnp.int32, shape, dim)


def split_two(a):
    high = a.astype(BF16)
    return high, (a - high.astype(F32)).astype(BF16)


def eye_pair():
    row = iota((LEV, 2 * LEV), 0)
    col = iota((LEV, 2 * LEV), 1)
    return ((col == row) | (col == row + LEV)).astype(BF16)


def ranks(held):
    marks = (iota((DEV, OWN), 0) == held).astype(BF16)
    before = (iota((OWN, OWN), 0) < iota((OWN, OWN), 1)).astype(BF16)
    return jnp.sum(marks.astype(F32) * nn(marks, before), axis=0, keepdims=True).astype(jnp.int32)


def request_kernel(holder, anchor, frac, innov, ivar, w_third, out):
    held = holder[...]
    rank = ranks(held)
    at = anchor[...].astype(F32)
    x = jnp.floor((at + 0.5) * (1.0 / (BY - 1)))
    y = at - (BY - 1) * x
    fields = [x + 1.0, y]
    for dim in range(2):
        value = frac[dim : dim + 1, :]
        for _ in range(3):
            piece = value.astype(BF16).astype(F32)
            fields.append(piece)
            value = value - piece
    fields = jnp.concatenate(fields, axis=0)
    fields = jnp.concatenate([fields] * (LEV // 8), axis=0)
    fields = jnp.where((iota((LEV, OWN), 0) >> 3) == rank, fields, 0.0).astype(BF16)
    each = down(ivar[...].reshape(1, CH))
    scaled = (innov[...] * jnp.concatenate([each, each], axis=1)).astype(BF16)
    pulled = tn(scaled, w_third[...]).astype(BF16)
    row = iota((DEV * ROWS, OWN), 0)
    to_slot = (row == held * ROWS + rank).astype(BF16)
    to_fields = (row == held * ROWS + CAP).astype(BF16)
    out[:, :LEV] = (nn(to_slot, pulled[:, :LEV]) + nt(to_fields, fields)).astype(BF16)
    out[:, LEV:] = nn(to_slot, pulled[:, LEV:]).astype(BF16)


def requests(holder, anchor, frac, innov, ivar, w_third):
    return pl.pallas_call(
        request_kernel,
        out_shape=jax.ShapeDtypeStruct((DEV * ROWS, HID), BF16),
        compiler_params=params(12),
        cost_estimate=cost(4),
        name="requests",
    )(holder, anchor, frac, innov, ivar, w_third)


def columns_kernel(control, background, spread, ct, bgt, x_up, x_down, y_up, y_down, wide, planes):
    step = pl.program_id(0)
    pair = eye_pair()
    wide[...] = background[...].astype(F32).reshape(LEV * CHUNK, BY)
    flat = control.reshape(LEV * CHUNK, BY)
    for i in range(CHUNK):
        here = pl.ds(i, LEV, stride=CHUNK)
        high, low = split_two(flat[here, :])
        back = wide[here, :].astype(BF16)
        both = jnp.concatenate(
            [
                jnp.concatenate([high, low], axis=1),
                jnp.concatenate([back, jnp.zeros_like(back)], axis=1),
            ],
            axis=0,
        )
        turned = nt(pair, both)
        ct[i] = turned[:, :LEV]
        bgt[i] = turned[:, LEV:].astype(BF16)
        for n, y in enumerate((0, 1, BY - 2, BY - 1)):
            planes[n, pl.ds(step * CHUNK + i, 1), :] = turned[y : y + 1, :LEV]

    @pl.when(step == 0)
    def _():
        x_down[:BY, :] = ct[0].astype(BF16)
        x_down[BY : 2 * BY, :] = ct[1].astype(BF16)

    @pl.when(step == pl.num_programs(0) - 1)
    def _():
        x_up[:BY, :] = ct[CHUNK - 2].astype(BF16)
        x_up[BY : 2 * BY, :] = ct[CHUNK - 1].astype(BF16)
        s = spread[...]
        turned = jnp.transpose(jnp.concatenate([s, s], axis=0))

        def rows(two):
            high, low = split_two(two)
            zero = jnp.zeros((12, BY), F32)
            return jnp.concatenate([high.astype(F32), low.astype(F32), zero], axis=0).astype(BF16)

        x_down[2 * BY :, :] = rows(s[0:2, :])
        x_up[2 * BY :, :] = rows(s[BX - 2 : BX, :])
        y_down[: 2 * BX, :] = planes[0:2].reshape(2 * BX, LEV).astype(BF16)
        y_up[: 2 * BX, :] = planes[2:4].reshape(2 * BX, LEV).astype(BF16)
        y_down[2 * BX :, :] = rows(turned[0:2, :])
        y_up[2 * BX :, :] = rows(turned[BY - 2 : BY, :])


def to_columns(control, background, spread):
    keep = lambda i: (0, 0)
    return pl.pallas_call(
        columns_kernel,
        grid=(BX // CHUNK,),
        in_specs=[
            pl.BlockSpec((LEV, CHUNK, BY), lambda i: (0, i, 0)),
            pl.BlockSpec((LEV, CHUNK, BY), lambda i: (0, i, 0)),
            pl.BlockSpec((BX, BY), keep),
        ],
        out_specs=[
            pl.BlockSpec((CHUNK, BY, LEV), lambda i: (i, 0, 0)),
            pl.BlockSpec((CHUNK, BY, LEV), lambda i: (i, 0, 0)),
            pl.BlockSpec((2 * BY + 16, LEV), keep),
            pl.BlockSpec((2 * BY + 16, LEV), keep),
            pl.BlockSpec((2 * BX + 16, LEV), keep),
            pl.BlockSpec((2 * BX + 16, LEV), keep),
        ],
        out_shape=[
            pltpu.HBM((BX, BY, LEV), F32),
            pltpu.HBM((BX, BY, LEV), BF16),
            jax.ShapeDtypeStruct((2 * BY + 16, LEV), BF16),
            jax.ShapeDtypeStruct((2 * BY + 16, LEV), BF16),
            jax.ShapeDtypeStruct((2 * BX + 16, LEV), BF16),
            jax.ShapeDtypeStruct((2 * BX + 16, LEV), BF16),
        ],
        scratch_shapes=[
            pltpu.VMEM((LEV * CHUNK, BY), F32),
            pltpu.VMEM((4, BX, LEV), F32),
        ],
        compiler_params=params(10, dimension_semantics=("arbitrary",)),
        cost_estimate=cost(6),
        name="columns",
    )(in_hbm(control), in_hbm(background), spread)


def shift(array, axis, by):
    count = lax.axis_size(axis)
    return lax.ppermute(array, axis, [(i, (i + by) % count) for i in range(count)])


def compose_kernel(x_up, x_down, y_low, y_high, up, down):
    rows = x_up.shape[0]
    up[:rows, :] = x_up[...]
    down[:rows, :] = x_down[...]
    low = y_low[...].astype(F32)
    high = y_high[...].astype(F32)
    fields = [low[2 * BX :], high[2 * BX :]] if low.shape[0] > 2 * BX else []
    for out, row in ((up, BX - 1), (down, 0)):
        pair = [low[BX + row : BX + row + 1], high[row : row + 1], jnp.zeros((14, LEV), F32)]
        out[rows:, :] = jnp.concatenate(pair + fields, axis=0).astype(BF16)


def compose(x_up, x_down, y_low, y_high):
    rows = x_up.shape[0] + 16 + 2 * (y_low.shape[0] - 2 * BX)
    return pl.pallas_call(
        compose_kernel,
        out_shape=[jax.ShapeDtypeStruct((rows, LEV), BF16)] * 2,
        compiler_params=params(2),
        name="compose",
    )(x_up, x_down, y_low, y_high)


def laplace(field, x, first, count):
    total = field[x + 1, pl.ds(first, count), :] + field[x - 1, pl.ds(first, count), :]
    total = total + field[x, pl.ds(first + 1, count), :]
    total = total + field[x, pl.ds(first - 1, count), :]
    return total - 4.0 * field[x, pl.ds(first, count), :]


def plane(field, x, y, count):
    flat = field.reshape(PX * PY, LEV)
    return flat[pl.ds(x * PY + y, count, stride=PY), :]


def set_plane(field, x, y, count, value):
    flat = field.reshape(PX * PY, LEV)
    flat[pl.ds(x * PY + y, count, stride=PY), :] = value


def plane_laplace(field, y):
    total = plane(field, 3, y, BX) + plane(field, 1, y, BX)
    total = total + plane(field, 2, y + 1, BX) + plane(field, 2, y - 1, BX)
    return total - 4.0 * plane(field, 2, y, BX)


def lanes(column):
    return jnp.broadcast_to(column, (column.shape[0], LEV))


def joined(rows, at):
    block = rows[at : at + 16, :].astype(F32)
    return block[0:2] + block[2:4]


def fill_y(field, y_low, y_high):
    for n in range(2):
        set_plane(field, 2, 6 + n, BX, y_low[n * BX : (n + 1) * BX, :].astype(F32))
        set_plane(field, 2, 8 + BY + n, BX, y_high[n * BX : (n + 1) * BX, :].astype(F32))


def fill_x(field, x_low, x_high, at):
    for n in range(2):
        field[n, 8 : 8 + BY, :] = x_low[n * BY : (n + 1) * BY, :].astype(F32)
        field[BX + 2 + n, 8 : 8 + BY, :] = x_high[n * BY : (n + 1) * BY, :].astype(F32)
    for rows, x in ((x_low, 1), (x_high, BX + 2)):
        pair = rows[at : at + 16, :].astype(F32)
        field[x, 7:8, :] = pair[0:1]
        field[x, 8 + BY : 9 + BY, :] = pair[1:2]


def coefficients(coef, spread, x_low, x_high, y_low, y_high, rows):
    square = jnp.concatenate(
        [joined(x_low, 2 * BY), spread[...], joined(x_high, 2 * BY), jnp.zeros((BY - PX, BY), F32)],
        axis=0,
    )
    turned = jnp.transpose(square)
    for x in rows:
        coef[x, 8 : 8 + BY, :] = lanes(turned[:, x : x + 1])
    sides = jnp.concatenate(
        [joined(y_low, 2 * BX), joined(y_high, 2 * BX), jnp.zeros((BY - 4, BY), F32)], axis=0
    )
    sides = jnp.transpose(sides)[:BX, :]
    for n in range(2):
        set_plane(coef, 2, 6 + n, BX, lanes(sides[:, n : n + 1]))
        set_plane(coef, 2, 8 + BY + n, BX, lanes(sides[:, 2 + n : 3 + n]))
    for block, x, lane in ((x_low, 1, BX - 1), (x_high, BX + 2, 0)):
        left = joined(block, 2 * BY + 32)
        right = joined(block, 2 * BY + 48)
        coef[x, 7:8, :] = lanes(left[1:2, lane : lane + 1])
        coef[x, 8 + BY : 9 + BY, :] = lanes(right[0:1, lane : lane + 1])


def joined(rows, at):
    block = rows[at : at + 16, :].astype(F32)
    return block[0:2] + block[2:4]


PARTS = BX // CHUNK


def increment_kernel(
    ct, spread, x_low, x_high, y_low, y_high, inc, coef, field, first, done, came, went
):
    def bring(part):
        at = pl.ds(part * CHUNK, CHUNK)
        to = field.at[pl.ds(2 + part * CHUNK, CHUNK), pl.ds(8, BY)]
        return pltpu.make_async_copy(ct.at[at], to, came.at[part])

    def leave(part):
        at = pl.ds(part * CHUNK, CHUNK)
        return pltpu.make_async_copy(done.at[at], inc.at[at], went.at[part])

    for part in range(PARTS):
        bring(part).start()
    coefficients(coef, spread, x_low, x_high, y_low, y_high, range(PX))
    fill_x(field, x_low, x_high, 2 * BY + 16)
    fill_y(field, y_low, y_high)

    def sweep_one(x, carry):
        middle = field[x, 8 : 8 + BY, :]
        first[x, 8 : 8 + BY, :] = middle + coef[x, 8 : 8 + BY, :] * laplace(field, x, 8, BY)
        return carry

    for part in range(PARTS):
        bring(part).wait()
        last = PX - 1 if part == PARTS - 1 else 1 + CHUNK * (part + 1)
        lax.fori_loop(1 + CHUNK * part, last, sweep_one, 0)
    for y in (7, 8 + BY):
        moved = plane(field, 2, y, BX) + plane(coef, 2, y, BX) * plane_laplace(field, y)
        set_plane(first, 2, y, BX, moved)

    def sweep_two(x, carry):
        middle = first[x, 8 : 8 + BY, :]
        result = middle + coef[x, 8 : 8 + BY, :] * laplace(first, x, 8, BY)
        done[x - 2] = result.astype(BF16)
        return carry

    for part in range(PARTS):
        lax.fori_loop(2 + CHUNK * part, 2 + CHUNK * (part + 1), sweep_two, 0)
        leave(part).start()
    for part in range(PARTS):
        leave(part).wait()


def increments(ct, spread, rims):
    any_space = pl.BlockSpec(memory_space=pltpu.HBM)
    whole = pl.BlockSpec(memory_space=pltpu.VMEM)
    return pl.pallas_call(
        increment_kernel,
        in_specs=[any_space] + [whole] * 5,
        out_specs=any_space,
        out_shape=pltpu.HBM((BX, BY, LEV), BF16),
        scratch_shapes=[pltpu.VMEM((PX, PY, LEV), F32)] * 3
        + [
            pltpu.VMEM((BX, BY, LEV), BF16),
            pltpu.SemaphoreType.DMA((PARTS,)),
            pltpu.SemaphoreType.DMA((PARTS,)),
        ],
        compiler_params=params(27),
        cost_estimate=cost(6),
        name="increment",
    )(in_hbm(ct), spread, *rims)


def decode(rows):
    back = lambda n: pltpu.roll(rows, LEV - n, 1)
    frac_x = back(2) + back(3) + back(4)
    frac_y = back(5) + back(6) + back(7)
    valid = rows > 0.5
    cell = jnp.where(valid, (rows - 1.0) * BY + back(1), 0.0).astype(jnp.int32)
    off = lambda w: jnp.where(valid, w, 0.0)
    return cell, (
        off((1.0 - frac_x) * (1.0 - frac_y)),
        off(frac_x * (1.0 - frac_y)),
        off((1.0 - frac_x) * frac_y),
        off(frac_x * frac_y),
    )


def gather_kernel(
    got, background, increment, reply, slots,
    wide, cells, table, ga, gb, gc, gd, spaced, bgt, inct, packed, came,
):
    part = CELLS // PARTS

    def bring(n, i):
        at = pl.ds(i * part, part)
        source = (background, increment)[n]
        return pltpu.make_async_copy(source.at[at], packed.at[n, at], came.at[n, i])

    for i in range(PARTS):
        bring(0, i).start()
        bring(1, i).start()
    wide[...] = got[...].astype(F32).reshape(DEV * ROWS, LEV)
    cell, weights = decode(wide[pl.ds(CAP, DEV, stride=ROWS), :])
    cells[...] = cell
    pltpu.sync_copy(cells, table)
    for i in range(PARTS):
        for n, wider in ((0, bgt), (1, inct)):
            bring(n, i).wait()

            def widen(j, carry):
                at = pl.ds(pl.multiple_of(i * part + j * BY, BY), BY)
                wider[at, :] = packed[n, at, :].astype(F32)
                return carry

            lax.fori_loop(0, part // BY, widen, 0)
    for k in range(CAP):

        def fetch(step, carry):
            for n in range(8):
                owner = step * 8 + n
                at = table[owner, 8 * k]
                to = pl.ds(2 * (k * DEV + owner), 2)
                ga[to, :] = bgt[pl.ds(at, 2), :]
                gb[to, :] = bgt[pl.ds(at + BY, 2), :]
                gc[to, :] = inct[pl.ds(at, 2), :]
                gd[to, :] = inct[pl.ds(at + BY, 2), :]
            return carry

        lax.fori_loop(0, DEV // 8, fetch, 0)
    spaced[...] = jnp.zeros_like(spaced)
    for k in range(CAP):
        w = [lanes(weight[:, 8 * k : 8 * k + 1]) for weight in weights]
        even = pl.ds(2 * DEV * k, DEV, stride=2)
        odd = pl.ds(2 * DEV * k + 1, DEV, stride=2)
        for n, (one, two) in enumerate(((ga, gb), (gc, gd))):
            mixed = w[0] * one[even, :] + w[1] * two[even, :]
            mixed = mixed + w[2] * one[odd, :]
            mixed = mixed + w[3] * two[odd, :]
            slots[k * DEV : (k + 1) * DEV, n * LEV : (n + 1) * LEV] = mixed.astype(BF16)
            spaced[n, pl.ds(k, DEV, stride=ROWS), :] = mixed
    reply[:, :LEV] = spaced[0].astype(BF16)
    reply[:, LEV:] = spaced[1].astype(BF16)


def gathered(got, bgt, inct):
    rows = pltpu.VMEM((2 * SLOTS, LEV), F32)
    whole = pl.BlockSpec(memory_space=pltpu.VMEM)
    return pl.pallas_call(
        gather_kernel,
        grid=(1,),
        in_specs=[pl.BlockSpec((DEV, ROWS, LEV), lambda i: (0, 0, 0))]
        + [pl.BlockSpec(memory_space=pltpu.HBM)] * 2,
        out_specs=[whole, whole],
        out_shape=[
            jax.ShapeDtypeStruct((DEV * ROWS, 2 * LEV), BF16),
            jax.ShapeDtypeStruct((SLOTS, 2 * LEV), BF16),
        ],
        scratch_shapes=[
            pltpu.VMEM((DEV * ROWS, LEV), F32),
            pltpu.VMEM((DEV, LEV), jnp.int32),
            pltpu.SMEM((DEV, LEV), jnp.int32),
            rows,
            rows,
            rows,
            rows,
            pltpu.VMEM((2, DEV * ROWS, LEV), F32),
            pltpu.VMEM((CELLS, LEV), F32),
            pltpu.VMEM((CELLS, LEV), F32),
            pltpu.VMEM((2, CELLS, LEV), BF16),
            pltpu.SemaphoreType.DMA((2, PARTS)),
        ],
        compiler_params=params(26),
        cost_estimate=cost(5),
        name="gather",
    )(got, in_hbm(bgt), in_hbm(inct))


def tangent(base, delta, w_first, b_first, w_second, b_second):
    h_one = jnp.tanh(nn(base, w_first) + b_first)
    d_one = 1.0 - h_one * h_one
    h_two = jnp.tanh(nn(h_one.astype(BF16), w_second) + b_second)
    d_two = 1.0 - h_two * h_two
    t_one = (d_one * nn(delta, w_first)).astype(BF16)
    t_two = (d_two * nn(t_one, w_second)).astype(BF16)
    return d_one, d_two, t_two


BLOCK = 256


def adjoint_kernel(
    got, slots, w_first, b_first, w_second, b_second, w_third, ivar,
    acc, x_up, x_down, y_up, y_down,
    wide, pulled, profile, cells, table, ca, cb,
):
    for n in range(HID // LEV):
        at = slice(n * LEV, (n + 1) * LEV)
        wide[...] = got[:, :, at].astype(F32).reshape(DEV * ROWS, LEV)
        for k in range(CAP):
            pulled[k * DEV : (k + 1) * DEV, at] = wide[pl.ds(k, DEV, stride=ROWS), :]
        if n == 0:
            cell, weights = decode(wide[pl.ds(CAP, DEV, stride=ROWS), :])
    cells[...] = cell
    pltpu.sync_copy(cells, table)

    def block(i, carry):
        here = pl.ds(pl.multiple_of(i * BLOCK, BLOCK), BLOCK)
        d_one, d_two, t_two = tangent(
            slots[here, :LEV], slots[here, LEV:],
            w_first[...], b_first[...], w_second[...], b_second[...],
        )
        change = nt(t_two, w_third[...]) * ivar[...].reshape(1, CH)
        s_two = (d_two * (nn(change.astype(BF16), w_third[...]) - pulled[here, :])).astype(BF16)
        s_one = (d_one * nt(s_two, w_second[...])).astype(BF16)
        profile[here, :] = nt(s_one, w_first[...])
        return carry

    lax.fori_loop(0, SLOTS // BLOCK, block, 0)
    acc[...] = jnp.zeros_like(acc)
    for k in range(CAP):
        grad = profile[k * DEV : (k + 1) * DEV, :]
        w = [lanes(weight[:, 8 * k : 8 * k + 1]) for weight in weights]
        even = pl.ds(2 * DEV * k, DEV, stride=2)
        odd = pl.ds(2 * DEV * k + 1, DEV, stride=2)
        ca[even, :] = w[0] * grad
        cb[even, :] = w[1] * grad
        ca[odd, :] = w[2] * grad
        cb[odd, :] = w[3] * grad
    for k in range(CAP):

        def add(step, carry):
            for n in range(8):
                owner = step * 8 + n
                at = table[owner, 8 * k]
                there = pl.ds(2 * (k * DEV + owner), 2)
                one = acc[pl.ds(at, 2), :] + ca[there, :]
                two = acc[pl.ds(at + BY, 2), :] + cb[there, :]
                acc[pl.ds(at, 2), :] = one
                acc[pl.ds(at + BY, 2), :] = two
            return carry

        lax.fori_loop(0, DEV // 8, add, 0)
    x_down[...] = acc[: 2 * BY, :].astype(BF16)
    x_up[...] = acc[CELLS - 2 * BY :, :].astype(BF16)
    for n in range(2):
        y_down[n * BX : (n + 1) * BX, :] = acc[pl.ds(n, BX, stride=BY), :].astype(BF16)
        y_up[n * BX : (n + 1) * BX, :] = acc[pl.ds(BY - 2 + n, BX, stride=BY), :].astype(BF16)


def adjoint(got, slots, w_first, b_first, w_second, b_second, w_third, ivar):
    return pl.pallas_call(
        adjoint_kernel,
        out_shape=[
            pltpu.VMEM((CELLS, LEV), F32),
            jax.ShapeDtypeStruct((2 * BY, LEV), BF16),
            jax.ShapeDtypeStruct((2 * BY, LEV), BF16),
            jax.ShapeDtypeStruct((2 * BX, LEV), BF16),
            jax.ShapeDtypeStruct((2 * BX, LEV), BF16),
        ],
        scratch_shapes=[
            pltpu.VMEM((DEV * ROWS, LEV), F32),
            pltpu.VMEM((SLOTS, HID), F32),
            pltpu.VMEM((SLOTS, LEV), F32),
            pltpu.VMEM((DEV, LEV), jnp.int32),
            pltpu.SMEM((DEV, LEV), jnp.int32),
            pltpu.VMEM((2 * SLOTS, LEV), F32),
            pltpu.VMEM((2 * SLOTS, LEV), F32),
        ],
        compiler_params=params(24),
        cost_estimate=cost(10),
        name="adjoint",
    )(got, slots, w_first, b_first, w_second, b_second, w_third, ivar)


def departure_kernel(
    reply, holder, innov, w_first, b_first, w_second, b_second, w_third, ivar, out
):
    held = holder[...]
    pick = (iota((OWN, DEV * ROWS), 1) == down(held * ROWS + ranks(held)).astype(jnp.int32)[:, 0:1]).astype(BF16)
    own = nn(pick, reply[...]).astype(BF16)
    _, _, t_two = tangent(
        own[:, :LEV], own[:, LEV:], w_first[...], b_first[...], w_second[...], b_second[...]
    )
    each = down(ivar[...].reshape(1, CH))
    out[...] = (nt(w_third[...], t_two) - innov[...]) * jnp.concatenate([each, each], axis=1)


def departures_of(reply, holder, innov, w_first, b_first, w_second, b_second, w_third, ivar):
    return pl.pallas_call(
        departure_kernel,
        out_shape=jax.ShapeDtypeStruct((CH, OWN), F32),
        compiler_params=params(12),
        cost_estimate=cost(4),
        name="departures",
    )(reply, holder, innov, w_first, b_first, w_second, b_second, w_third, ivar)


def gradient_kernel(edge, acc, spread, ax_low, ax_high, ay_low, ay_high, y_low, y_high, *rest):
    if edge:
        x_low, x_high, control, _, out, coef, field, grown, second = rest
    else:
        control, out, coef, field, grown, second = rest
    step = pl.program_id(0)
    first = step * (PARTS - 1) * CHUNK if edge else (step + 1) * CHUNK

    @pl.when(step == 0)
    def _():
        rows = [*range(12), *range(PX - 12, PX)] if edge else range(CHUNK, PX - CHUNK)
        coefficients(coef, spread, ax_low, ax_high, ay_low, ay_high, rows)
        fill_y(field, y_low, y_high)
        if edge:
            fill_x(field, x_low, x_high, 2 * BY)

    def fill(x, carry):
        field[x, 8 : 8 + BY, :] = acc[pl.ds(pl.multiple_of((x - 2) * BY, BY), BY), :]
        return carry

    if edge:
        start, stop = jnp.where(step == 0, 2, first), jnp.where(step == 0, 12, PX - 2)
        lax.fori_loop(start, stop, fill, 0)
    else:
        lax.fori_loop(jnp.where(step == 0, first, first + 4), first + CHUNK + 4, fill, 0)
    span = CHUNK + 4

    def scale(i, carry):
        grown[i] = field[first + i] * coef[first + i]
        return carry

    lax.fori_loop(0, span, scale, 0)

    def sweep_one(i, carry):
        value = field[first + i, 8 : 8 + BY, :] + laplace(grown, i, 8, BY)
        second[1, i, 8 : 8 + BY, :] = value
        second[0, i, 8 : 8 + BY, :] = coef[first + i, 8 : 8 + BY, :] * value
        return carry

    lax.fori_loop(1, span - 1, sweep_one, 0)

    def column(ref, offset, y):
        flat = ref.reshape(ref.shape[0] * PY, LEV)
        return flat[pl.ds((first + offset) * PY + y, CHUNK, stride=PY), :]

    def local(ref, offset, y):
        flat = ref.reshape(ref.shape[0] * PY, LEV)
        return flat[pl.ds(offset * PY + y, CHUNK, stride=PY), :]

    scaled = second.at[0]
    flat_scaled = scaled.reshape(span * PY, LEV)
    for y in (7, 8 + BY):
        total = local(grown, 3, y) + local(grown, 1, y)
        total = total + local(grown, 2, y + 1) + local(grown, 2, y - 1)
        value = column(field, 2, y) + (total - 4.0 * local(grown, 2, y))
        flat_scaled[pl.ds(2 * PY + y, CHUNK, stride=PY), :] = column(coef, 2, y) * value
    pair = eye_pair()
    flat_out = out.reshape(LEV * CHUNK, BY)
    flat_control = control.reshape(LEV * CHUNK, BY)
    for i in range(CHUNK):
        value = second[1, 2 + i, 8 : 8 + BY, :] + laplace(scaled, 2 + i, 8, BY)
        high_part, low_part = split_two(value)
        turned = nt(pair, jnp.concatenate([high_part, low_part], axis=1))
        here = pl.ds(i, LEV, stride=CHUNK)
        flat_out[here, :] = turned + flat_control[here, :]


def gradient_of(acc, spread, before, rims, control, so_far=None):
    edge = so_far is not None
    whole = pl.BlockSpec(memory_space=pltpu.VMEM)
    if edge:
        block = pl.BlockSpec((LEV, CHUNK, BY), lambda i: (0, i * (PARTS - 1), 0))
    else:
        block = pl.BlockSpec((LEV, CHUNK, BY), lambda i: (0, i + 1, 0))
    operands = [in_vmem(acc), spread, *before, *rims, in_hbm(control)]
    specs = [whole] * (len(operands) - 1) + [block]
    if edge:
        operands.append(in_hbm(so_far))
        specs.append(pl.BlockSpec(memory_space=pltpu.HBM))
    return pl.pallas_call(
        functools.partial(gradient_kernel, edge),
        grid=(2 if edge else PARTS - 2,),
        in_specs=specs,
        out_specs=block,
        out_shape=pltpu.HBM((LEV, BX, BY), F32),
        input_output_aliases={len(operands) - 1: 0} if edge else {},
        scratch_shapes=[
            pltpu.VMEM((PX, PY, LEV), F32),
            pltpu.VMEM((PX, PY, LEV), F32),
            pltpu.VMEM((CHUNK + 4, PY, LEV), F32),
            pltpu.VMEM((2, CHUNK + 4, PY, LEV), F32),
        ],
        compiler_params=params(20, dimension_semantics=("arbitrary",)),
        cost_estimate=cost(2 if edge else 6),
        name="edges" if edge else "interior",
    )(*operands)


def exchange(array):
    return lax.all_to_all(array, ("tile", "obs"), split_axis=0, concat_axis=0, tiled=True)


def per_device(
    control,
    background,
    spread,
    obs_holder,
    obs_anchor,
    obs_frac,
    innovation,
    inverse_var,
    w_first,
    b_first,
    w_second,
    b_second,
    w_third,
):
    b_one = b_first.reshape(1, HID)
    b_two = b_second.reshape(1, HID)
    holder = obs_holder.reshape(1, OWN)
    innov = innovation.T
    w_last = w_third.T
    ct, bgt, x_up, x_down, y_up, y_down = to_columns(control, background, spread)
    ay_low, ay_high = shift(y_up, "obs", 1), shift(y_down, "obs", -1)
    asked = requests(holder, obs_anchor.reshape(1, OWN), obs_frac, innov, inverse_var, w_last)
    x_up, x_down = compose(x_up, x_down, ay_low, ay_high)
    ax_low, ax_high = shift(x_up, "tile", 1), shift(x_down, "tile", -1)
    before = (ax_low, ax_high, ay_low, ay_high)
    got = exchange(asked.reshape(DEV, ROWS, HID))
    inct = increments(ct, spread, before)
    reply, slots = gathered(got, bgt.reshape(CELLS, LEV), inct.reshape(CELLS, LEV))
    reply = exchange(reply.reshape(DEV, ROWS, 2 * LEV))
    acc, x_up, x_down, y_up, y_down = adjoint(
        got, slots, w_first, b_one, w_second, b_two, w_last, inverse_var
    )
    y_low, y_high = shift(y_up, "obs", 1), shift(y_down, "obs", -1)
    x_up, x_down = compose(x_up, x_down, y_low, y_high)
    x_low, x_high = shift(x_up, "tile", 1), shift(x_down, "tile", -1)
    gradient = gradient_of(acc, spread, before, (y_low, y_high), control)
    gradient = gradient_of(acc, spread, before, (y_low, y_high, x_low, x_high), control, gradient)
    departures = departures_of(
        reply.reshape(DEV * ROWS, 2 * LEV), holder, innov,
        w_first, b_one, w_second, b_two, w_last, inverse_var,
    ).T
    return departures, gradient


def solution(mesh):
    return jax.shard_map(
        per_device,
        mesh=mesh,
        in_specs=(
            P(None, "tile", "obs"),
            P(None, "tile", "obs"),
            P("tile", "obs"),
            P(("tile", "obs"), None),
            P(("tile", "obs")),
            P(None, ("tile", "obs")),
            P(("tile", "obs"), None),
            P(),
            P(),
            P(),
            P(),
            P(),
            P(),
        ),
        out_specs=(P(("tile", "obs"), None), P(None, "tile", "obs")),
        check_vma=False,
    )
```

```python
import jax
import jax.numpy as jnp
from jax import lax
from jax.experimental import pallas as pl
from jax.experimental.pallas import tpu as pltpu
from jax.sharding import PartitionSpec as P


F32 = jnp.float32
BF16 = jnp.bfloat16
LEV = 128
BX = 64
BY = 128
CELLS = BX * BY
OWN = 256
DEV = 128
CAP = 6
ROWS = 8
SLOTS = CAP * DEV
HID = 512
CH = 616
PX = BX + 4
PY = BY + 16
CHUNK = 8
TALL = 16


def params(mib, **extra):
    return pltpu.CompilerParams(vmem_limit_bytes=mib * 1024 * 1024, **extra)


def cost(us):
    return pl.CostEstimate(flops=int(us * 1.0e9), bytes_accessed=0, transcendentals=0)


def tn(a, b):
    return lax.dot_general(a, b, (((0,), (0,)), ((), ())), preferred_element_type=F32)


def down(row):
    return jnp.transpose(jnp.broadcast_to(row, (LEV, row.shape[1])))


def in_vmem(array):
    return pltpu.with_memory_space_constraint(array, pltpu.VMEM)


def in_hbm(array):
    return pltpu.with_memory_space_constraint(array, pltpu.HBM)


def nn(a, b):
    return jnp.dot(a, b, preferred_element_type=F32)


def nt(a, b):
    return lax.dot_general(a, b, (((1,), (1,)), ((), ())), preferred_element_type=F32)


def iota(shape, dim):
    return lax.broadcasted_iota(jnp.int32, shape, dim)


def split_two(a):
    high = a.astype(BF16)
    return high, (a - high.astype(F32)).astype(BF16)


def eye_pair():
    row = iota((LEV, 2 * LEV), 0)
    col = iota((LEV, 2 * LEV), 1)
    return ((col == row) | (col == row + LEV)).astype(BF16)


def ranks(held):
    marks = (iota((DEV, OWN), 0) == held).astype(BF16)
    before = (iota((OWN, OWN), 0) < iota((OWN, OWN), 1)).astype(BF16)
    return jnp.sum(marks.astype(F32) * nn(marks, before), axis=0, keepdims=True).astype(jnp.int32)


def request_kernel(holder, anchor, frac, innov, ivar, w_third, out):
    held = holder[...]
    rank = ranks(held)
    at = anchor[...].astype(F32)
    x = jnp.floor((at + 0.5) * (1.0 / (BY - 1)))
    y = at - (BY - 1) * x
    fields = [x + 1.0, y]
    for dim in range(2):
        value = frac[dim : dim + 1, :]
        for _ in range(3):
            piece = value.astype(BF16).astype(F32)
            fields.append(piece)
            value = value - piece
    fields = jnp.concatenate(fields, axis=0)
    fields = jnp.concatenate([fields] * (LEV // 8), axis=0)
    fields = jnp.where((iota((LEV, OWN), 0) >> 3) == rank, fields, 0.0).astype(BF16)
    each = down(ivar[...].reshape(1, CH))
    scaled = (innov[...] * jnp.concatenate([each, each], axis=1)).astype(BF16)
    pulled = tn(scaled, w_third[...]).astype(BF16)
    row = iota((DEV * ROWS, OWN), 0)
    to_slot = (row == held * ROWS + rank).astype(BF16)
    to_fields = (row == held * ROWS + CAP).astype(BF16)
    out[:, :LEV] = (nn(to_slot, pulled[:, :LEV]) + nt(to_fields, fields)).astype(BF16)
    out[:, LEV:] = nn(to_slot, pulled[:, LEV:]).astype(BF16)


def requests(holder, anchor, frac, innov, ivar, w_third):
    return pl.pallas_call(
        request_kernel,
        out_shape=jax.ShapeDtypeStruct((DEV * ROWS, HID), BF16),
        compiler_params=params(12),
        cost_estimate=cost(4),
        name="requests",
    )(*map(in_hbm, (holder, anchor, frac, innov, ivar, w_third)))


def columns_kernel(control, background, spread, field, bgt, x_up, x_down, y_up, y_down, wide, planes):
    step = pl.program_id(0)
    pair = eye_pair()
    wide[...] = background[...].astype(F32).reshape(LEV * TALL, BY)
    flat = control.reshape(LEV * TALL, BY)
    for i in range(TALL):
        here = pl.ds(i, LEV, stride=TALL)
        high, low = split_two(flat[here, :])
        back = wide[here, :].astype(BF16)
        both = jnp.concatenate(
            [
                jnp.concatenate([high, low], axis=1),
                jnp.concatenate([back, jnp.zeros_like(back)], axis=1),
            ],
            axis=0,
        )
        turned = nt(pair, both)
        field[step * TALL + i + 2, 8 : 8 + BY, :] = turned[:, :LEV]
        bgt[i] = turned[:, LEV:].astype(BF16)
        for n, y in enumerate((0, 1, BY - 2, BY - 1)):
            planes[n, pl.ds(step * TALL + i, 1), :] = turned[y : y + 1, :LEV]

    @pl.when(step == 0)
    def _():
        x_down[:BY, :] = field[2, 8 : 8 + BY, :].astype(BF16)
        x_down[BY : 2 * BY, :] = field[3, 8 : 8 + BY, :].astype(BF16)

    @pl.when(step == pl.num_programs(0) - 1)
    def _():
        x_up[:BY, :] = field[BX, 8 : 8 + BY, :].astype(BF16)
        x_up[BY : 2 * BY, :] = field[BX + 1, 8 : 8 + BY, :].astype(BF16)
        s = spread[...]
        turned = jnp.transpose(jnp.concatenate([s, s], axis=0))

        def rows(two):
            high, low = split_two(two)
            zero = jnp.zeros((12, BY), F32)
            return jnp.concatenate([high.astype(F32), low.astype(F32), zero], axis=0).astype(BF16)

        x_down[2 * BY :, :] = rows(s[0:2, :])
        x_up[2 * BY :, :] = rows(s[BX - 2 : BX, :])
        y_down[: 2 * BX, :] = planes[0:2].reshape(2 * BX, LEV).astype(BF16)
        y_up[: 2 * BX, :] = planes[2:4].reshape(2 * BX, LEV).astype(BF16)
        y_down[2 * BX :, :] = rows(turned[0:2, :])
        y_up[2 * BX :, :] = rows(turned[BY - 2 : BY, :])


def to_columns(control, background, spread):
    keep = lambda i: (0, 0)
    return pl.pallas_call(
        columns_kernel,
        grid=(BX // TALL,),
        in_specs=[
            pl.BlockSpec((LEV, TALL, BY), lambda i: (0, i, 0)),
            pl.BlockSpec((LEV, TALL, BY), lambda i: (0, i, 0)),
            pl.BlockSpec((BX, BY), keep),
        ],
        out_specs=[
            pl.BlockSpec(memory_space=pltpu.VMEM),
            pl.BlockSpec((TALL, BY, LEV), lambda i: (i, 0, 0)),
            pl.BlockSpec((2 * BY + 16, LEV), keep),
            pl.BlockSpec((2 * BY + 16, LEV), keep),
            pl.BlockSpec((2 * BX + 16, LEV), keep),
            pl.BlockSpec((2 * BX + 16, LEV), keep),
        ],
        out_shape=[
            pltpu.VMEM((PX, PY, LEV), F32),
            pltpu.HBM((BX, BY, LEV), BF16),
            jax.ShapeDtypeStruct((2 * BY + 16, LEV), BF16),
            jax.ShapeDtypeStruct((2 * BY + 16, LEV), BF16),
            jax.ShapeDtypeStruct((2 * BX + 16, LEV), BF16),
            jax.ShapeDtypeStruct((2 * BX + 16, LEV), BF16),
        ],
        scratch_shapes=[
            pltpu.VMEM((LEV * TALL, BY), F32),
            pltpu.VMEM((4, BX, LEV), F32),
        ],
        compiler_params=params(16, dimension_semantics=("arbitrary",)),
        cost_estimate=cost(6),
        name="columns",
    )(in_hbm(control), in_hbm(background), spread)


def shift(array, axis, by):
    count = lax.axis_size(axis)
    return lax.ppermute(array, axis, [(i, (i + by) % count) for i in range(count)])


def compose_kernel(x_up, x_down, y_low, y_high, up, down):
    rows = x_up.shape[0]
    up[:rows, :] = x_up[...]
    down[:rows, :] = x_down[...]
    low = y_low[...].astype(F32)
    high = y_high[...].astype(F32)
    fields = [low[2 * BX :], high[2 * BX :]] if low.shape[0] > 2 * BX else []
    for out, row in ((up, BX - 1), (down, 0)):
        pair = [low[BX + row : BX + row + 1], high[row : row + 1], jnp.zeros((14, LEV), F32)]
        out[rows:, :] = jnp.concatenate(pair + fields, axis=0).astype(BF16)


def compose(x_up, x_down, y_low, y_high):
    rows = x_up.shape[0] + 16 + 2 * (y_low.shape[0] - 2 * BX)
    return pl.pallas_call(
        compose_kernel,
        out_shape=[jax.ShapeDtypeStruct((rows, LEV), BF16)] * 2,
        compiler_params=params(2),
        name="compose",
    )(x_up, x_down, y_low, y_high)


def laplace(field, x, first, count):
    total = field[x + 1, pl.ds(first, count), :] + field[x - 1, pl.ds(first, count), :]
    total = total + field[x, pl.ds(first + 1, count), :]
    total = total + field[x, pl.ds(first - 1, count), :]
    return total - 4.0 * field[x, pl.ds(first, count), :]


def plane(field, x, y, count):
    flat = field.reshape(PX * PY, LEV)
    return flat[pl.ds(x * PY + y, count, stride=PY), :]


def set_plane(field, x, y, count, value):
    flat = field.reshape(PX * PY, LEV)
    flat[pl.ds(x * PY + y, count, stride=PY), :] = value


def plane_laplace(field, y):
    total = plane(field, 3, y, BX) + plane(field, 1, y, BX)
    total = total + plane(field, 2, y + 1, BX) + plane(field, 2, y - 1, BX)
    return total - 4.0 * plane(field, 2, y, BX)


def lanes(column):
    return jnp.broadcast_to(column, (column.shape[0], LEV))


def joined(rows, at):
    block = rows[at : at + 16, :].astype(F32)
    return block[0:2] + block[2:4]


def fill_y(field, y_low, y_high):
    for n in range(2):
        set_plane(field, 2, 6 + n, BX, y_low[n * BX : (n + 1) * BX, :].astype(F32))
        set_plane(field, 2, 8 + BY + n, BX, y_high[n * BX : (n + 1) * BX, :].astype(F32))


def fill_x(field, x_low, x_high, at):
    for n in range(2):
        field[n, 8 : 8 + BY, :] = x_low[n * BY : (n + 1) * BY, :].astype(F32)
        field[BX + 2 + n, 8 : 8 + BY, :] = x_high[n * BY : (n + 1) * BY, :].astype(F32)
    for rows, x in ((x_low, 1), (x_high, BX + 2)):
        pair = rows[at : at + 16, :].astype(F32)
        field[x, 7:8, :] = pair[0:1]
        field[x, 8 + BY : 9 + BY, :] = pair[1:2]


def main_coefficients(coef, spread):
    square = jnp.concatenate([spread[...], jnp.zeros((BY - BX, BY), F32)], axis=0)
    turned = jnp.transpose(square)
    for x in range(BX):
        coef[x + 2, 8 : 8 + BY, :] = lanes(turned[:, x : x + 1])


def rim_coefficients(coef, x_low, x_high, y_low, y_high):
    ends = jnp.concatenate(
        [joined(x_low, 2 * BY), joined(x_high, 2 * BY), jnp.zeros((BY - 4, BY), F32)], axis=0
    )
    ends = jnp.transpose(ends)
    for n, x in enumerate((0, 1, BX + 2, BX + 3)):
        coef[x, 8 : 8 + BY, :] = lanes(ends[:, n : n + 1])
    sides = jnp.concatenate(
        [joined(y_low, 2 * BX), joined(y_high, 2 * BX), jnp.zeros((BY - 4, BY), F32)], axis=0
    )
    sides = jnp.transpose(sides)[:BX, :]
    for n in range(2):
        set_plane(coef, 2, 6 + n, BX, lanes(sides[:, n : n + 1]))
        set_plane(coef, 2, 8 + BY + n, BX, lanes(sides[:, 2 + n : 3 + n]))
    for block, x, lane in ((x_low, 1, BX - 1), (x_high, BX + 2, 0)):
        left = joined(block, 2 * BY + 32)
        right = joined(block, 2 * BY + 48)
        coef[x, 7:8, :] = lanes(left[1:2, lane : lane + 1])
        coef[x, 8 + BY : 9 + BY, :] = lanes(right[0:1, lane : lane + 1])


def spread_kernel(spread, coef):
    main_coefficients(coef, spread)


def over_lanes(spread):
    return pl.pallas_call(
        spread_kernel,
        out_shape=pltpu.VMEM((PX, PY, LEV), F32),
        compiler_params=params(2),
        cost_estimate=cost(1),
        name="spread",
    )(spread)


def joined(rows, at):
    block = rows[at : at + 16, :].astype(F32)
    return block[0:2] + block[2:4]


PARTS = BX // CHUNK


def increment_kernel(
    _field, _coef, x_low, x_high, y_low, y_high, inc, field, coef, first, done, went
):
    def leave(part):
        at = pl.ds(part * CHUNK, CHUNK)
        return pltpu.make_async_copy(done.at[at], inc.at[at], went.at[part])

    rim_coefficients(coef, x_low, x_high, y_low, y_high)
    fill_x(field, x_low, x_high, 2 * BY + 16)
    fill_y(field, y_low, y_high)

    def sweep_one(x, carry):
        middle = field[x, 8 : 8 + BY, :]
        first[x, 8 : 8 + BY, :] = middle + coef[x, 8 : 8 + BY, :] * laplace(field, x, 8, BY)
        return carry

    lax.fori_loop(1, PX - 1, sweep_one, 0)
    for y in (7, 8 + BY):
        moved = plane(field, 2, y, BX) + plane(coef, 2, y, BX) * plane_laplace(field, y)
        set_plane(first, 2, y, BX, moved)

    def sweep_two(x, carry):
        middle = first[x, 8 : 8 + BY, :]
        result = middle + coef[x, 8 : 8 + BY, :] * laplace(first, x, 8, BY)
        done[x - 2] = result.astype(BF16)
        return carry

    for part in range(PARTS):
        lax.fori_loop(2 + CHUNK * part, 2 + CHUNK * (part + 1), sweep_two, 0)
        leave(part).start()
    for part in range(PARTS):
        leave(part).wait()


def increments(field, coef, rims):
    whole = pl.BlockSpec(memory_space=pltpu.VMEM)
    return pl.pallas_call(
        increment_kernel,
        in_specs=[whole] * 6,
        out_specs=[pl.BlockSpec(memory_space=pltpu.HBM), whole, whole],
        out_shape=[
            pltpu.HBM((BX, BY, LEV), BF16),
            pltpu.VMEM((PX, PY, LEV), F32),
            pltpu.VMEM((PX, PY, LEV), F32),
        ],
        input_output_aliases={0: 1, 1: 2},
        scratch_shapes=[
            pltpu.VMEM((PX, PY, LEV), F32),
            pltpu.VMEM((BX, BY, LEV), BF16),
            pltpu.SemaphoreType.DMA((PARTS,)),
        ],
        compiler_params=params(12),
        cost_estimate=cost(6),
        name="increment",
    )(in_vmem(field), in_vmem(coef), *rims)[0]


def decode(rows):
    back = lambda n: pltpu.roll(rows, LEV - n, 1)
    frac_x = back(2) + back(3) + back(4)
    frac_y = back(5) + back(6) + back(7)
    valid = rows > 0.5
    cell = jnp.where(valid, (rows - 1.0) * BY + back(1), 0.0).astype(jnp.int32)
    off = lambda w: jnp.where(valid, w, 0.0)
    return cell, (
        off((1.0 - frac_x) * (1.0 - frac_y)),
        off(frac_x * (1.0 - frac_y)),
        off((1.0 - frac_x) * frac_y),
        off(frac_x * frac_y),
    )


def gather_kernel(
    got, background, increment, reply, slots,
    wide, cells, table, ga, gb, gc, gd, spaced, bgt, inct, packed, came,
):
    part = CELLS // PARTS

    def bring(n, i):
        at = pl.ds(i * part, part)
        source = (background, increment)[n]
        return pltpu.make_async_copy(source.at[at], packed.at[n, at], came.at[n, i])

    for i in range(PARTS):
        bring(0, i).start()
        bring(1, i).start()
    wide[...] = got[...].astype(F32).reshape(DEV * ROWS, LEV)
    cell, weights = decode(wide[pl.ds(CAP, DEV, stride=ROWS), :])
    cells[...] = cell
    pltpu.sync_copy(cells, table)
    for i in range(PARTS):
        for n, wider in ((0, bgt), (1, inct)):
            bring(n, i).wait()

            def widen(j, carry):
                at = pl.ds(pl.multiple_of(i * part + j * BY, BY), BY)
                wider[at, :] = packed[n, at, :].astype(F32)
                return carry

            lax.fori_loop(0, part // BY, widen, 0)
    for k in range(CAP):

        def fetch(step, carry):
            for n in range(8):
                owner = step * 8 + n
                at = table[owner, 8 * k]
                to = pl.ds(2 * (k * DEV + owner), 2)
                ga[to, :] = bgt[pl.ds(at, 2), :]
                gb[to, :] = bgt[pl.ds(at + BY, 2), :]
                gc[to, :] = inct[pl.ds(at, 2), :]
                gd[to, :] = inct[pl.ds(at + BY, 2), :]
            return carry

        lax.fori_loop(0, DEV // 8, fetch, 0)
    spaced[...] = jnp.zeros_like(spaced)
    for k in range(CAP):
        w = [lanes(weight[:, 8 * k : 8 * k + 1]) for weight in weights]
        even = pl.ds(2 * DEV * k, DEV, stride=2)
        odd = pl.ds(2 * DEV * k + 1, DEV, stride=2)
        for n, (one, two) in enumerate(((ga, gb), (gc, gd))):
            mixed = w[0] * one[even, :] + w[1] * two[even, :]
            mixed = mixed + w[2] * one[odd, :]
            mixed = mixed + w[3] * two[odd, :]
            slots[k * DEV : (k + 1) * DEV, n * LEV : (n + 1) * LEV] = mixed.astype(BF16)
            spaced[n, pl.ds(k, DEV, stride=ROWS), :] = mixed
    reply[:, :LEV] = spaced[0].astype(BF16)
    reply[:, LEV:] = spaced[1].astype(BF16)


def gathered(got, bgt, inct):
    rows = pltpu.VMEM((2 * SLOTS, LEV), F32)
    whole = pl.BlockSpec(memory_space=pltpu.VMEM)
    return pl.pallas_call(
        gather_kernel,
        grid=(1,),
        in_specs=[pl.BlockSpec((DEV, ROWS, LEV), lambda i: (0, 0, 0))]
        + [pl.BlockSpec(memory_space=pltpu.HBM)] * 2,
        out_specs=[whole, whole],
        out_shape=[
            jax.ShapeDtypeStruct((DEV * ROWS, 2 * LEV), BF16),
            jax.ShapeDtypeStruct((SLOTS, 2 * LEV), BF16),
        ],
        scratch_shapes=[
            pltpu.VMEM((DEV * ROWS, LEV), F32),
            pltpu.VMEM((DEV, LEV), jnp.int32),
            pltpu.SMEM((DEV, LEV), jnp.int32),
            rows,
            rows,
            rows,
            rows,
            pltpu.VMEM((2, DEV * ROWS, LEV), F32),
            pltpu.VMEM((CELLS, LEV), F32),
            pltpu.VMEM((CELLS, LEV), F32),
            pltpu.VMEM((2, CELLS, LEV), BF16),
            pltpu.SemaphoreType.DMA((2, PARTS)),
        ],
        compiler_params=params(26),
        cost_estimate=cost(5),
        name="gather",
    )(got, in_hbm(bgt), in_hbm(inct))


def tangent(base, delta, w_first, b_first, w_second, b_second):
    h_one = jnp.tanh(nn(base, w_first) + b_first)
    d_one = 1.0 - h_one * h_one
    h_two = jnp.tanh(nn(h_one.astype(BF16), w_second) + b_second)
    d_two = 1.0 - h_two * h_two
    t_one = (d_one * nn(delta, w_first)).astype(BF16)
    t_two = (d_two * nn(t_one, w_second)).astype(BF16)
    return d_one, d_two, t_two


BLOCK = 768


def adjoint_kernel(
    got, slots, w_first, b_first, w_second, b_second, w_third, ivar,
    acc, x_up, x_down, y_up, y_down,
    wide, pulled, profile, cells, table, ca, cb,
):
    for n in range(HID // LEV):
        at = slice(n * LEV, (n + 1) * LEV)
        wide[...] = got[:, :, at].astype(F32).reshape(DEV * ROWS, LEV)
        for k in range(CAP):
            pulled[k * DEV : (k + 1) * DEV, at] = wide[pl.ds(k, DEV, stride=ROWS), :]
        if n == 0:
            cell, weights = decode(wide[pl.ds(CAP, DEV, stride=ROWS), :])
    cells[...] = cell
    pltpu.sync_copy(cells, table)

    def block(i, carry):
        here = pl.ds(pl.multiple_of(i * BLOCK, BLOCK), BLOCK)
        d_one, d_two, t_two = tangent(
            slots[here, :LEV], slots[here, LEV:],
            w_first[...], b_first[...], w_second[...], b_second[...],
        )
        change = nt(t_two, w_third[...]) * ivar[...].reshape(1, CH)
        s_two = (d_two * (nn(change.astype(BF16), w_third[...]) - pulled[here, :])).astype(BF16)
        s_one = (d_one * nt(s_two, w_second[...])).astype(BF16)
        profile[here, :] = nt(s_one, w_first[...])
        return carry

    lax.fori_loop(0, SLOTS // BLOCK, block, 0)
    acc[...] = jnp.zeros_like(acc)
    for k in range(CAP):
        grad = profile[k * DEV : (k + 1) * DEV, :]
        w = [lanes(weight[:, 8 * k : 8 * k + 1]) for weight in weights]
        even = pl.ds(2 * DEV * k, DEV, stride=2)
        odd = pl.ds(2 * DEV * k + 1, DEV, stride=2)
        ca[even, :] = w[0] * grad
        cb[even, :] = w[1] * grad
        ca[odd, :] = w[2] * grad
        cb[odd, :] = w[3] * grad
    for k in range(CAP):

        def add(step, carry):
            for n in range(8):
                owner = step * 8 + n
                at = table[owner, 8 * k]
                there = pl.ds(2 * (k * DEV + owner), 2)
                one = acc[pl.ds(at, 2), :] + ca[there, :]
                two = acc[pl.ds(at + BY, 2), :] + cb[there, :]
                acc[pl.ds(at, 2), :] = one
                acc[pl.ds(at + BY, 2), :] = two
            return carry

        lax.fori_loop(0, DEV // 8, add, 0)
    x_down[...] = acc[: 2 * BY, :].astype(BF16)
    x_up[...] = acc[CELLS - 2 * BY :, :].astype(BF16)
    for n in range(2):
        y_down[n * BX : (n + 1) * BX, :] = acc[pl.ds(n, BX, stride=BY), :].astype(BF16)
        y_up[n * BX : (n + 1) * BX, :] = acc[pl.ds(BY - 2 + n, BX, stride=BY), :].astype(BF16)


def adjoint(got, slots, w_first, b_first, w_second, b_second, w_third, ivar):
    return pl.pallas_call(
        adjoint_kernel,
        out_shape=[
            pltpu.VMEM((CELLS, LEV), F32),
            jax.ShapeDtypeStruct((2 * BY, LEV), BF16),
            jax.ShapeDtypeStruct((2 * BY, LEV), BF16),
            jax.ShapeDtypeStruct((2 * BX, LEV), BF16),
            jax.ShapeDtypeStruct((2 * BX, LEV), BF16),
        ],
        scratch_shapes=[
            pltpu.VMEM((DEV * ROWS, LEV), F32),
            pltpu.VMEM((SLOTS, HID), F32),
            pltpu.VMEM((SLOTS, LEV), F32),
            pltpu.VMEM((DEV, LEV), jnp.int32),
            pltpu.SMEM((DEV, LEV), jnp.int32),
            pltpu.VMEM((2 * SLOTS, LEV), F32),
            pltpu.VMEM((2 * SLOTS, LEV), F32),
        ],
        compiler_params=params(32),
        cost_estimate=cost(10),
        name="adjoint",
    )(got, slots, w_first, b_first, w_second, b_second, w_third, ivar)


def departure_kernel(
    reply, holder, innov, w_first, b_first, w_second, b_second, w_third, ivar, out
):
    held = holder[...]
    pick = (iota((OWN, DEV * ROWS), 1) == down(held * ROWS + ranks(held)).astype(jnp.int32)[:, 0:1]).astype(BF16)
    own = nn(pick, reply[...]).astype(BF16)
    _, _, t_two = tangent(
        own[:, :LEV], own[:, LEV:], w_first[...], b_first[...], w_second[...], b_second[...]
    )
    each = down(ivar[...].reshape(1, CH))
    out[...] = (nt(w_third[...], t_two) - innov[...]) * jnp.concatenate([each, each], axis=1)


def departures_of(reply, holder, innov, w_first, b_first, w_second, b_second, w_third, ivar):
    return pl.pallas_call(
        departure_kernel,
        out_shape=jax.ShapeDtypeStruct((CH, OWN), F32),
        compiler_params=params(12),
        cost_estimate=cost(4),
        name="departures",
    )(reply, holder, innov, w_first, b_first, w_second, b_second, w_third, ivar)


def ready_kernel(
    acc, spread, ax_low, ax_high, ay_low, ay_high, control,
    coef, grown, scaled, held, low, high, field, came,
):
    copies = [
        pltpu.make_async_copy(control.at[:, pl.ds(at, to.shape[1])], to, came.at[n])
        for n, (to, at) in enumerate(((held, CHUNK), (low, 0), (high, BX - CHUNK)))
    ]
    for copy in copies:
        copy.start()
    main_coefficients(coef, spread)
    rim_coefficients(coef, ax_low, ax_high, ay_low, ay_high)
    for x in (1, BX + 2):
        field[x] = jnp.zeros((PY, LEV), F32)
    for y in (7, 8 + BY):
        set_plane(field, 2, y, BX, jnp.zeros((BX, LEV), F32))

    def scale(x, carry):
        at = pl.ds(pl.multiple_of((x - 2) * BY, BY), BY)
        field[x, 8 : 8 + BY, :] = coef[x, 8 : 8 + BY, :] * acc[at, :]
        return carry

    lax.fori_loop(2, PX - 2, scale, 0)

    def sweep_one(x, carry):
        at = pl.ds(pl.multiple_of((x - 2) * BY, BY), BY)
        value = acc[at, :] + laplace(field, x, 8, BY)
        grown[x - 2] = value
        scaled[x, 8 : 8 + BY, :] = coef[x, 8 : 8 + BY, :] * value
        return carry

    lax.fori_loop(2, PX - 2, sweep_one, 0)
    for copy in copies:
        copy.wait()


INNER = BX - 2 * CHUNK


def ready(acc, spread, before, control):
    whole = pl.BlockSpec(memory_space=pltpu.VMEM)
    return pl.pallas_call(
        ready_kernel,
        in_specs=[whole] * 6 + [pl.BlockSpec(memory_space=pltpu.HBM)],
        out_specs=[whole] * 6,
        out_shape=[
            pltpu.VMEM((PX, PY, LEV), F32),
            pltpu.VMEM((BX, BY, LEV), F32),
            pltpu.VMEM((PX, PY, LEV), F32),
            pltpu.VMEM((LEV, INNER, BY), F32),
            pltpu.VMEM((LEV, CHUNK, BY), F32),
            pltpu.VMEM((LEV, CHUNK, BY), F32),
        ],
        scratch_shapes=[pltpu.VMEM((PX, PY, LEV), F32), pltpu.SemaphoreType.DMA((3,))],
        compiler_params=params(8),
        cost_estimate=cost(3),
        name="ready",
    )(in_vmem(acc), spread, *before, in_hbm(control))


def finish_rows(grown, scaled, held, first, count, offset, pair):
    flat = held.reshape(LEV * held.shape[1], BY)
    for i in range(count):
        x = first + i
        value = grown[x] + laplace(scaled, x + 2, 8, BY)
        high, low = split_two(value)
        turned = nt(pair, jnp.concatenate([high, low], axis=1))
        here = pl.ds(offset + i, LEV, stride=held.shape[1])
        flat[here, :] = turned + flat[here, :]


def interior_kernel(
    acc, coef, y_low, y_high, _held, _grown, _scaled, out, held, grown, scaled, went
):
    edge = iota((BX, LEV), 0)
    for rows, near, far, side, inner in (
        (y_low, 1, 0, 7, 8),
        (y_high, 0, 1, 8 + BY, 7 + BY),
    ):
        here = rows[near * BX : (near + 1) * BX, :].astype(F32)
        there = rows[far * BX : (far + 1) * BX, :].astype(F32)
        weight = plane(coef, 2, side, BX)
        mine = weight * here
        over = side + (-1 if side < 8 else 1)
        total = jnp.where(edge == BX - 1, 0.0, pltpu.roll(mine, BX - 1, 0))
        total = total + jnp.where(edge == 0, 0.0, pltpu.roll(mine, 1, 0))
        touching = acc[pl.ds(inner - 8, BX, stride=BY), :]
        inside = plane(coef, 2, inner, BX)
        total = total + inside * touching + plane(coef, 2, over, BX) * there
        set_plane(scaled, 2, side, BX, weight * (here + (total - 4.0 * mine)))
        flat = grown.reshape(CELLS, LEV)
        at = pl.ds(inner - 8, BX, stride=BY)
        fixed = flat[at, :] + mine
        flat[at, :] = fixed
        set_plane(scaled, 2, inner, BX, inside * fixed)
    pair = eye_pair()

    def leave(part):
        return pltpu.make_async_copy(
            held.at[:, pl.ds(part * TALL, TALL)],
            out.at[:, pl.ds(CHUNK + part * TALL, TALL)],
            went.at[part],
        )

    for part in range(INNER // TALL):
        first = part * TALL

        def some(step, carry):
            flat = held.reshape(LEV * INNER, BY)
            for i in range(4):
                at = first + step * 4 + i
                value = grown[CHUNK + at] + laplace(scaled, CHUNK + at + 2, 8, BY)
                high, low = split_two(value)
                turned = nt(pair, jnp.concatenate([high, low], axis=1))
                here = pl.ds(at, LEV, stride=INNER)
                flat[here, :] = turned + flat[here, :]
            return carry

        lax.fori_loop(0, TALL // 4, some, 0)
        leave(part).start()
    for part in range(INNER // TALL):
        leave(part).wait()


def interior(acc, coef, rims, held, grown, scaled):
    whole = pl.BlockSpec(memory_space=pltpu.VMEM)
    hbm = pl.BlockSpec(memory_space=pltpu.HBM)
    return pl.pallas_call(
        interior_kernel,
        in_specs=[whole] * 7,
        out_specs=[hbm] + [whole] * 3,
        out_shape=[
            pltpu.HBM((LEV, BX, BY), F32),
            pltpu.VMEM((LEV, INNER, BY), F32),
            pltpu.VMEM((BX, BY, LEV), F32),
            pltpu.VMEM((PX, PY, LEV), F32),
        ],
        input_output_aliases={4: 1, 5: 2, 6: 3},
        scratch_shapes=[pltpu.SemaphoreType.DMA((INNER // TALL,))],
        compiler_params=params(4),
        cost_estimate=cost(5),
        name="interior",
    )(in_vmem(acc), in_vmem(coef), *rims, in_vmem(held), in_vmem(grown), in_vmem(scaled))


def edges_kernel(
    acc, coef, x_low, x_high, _out, _grown, _scaled, _low, _high,
    out, grown, scaled, low, high, line, went,
):
    held = (low, high)

    def leave(n):
        at = pl.ds(n * (BX - CHUNK), CHUNK)
        return pltpu.make_async_copy(held[n], out.at[:, at], went.at[n])

    main = pl.ds(8, BY)
    for rows, near, side, inner in ((x_low, 1, 1, 2), (x_high, 0, BX + 2, BX + 1)):
        here = rows[near * BY : (near + 1) * BY, :].astype(F32)
        there = rows[(1 - near) * BY : (2 - near) * BY, :].astype(F32)
        pair = rows[2 * BY : 2 * BY + 16, :].astype(F32)
        weight = coef[side, main, :]
        mine = weight * here
        line[main, :] = mine
        for n, y in enumerate((7, 8 + BY)):
            corner = coef[side, y : y + 1, :] * pair[n : n + 1]
            line[y : y + 1, :] = corner
            scaled[inner, y : y + 1, :] = (
                scaled[inner, y : y + 1, :] + coef[inner, y : y + 1, :] * corner
            )
        inside = coef[inner, main, :]
        total = inside * acc[(inner - 2) * BY : (inner - 1) * BY, :]
        total = total + coef[side + (-1 if side < 8 else 1), main, :] * there
        total = total + line[9 : 9 + BY, :] + line[7 : 7 + BY, :]
        scaled[side, main, :] = weight * (here + (total - 4.0 * mine))
        fixed = grown[inner - 2] + mine
        grown[inner - 2] = fixed
        scaled[inner, main, :] = inside * fixed
    pair = eye_pair()
    for n in range(2):
        finish_rows(grown, scaled, held[n], n * (BX - CHUNK), CHUNK, 0, pair)
        leave(n).start()
    for n in range(2):
        leave(n).wait()


def edges(acc, coef, rims, so_far, grown, scaled, low, high):
    whole = pl.BlockSpec(memory_space=pltpu.VMEM)
    hbm = pl.BlockSpec(memory_space=pltpu.HBM)
    return pl.pallas_call(
        edges_kernel,
        in_specs=[whole] * 4 + [hbm] + [whole] * 4,
        out_specs=[hbm] + [whole] * 4,
        out_shape=[
            pltpu.HBM((LEV, BX, BY), F32),
            pltpu.VMEM((BX, BY, LEV), F32),
            pltpu.VMEM((PX, PY, LEV), F32),
            pltpu.VMEM((LEV, CHUNK, BY), F32),
            pltpu.VMEM((LEV, CHUNK, BY), F32),
        ],
        input_output_aliases={4: 0, 5: 1, 6: 2, 7: 3, 8: 4},
        scratch_shapes=[pltpu.VMEM((PY, LEV), F32), pltpu.SemaphoreType.DMA((2,))],
        compiler_params=params(4),
        cost_estimate=cost(2),
        name="edges",
    )(
        in_vmem(acc), in_vmem(coef), *rims, in_hbm(so_far),
        in_vmem(grown), in_vmem(scaled), in_vmem(low), in_vmem(high),
    )[0]


def exchange(array):
    return lax.all_to_all(array, ("tile", "obs"), split_axis=0, concat_axis=0, tiled=True)


def per_device(
    control,
    background,
    spread,
    obs_holder,
    obs_anchor,
    obs_frac,
    innovation,
    inverse_var,
    w_first,
    b_first,
    w_second,
    b_second,
    w_third,
):
    b_one = b_first.reshape(1, HID)
    b_two = b_second.reshape(1, HID)
    holder = obs_holder.reshape(1, OWN)
    innov = innovation.T
    w_last = w_third.T
    asked = requests(holder, obs_anchor.reshape(1, OWN), obs_frac, innov, inverse_var, w_last)
    got = exchange(asked.reshape(DEV, ROWS, HID))
    field, bgt, x_up, x_down, y_up, y_down = to_columns(control, background, spread)
    ay_low, ay_high = shift(y_up, "obs", 1), shift(y_down, "obs", -1)
    wide = over_lanes(spread)
    x_up, x_down = compose(x_up, x_down, ay_low, ay_high)
    ax_low, ax_high = shift(x_up, "tile", 1), shift(x_down, "tile", -1)
    before = (ax_low, ax_high, ay_low, ay_high)
    inct = increments(field, wide, before)
    reply, slots = gathered(got, bgt.reshape(CELLS, LEV), inct.reshape(CELLS, LEV))
    reply = exchange(reply.reshape(DEV, ROWS, 2 * LEV))
    acc, x_up, x_down, y_up, y_down = adjoint(
        got, slots, w_first, b_one, w_second, b_two, w_last, inverse_var
    )
    y_low, y_high = shift(y_up, "obs", 1), shift(y_down, "obs", -1)
    coef, grown, scaled, *held = ready(acc, spread, before, control)
    x_up, x_down = compose(x_up, x_down, y_low, y_high)
    x_low, x_high = shift(x_up, "tile", 1), shift(x_down, "tile", -1)
    gradient, _, grown, scaled = interior(acc, coef, (y_low, y_high), held[0], grown, scaled)
    gradient = edges(
        acc, coef, (x_low, x_high), gradient, grown, scaled, held[1], held[2]
    )
    departures = departures_of(
        reply.reshape(DEV * ROWS, 2 * LEV), holder, innov,
        w_first, b_one, w_second, b_two, w_last, inverse_var,
    ).T
    return departures, gradient


def solution(mesh):
    return jax.shard_map(
        per_device,
        mesh=mesh,
        in_specs=(
            P(None, "tile", "obs"),
            P(None, "tile", "obs"),
            P("tile", "obs"),
            P(("tile", "obs"), None),
            P(("tile", "obs")),
            P(None, ("tile", "obs")),
            P(("tile", "obs"), None),
            P(),
            P(),
            P(),
            P(),
            P(),
            P(),
        ),
        out_specs=(P(("tile", "obs"), None), P(None, "tile", "obs")),
        check_vma=False,
    )
```

```python
import jax
import jax.numpy as jnp
from jax import lax
from jax.experimental import pallas as pl
from jax.experimental.pallas import tpu as pltpu
from jax.sharding import PartitionSpec as P


F32 = jnp.float32
BF16 = jnp.bfloat16
LEV = 128
BX = 64
BY = 128
CELLS = BX * BY
OWN = 256
DEV = 128
CAP = 6
ROWS = 8
SLOTS = CAP * DEV
HID = 512
CH = 616
PX = BX + 4
PY = BY + 16
CHUNK = 8
TALL = 16


def params(mib, **extra):
    return pltpu.CompilerParams(vmem_limit_bytes=mib * 1024 * 1024, **extra)


def cost(us):
    return pl.CostEstimate(flops=int(us * 1.0e9), bytes_accessed=0, transcendentals=0)


def tn(a, b):
    return lax.dot_general(a, b, (((0,), (0,)), ((), ())), preferred_element_type=F32)


def down(row):
    return jnp.transpose(jnp.broadcast_to(row, (LEV, row.shape[1])))


def in_vmem(array):
    return pltpu.with_memory_space_constraint(array, pltpu.VMEM)


def in_hbm(array):
    return pltpu.with_memory_space_constraint(array, pltpu.HBM)


def nn(a, b):
    return jnp.dot(a, b, preferred_element_type=F32)


def nt(a, b):
    return lax.dot_general(a, b, (((1,), (1,)), ((), ())), preferred_element_type=F32)


def iota(shape, dim):
    return lax.broadcasted_iota(jnp.int32, shape, dim)


def split_two(a):
    high = a.astype(BF16)
    return high, (a - high.astype(F32)).astype(BF16)


def eye():
    return (iota((LEV, LEV), 0) == iota((LEV, LEV), 1)).astype(BF16)


def ranks(held):
    marks = (iota((DEV, OWN), 0) == held).astype(BF16)
    before = (iota((OWN, OWN), 0) < iota((OWN, OWN), 1)).astype(BF16)
    return jnp.sum(marks.astype(F32) * nn(marks, before), axis=0, keepdims=True).astype(jnp.int32)


def request_kernel(holder, anchor, frac, ivar, innov, w_third, out):
    held = holder[...]
    rank = ranks(held)
    at = anchor[...].astype(F32)
    x = jnp.floor((at + 0.5) * (1.0 / (BY - 1)))
    y = at - (BY - 1) * x
    fields = [x + 1.0, y]
    for dim in range(2):
        value = frac[dim : dim + 1, :]
        for _ in range(3):
            piece = value.astype(BF16).astype(F32)
            fields.append(piece)
            value = value - piece
    fields = jnp.concatenate(fields, axis=0)
    fields = jnp.concatenate([fields] * (LEV // 8), axis=0)
    fields = jnp.where((iota((LEV, OWN), 0) >> 3) == rank, fields, 0.0).astype(BF16)
    each = down(ivar[...].reshape(1, CH))
    row = iota((DEV * ROWS, OWN), 0)
    to_slot = (row == held * ROWS + rank).astype(BF16)
    to_fields = (row == held * ROWS + CAP).astype(BF16)
    scaled = (innov[...] * jnp.concatenate([each, each], axis=1)).astype(BF16)
    pulled = tn(scaled, w_third[...]).astype(BF16)
    out[:, :LEV] = (nn(to_slot, pulled[:, :LEV]) + nt(to_fields, fields)).astype(BF16)
    out[:, LEV:] = nn(to_slot, pulled[:, LEV:]).astype(BF16)


def requests(holder, anchor, frac, innov, ivar, w_third):
    return pl.pallas_call(
        request_kernel,
        out_shape=jax.ShapeDtypeStruct((DEV * ROWS, HID), BF16),
        compiler_params=params(12),
        cost_estimate=cost(4),
        name="requests",
    )(*map(in_hbm, (holder, anchor, frac, ivar, innov, w_third)))


def columns_kernel(
    control, background, spread, field, bgt, x_up, x_down, y_up, y_down,
    held, back_held, wide, turned_back, planes, came, back_came, went,
):
    tall = BX // TALL

    def bring(part):
        at = pl.ds(part * TALL, TALL)
        return pltpu.make_async_copy(control.at[:, at], held.at[part], came.at[part])

    def leave(part):
        at = pl.ds(part * TALL, TALL)
        return pltpu.make_async_copy(turned_back.at[at], bgt.at[at], went.at[part])

    fetch = pltpu.make_async_copy(background, back_held, back_came)
    bring(0).start()
    fetch.start()
    for part in range(1, tall):
        bring(part).start()
    unit = eye()
    fetch.wait()

    def turn(part, carry):
        first = pl.multiple_of(part * TALL, TALL)
        wide[...] = back_held[:, pl.ds(first, TALL), :].astype(F32).reshape(LEV * TALL, BY)
        bring(part).wait()
        flat = held.at[part].reshape(LEV * TALL, BY)
        for i in range(TALL):
            here = pl.ds(i, LEV, stride=TALL)
            turned = jnp.transpose(flat[here, :])
            field[first + i + 2, 8 : 8 + BY, :] = turned
            back = wide[here, :].astype(BF16)
            turned_back[first + i] = nt(unit, back).astype(BF16)
            for n, y in enumerate((0, 1, BY - 2, BY - 1)):
                planes[n, pl.ds(first + i, 1), :] = turned[y : y + 1, :LEV]
        leave(part).start()
        return carry

    lax.fori_loop(0, tall, turn, 0)
    x_down[:BY, :] = field[2, 8 : 8 + BY, :].astype(BF16)
    x_down[BY : 2 * BY, :] = field[3, 8 : 8 + BY, :].astype(BF16)
    x_up[:BY, :] = field[BX, 8 : 8 + BY, :].astype(BF16)
    x_up[BY : 2 * BY, :] = field[BX + 1, 8 : 8 + BY, :].astype(BF16)
    s = spread[...]
    turned = jnp.transpose(jnp.concatenate([s, s], axis=0))

    def rows(two):
        high, low = split_two(two)
        zero = jnp.zeros((12, BY), F32)
        return jnp.concatenate([high.astype(F32), low.astype(F32), zero], axis=0).astype(BF16)

    x_down[2 * BY :, :] = rows(s[0:2, :])
    x_up[2 * BY :, :] = rows(s[BX - 2 : BX, :])
    y_down[: 2 * BX, :] = planes[0:2].reshape(2 * BX, LEV).astype(BF16)
    y_up[: 2 * BX, :] = planes[2:4].reshape(2 * BX, LEV).astype(BF16)
    y_down[2 * BX :, :] = rows(turned[0:2, :])
    y_up[2 * BX :, :] = rows(turned[BY - 2 : BY, :])
    for part in range(tall):
        leave(part).wait()


def to_columns(control, background, spread):
    hbm = pl.BlockSpec(memory_space=pltpu.HBM)
    whole = pl.BlockSpec(memory_space=pltpu.VMEM)
    return pl.pallas_call(
        columns_kernel,
        in_specs=[hbm, hbm, whole],
        out_specs=[whole, hbm] + [whole] * 4,
        out_shape=[
            pltpu.VMEM((PX, PY, LEV), F32),
            pltpu.HBM((BX, BY, LEV), BF16),
            jax.ShapeDtypeStruct((2 * BY + 16, LEV), BF16),
            jax.ShapeDtypeStruct((2 * BY + 16, LEV), BF16),
            jax.ShapeDtypeStruct((2 * BX + 16, LEV), BF16),
            jax.ShapeDtypeStruct((2 * BX + 16, LEV), BF16),
        ],
        scratch_shapes=[
            pltpu.VMEM((BX // TALL, LEV, TALL, BY), F32),
            pltpu.VMEM((LEV, BX, BY), BF16),
            pltpu.VMEM((LEV * TALL, BY), F32),
            pltpu.VMEM((BX, BY, LEV), BF16),
            pltpu.VMEM((4, BX, LEV), F32),
            pltpu.SemaphoreType.DMA((BX // TALL,)),
            pltpu.SemaphoreType.DMA,
            pltpu.SemaphoreType.DMA((BX // TALL,)),
        ],
        compiler_params=params(16),
        cost_estimate=cost(6),
        name="columns",
    )(in_hbm(control), in_hbm(background), spread)


def shift(array, axis, by):
    count = lax.axis_size(axis)
    return lax.ppermute(array, axis, [(i, (i + by) % count) for i in range(count)])


def compose_kernel(x_up, x_down, y_low, y_high, up, down):
    rows = x_up.shape[0]
    up[:rows, :] = x_up[...]
    down[:rows, :] = x_down[...]
    low = y_low[...].astype(F32)
    high = y_high[...].astype(F32)
    fields = [low[2 * BX :], high[2 * BX :]] if low.shape[0] > 2 * BX else []
    for out, row in ((up, BX - 1), (down, 0)):
        pair = [low[BX + row : BX + row + 1], high[row : row + 1], jnp.zeros((14, LEV), F32)]
        out[rows:, :] = jnp.concatenate(pair + fields, axis=0).astype(BF16)


def compose(x_up, x_down, y_low, y_high):
    rows = x_up.shape[0] + 16 + 2 * (y_low.shape[0] - 2 * BX)
    return pl.pallas_call(
        compose_kernel,
        out_shape=[jax.ShapeDtypeStruct((rows, LEV), BF16)] * 2,
        compiler_params=params(2),
        name="compose",
    )(x_up, x_down, y_low, y_high)


def laplace(field, x, first, count):
    total = field[x + 1, pl.ds(first, count), :] + field[x - 1, pl.ds(first, count), :]
    total = total + field[x, pl.ds(first + 1, count), :]
    total = total + field[x, pl.ds(first - 1, count), :]
    return total - 4.0 * field[x, pl.ds(first, count), :]


def plane(field, x, y, count):
    flat = field.reshape(PX * PY, LEV)
    return flat[pl.ds(x * PY + y, count, stride=PY), :]


def set_plane(field, x, y, count, value):
    flat = field.reshape(PX * PY, LEV)
    flat[pl.ds(x * PY + y, count, stride=PY), :] = value


def plane_laplace(field, y):
    total = plane(field, 3, y, BX) + plane(field, 1, y, BX)
    total = total + plane(field, 2, y + 1, BX) + plane(field, 2, y - 1, BX)
    return total - 4.0 * plane(field, 2, y, BX)


def lanes(column):
    return jnp.broadcast_to(column, (column.shape[0], LEV))


def joined(rows, at):
    block = rows[at : at + 16, :].astype(F32)
    return block[0:2] + block[2:4]


def fill_y(field, y_low, y_high):
    for n in range(2):
        set_plane(field, 2, 6 + n, BX, y_low[n * BX : (n + 1) * BX, :].astype(F32))
        set_plane(field, 2, 8 + BY + n, BX, y_high[n * BX : (n + 1) * BX, :].astype(F32))


def fill_x(field, x_low, x_high, at):
    for n in range(2):
        field[n, 8 : 8 + BY, :] = x_low[n * BY : (n + 1) * BY, :].astype(F32)
        field[BX + 2 + n, 8 : 8 + BY, :] = x_high[n * BY : (n + 1) * BY, :].astype(F32)
    for rows, x in ((x_low, 1), (x_high, BX + 2)):
        pair = rows[at : at + 16, :].astype(F32)
        field[x, 7:8, :] = pair[0:1]
        field[x, 8 + BY : 9 + BY, :] = pair[1:2]


def main_coefficients(coef, spread):
    square = jnp.concatenate([spread[...], jnp.zeros((BY - BX, BY), F32)], axis=0)
    turned = jnp.transpose(square)
    for x in range(BX):
        coef[x + 2, 8 : 8 + BY, :] = lanes(turned[:, x : x + 1])


def rim_coefficients(coef, x_low, x_high, y_low, y_high):
    ends = jnp.concatenate(
        [joined(x_low, 2 * BY), joined(x_high, 2 * BY), jnp.zeros((BY - 4, BY), F32)], axis=0
    )
    ends = jnp.transpose(ends)
    for n, x in enumerate((0, 1, BX + 2, BX + 3)):
        coef[x, 8 : 8 + BY, :] = lanes(ends[:, n : n + 1])
    sides = jnp.concatenate(
        [joined(y_low, 2 * BX), joined(y_high, 2 * BX), jnp.zeros((BY - 4, BY), F32)], axis=0
    )
    sides = jnp.transpose(sides)[:BX, :]
    for n in range(2):
        set_plane(coef, 2, 6 + n, BX, lanes(sides[:, n : n + 1]))
        set_plane(coef, 2, 8 + BY + n, BX, lanes(sides[:, 2 + n : 3 + n]))
    for block, x, lane in ((x_low, 1, BX - 1), (x_high, BX + 2, 0)):
        left = joined(block, 2 * BY + 32)
        right = joined(block, 2 * BY + 48)
        coef[x, 7:8, :] = lanes(left[1:2, lane : lane + 1])
        coef[x, 8 + BY : 9 + BY, :] = lanes(right[0:1, lane : lane + 1])


def sweep(to, field, coef, x):
    middle = field[x, 8 : 8 + BY, :]
    to[x, 8 : 8 + BY, :] = middle + coef[x, 8 : 8 + BY, :] * laplace(field, x, 8, BY)


def early_kernel(spread, field, coef, first):
    main_coefficients(coef, spread)

    def one(x, carry):
        sweep(first, field, coef, x)
        return carry

    lax.fori_loop(3, PX - 3, one, 0)


def early(spread, field):
    return pl.pallas_call(
        early_kernel,
        out_shape=[pltpu.VMEM((PX, PY, LEV), F32), pltpu.VMEM((PX, PY, LEV), F32)],
        compiler_params=params(2),
        cost_estimate=cost(2),
        name="early",
    )(spread, in_vmem(field))


def joined(rows, at):
    block = rows[at : at + 16, :].astype(F32)
    return block[0:2] + block[2:4]


PARTS = BX // CHUNK


def increment_kernel(
    _field, _coef, _first, x_low, x_high, y_low, y_high,
    inc, kept, field, coef, first, done, went, kept_went,
):
    def leave(part):
        at = pl.ds(part * CHUNK, CHUNK)
        return pltpu.make_async_copy(done.at[at], inc.at[at], went.at[part])

    rim_coefficients(coef, x_low, x_high, y_low, y_high)
    keep = pltpu.make_async_copy(coef, kept, kept_went)
    keep.start()
    fill_x(field, x_low, x_high, 2 * BY + 16)
    fill_y(field, y_low, y_high)

    for x in (1, 2, BX + 1, BX + 2):
        sweep(first, field, coef, x)
    for y in (7, 8, 7 + BY, 8 + BY):
        moved = plane(field, 2, y, BX) + plane(coef, 2, y, BX) * plane_laplace(field, y)
        set_plane(first, 2, y, BX, moved)

    def sweep_two(x, carry):
        middle = first[x, 8 : 8 + BY, :]
        result = middle + coef[x, 8 : 8 + BY, :] * laplace(first, x, 8, BY)
        done[x - 2] = result.astype(BF16)
        return carry

    for part in range(PARTS):
        lax.fori_loop(2 + CHUNK * part, 2 + CHUNK * (part + 1), sweep_two, 0)
        leave(part).start()
    for part in range(PARTS):
        leave(part).wait()
    keep.wait()


def increments(field, coef, first, rims):
    whole = pl.BlockSpec(memory_space=pltpu.VMEM)
    padded = pltpu.VMEM((PX, PY, LEV), F32)
    return pl.pallas_call(
        increment_kernel,
        in_specs=[whole] * 7,
        out_specs=[pl.BlockSpec(memory_space=pltpu.HBM)] * 2 + [whole] * 3,
        out_shape=[
            pltpu.HBM((BX, BY, LEV), BF16),
            pltpu.HBM((PX, PY, LEV), F32),
            padded,
            padded,
            padded,
        ],
        input_output_aliases={0: 2, 1: 3, 2: 4},
        scratch_shapes=[
            pltpu.VMEM((BX, BY, LEV), BF16),
            pltpu.SemaphoreType.DMA((PARTS,)),
            pltpu.SemaphoreType.DMA,
        ],
        compiler_params=params(8),
        cost_estimate=cost(6),
        name="increment",
    )(in_vmem(field), in_vmem(coef), in_vmem(first), *rims)[:2]


def decode(rows):
    back = lambda n: pltpu.roll(rows, LEV - n, 1)
    frac_x = back(2) + back(3) + back(4)
    frac_y = back(5) + back(6) + back(7)
    valid = rows > 0.5
    cell = jnp.where(valid, ((rows - 1.0) * BY + back(1)).astype(jnp.int32), 2 * iota(rows.shape, 0))
    off = lambda w: jnp.where(valid, w, 0.0)
    return cell, (
        off((1.0 - frac_x) * (1.0 - frac_y)),
        off(frac_x * (1.0 - frac_y)),
        off((1.0 - frac_x) * frac_y),
        off(frac_x * frac_y),
    )


def gather_kernel(
    got, background, increment, reply, slots,
    wide, cells, table, ga, gb, spaced, both, packed, came,
):
    part = CELLS // PARTS

    def bring(n, i):
        at = pl.ds(i * part, part)
        source = (background, increment)[n]
        return pltpu.make_async_copy(source.at[at], packed.at[n, at], came.at[n, i])

    for i in range(PARTS):
        bring(0, i).start()
        bring(1, i).start()
    wide[...] = got[...].astype(F32).reshape(DEV * ROWS, LEV)
    cell, weights = decode(wide[pl.ds(CAP, DEV, stride=ROWS), :])
    cells[...] = cell
    pltpu.sync_copy(cells, table)
    for i in range(PARTS):
        for n in range(2):
            bring(n, i).wait()

            def widen(j, carry):
                first = pl.multiple_of(i * part + j * BY, BY)
                both[pl.ds(2 * first + n, BY, stride=2), :] = packed[n, pl.ds(first, BY), :].astype(F32)
                return carry

            lax.fori_loop(0, part // BY, widen, 0)
    for k in range(CAP):

        def fetch(step, carry):
            for n in range(8):
                owner = step * 8 + n
                at = table[owner, 8 * k]
                to = pl.ds(4 * (k * DEV + owner), 4)
                ga[to, :] = both[pl.ds(2 * at, 4), :]
                gb[to, :] = both[pl.ds(2 * (at + BY), 4), :]
            return carry

        lax.fori_loop(0, DEV // 8, fetch, 0)
    spaced[...] = jnp.zeros_like(spaced)
    for k in range(CAP):
        w = [lanes(weight[:, 8 * k : 8 * k + 1]) for weight in weights]
        for n in range(2):
            here = pl.ds(4 * DEV * k + n, DEV, stride=4)
            next_to = pl.ds(4 * DEV * k + 2 + n, DEV, stride=4)
            mixed = w[0] * ga[here, :] + w[1] * gb[here, :]
            mixed = mixed + w[2] * ga[next_to, :]
            mixed = mixed + w[3] * gb[next_to, :]
            slots[k * DEV : (k + 1) * DEV, n * LEV : (n + 1) * LEV] = mixed.astype(BF16)
            spaced[n, pl.ds(k, DEV, stride=ROWS), :] = mixed
    reply[:, :LEV] = spaced[0].astype(BF16)
    reply[:, LEV:] = spaced[1].astype(BF16)


def gathered(got, bgt, inct):
    rows = pltpu.VMEM((4 * SLOTS, LEV), F32)
    whole = pl.BlockSpec(memory_space=pltpu.VMEM)
    return pl.pallas_call(
        gather_kernel,
        grid=(1,),
        in_specs=[pl.BlockSpec((DEV, ROWS, LEV), lambda i: (0, 0, 0))]
        + [pl.BlockSpec(memory_space=pltpu.HBM)] * 2,
        out_specs=[whole, whole],
        out_shape=[
            jax.ShapeDtypeStruct((DEV * ROWS, 2 * LEV), BF16),
            jax.ShapeDtypeStruct((SLOTS, 2 * LEV), BF16),
        ],
        scratch_shapes=[
            pltpu.VMEM((DEV * ROWS, LEV), F32),
            pltpu.VMEM((DEV, LEV), jnp.int32),
            pltpu.SMEM((DEV, LEV), jnp.int32),
            rows,
            rows,
            pltpu.VMEM((2, DEV * ROWS, LEV), F32),
            pltpu.VMEM((2 * CELLS, LEV), F32),
            pltpu.VMEM((2, CELLS, LEV), BF16),
            pltpu.SemaphoreType.DMA((2, PARTS)),
        ],
        compiler_params=params(26),
        cost_estimate=cost(5),
        name="gather",
    )(got, in_hbm(bgt), in_hbm(inct))


def tangent(base, delta, w_first, b_first, w_second, b_second):
    h_one = jnp.tanh(nn(base, w_first) + b_first)
    d_one = 1.0 - h_one * h_one
    h_two = jnp.tanh(nn(h_one.astype(BF16), w_second) + b_second)
    d_two = 1.0 - h_two * h_two
    t_one = (d_one * nn(delta, w_first)).astype(BF16)
    t_two = (d_two * nn(t_one, w_second)).astype(BF16)
    return d_one, d_two, t_two


BLOCK = 768


def adjoint_kernel(
    got, slots, w_first, b_first, w_second, b_second, w_third, ivar, kept, control,
    acc, x_up, x_down, y_up, y_down, coef, held, low, high,
    wide, pulled, profile, cells, table, ca, cb, came,
):
    copies = [pltpu.make_async_copy(kept, coef, came.at[3])] + [
        pltpu.make_async_copy(control.at[:, pl.ds(at, to.shape[1])], to, came.at[n])
        for n, (to, at) in enumerate(((held, CHUNK), (low, 0), (high, BX - CHUNK)))
    ]
    for copy in copies:
        copy.start()
    for n in range(HID // LEV):
        at = slice(n * LEV, (n + 1) * LEV)
        wide[...] = got[:, :, at].astype(F32).reshape(DEV * ROWS, LEV)
        for k in range(CAP):
            pulled[k * DEV : (k + 1) * DEV, at] = wide[pl.ds(k, DEV, stride=ROWS), :]
        if n == 0:
            cell, weights = decode(wide[pl.ds(CAP, DEV, stride=ROWS), :])
    cells[...] = cell
    pltpu.sync_copy(cells, table)

    def block(i, carry):
        here = pl.ds(pl.multiple_of(i * BLOCK, BLOCK), BLOCK)
        d_one, d_two, t_two = tangent(
            slots[here, :LEV], slots[here, LEV:],
            w_first[...], b_first[...], w_second[...], b_second[...],
        )
        change = nt(t_two, w_third[...]) * ivar[...].reshape(1, CH)
        s_two = (d_two * (nn(change.astype(BF16), w_third[...]) - pulled[here, :])).astype(BF16)
        s_one = (d_one * nt(s_two, w_second[...])).astype(BF16)
        profile[here, :] = nt(s_one, w_first[...])
        return carry

    lax.fori_loop(0, SLOTS // BLOCK, block, 0)
    acc[...] = jnp.zeros_like(acc)
    for k in range(CAP):
        grad = profile[k * DEV : (k + 1) * DEV, :]
        w = [lanes(weight[:, 8 * k : 8 * k + 1]) for weight in weights]
        even = pl.ds(2 * DEV * k, DEV, stride=2)
        odd = pl.ds(2 * DEV * k + 1, DEV, stride=2)
        ca[even, :] = w[0] * grad
        cb[even, :] = w[1] * grad
        ca[odd, :] = w[2] * grad
        cb[odd, :] = w[3] * grad
    for k in range(CAP):

        def add(step, carry):
            for n in range(8):
                owner = step * 8 + n
                at = table[owner, 8 * k]
                there = pl.ds(2 * (k * DEV + owner), 2)
                one = acc[pl.ds(at, 2), :] + ca[there, :]
                two = acc[pl.ds(at + BY, 2), :] + cb[there, :]
                acc[pl.ds(at, 2), :] = one
                acc[pl.ds(at + BY, 2), :] = two
            return carry

        lax.fori_loop(0, DEV // 8, add, 0)
    x_down[...] = acc[: 2 * BY, :].astype(BF16)
    x_up[...] = acc[CELLS - 2 * BY :, :].astype(BF16)
    for n in range(2):
        y_down[n * BX : (n + 1) * BX, :] = acc[pl.ds(n, BX, stride=BY), :].astype(BF16)
        y_up[n * BX : (n + 1) * BX, :] = acc[pl.ds(BY - 2 + n, BX, stride=BY), :].astype(BF16)
    for copy in copies:
        copy.wait()


INNER = BX - 2 * CHUNK


def adjoint(got, slots, w_first, b_first, w_second, b_second, w_third, ivar, kept, control):
    whole = pl.BlockSpec(memory_space=pltpu.VMEM)
    return pl.pallas_call(
        adjoint_kernel,
        in_specs=[whole] * 8 + [pl.BlockSpec(memory_space=pltpu.HBM)] * 2,
        out_specs=[whole] * 9,
        out_shape=[
            pltpu.VMEM((CELLS, LEV), F32),
            jax.ShapeDtypeStruct((2 * BY, LEV), BF16),
            jax.ShapeDtypeStruct((2 * BY, LEV), BF16),
            jax.ShapeDtypeStruct((2 * BX, LEV), BF16),
            jax.ShapeDtypeStruct((2 * BX, LEV), BF16),
            pltpu.VMEM((PX, PY, LEV), F32),
            pltpu.VMEM((LEV, INNER, BY), F32),
            pltpu.VMEM((LEV, CHUNK, BY), F32),
            pltpu.VMEM((LEV, CHUNK, BY), F32),
        ],
        scratch_shapes=[
            pltpu.VMEM((DEV * ROWS, LEV), F32),
            pltpu.VMEM((SLOTS, HID), F32),
            pltpu.VMEM((SLOTS, LEV), F32),
            pltpu.VMEM((DEV, LEV), jnp.int32),
            pltpu.SMEM((DEV, LEV), jnp.int32),
            pltpu.VMEM((2 * SLOTS, LEV), F32),
            pltpu.VMEM((2 * SLOTS, LEV), F32),
            pltpu.SemaphoreType.DMA((4,)),
        ],
        compiler_params=params(32),
        cost_estimate=cost(10),
        name="adjoint",
    )(
        got, slots, w_first, b_first, w_second, b_second, w_third, ivar,
        in_hbm(kept), in_hbm(control),
    )


def departure_kernel(
    reply, holder, innov, w_first, b_first, w_second, b_second, w_third, ivar, out
):
    held = holder[...]
    pick = (iota((OWN, DEV * ROWS), 1) == down(held * ROWS + ranks(held)).astype(jnp.int32)[:, 0:1]).astype(BF16)
    own = nn(pick, reply[...]).astype(BF16)
    _, _, t_two = tangent(
        own[:, :LEV], own[:, LEV:], w_first[...], b_first[...], w_second[...], b_second[...]
    )
    each = down(ivar[...].reshape(1, CH))
    out[...] = (nt(w_third[...], t_two) - innov[...]) * jnp.concatenate([each, each], axis=1)


def departures_of(reply, holder, innov, w_first, b_first, w_second, b_second, w_third, ivar):
    return pl.pallas_call(
        departure_kernel,
        out_shape=jax.ShapeDtypeStruct((CH, OWN), F32),
        compiler_params=params(12),
        cost_estimate=cost(4),
        name="departures",
    )(reply, holder, innov, w_first, b_first, w_second, b_second, w_third, ivar)


def ready_kernel(acc, coef, grown, scaled, field):
    for x in (1, BX + 2):
        field[x] = jnp.zeros((PY, LEV), F32)
    for y in (7, 8 + BY):
        set_plane(field, 2, y, BX, jnp.zeros((BX, LEV), F32))

    def scale(x, carry):
        at = pl.ds(pl.multiple_of((x - 2) * BY, BY), BY)
        field[x, 8 : 8 + BY, :] = coef[x, 8 : 8 + BY, :] * acc[at, :]
        return carry

    lax.fori_loop(2, PX - 2, scale, 0)

    def sweep_one(x, carry):
        at = pl.ds(pl.multiple_of((x - 2) * BY, BY), BY)
        value = acc[at, :] + laplace(field, x, 8, BY)
        grown[x - 2] = value
        scaled[x, 8 : 8 + BY, :] = coef[x, 8 : 8 + BY, :] * value
        return carry

    lax.fori_loop(2, PX - 2, sweep_one, 0)


def ready(acc, coef):
    return pl.pallas_call(
        ready_kernel,
        out_shape=[pltpu.VMEM((BX, BY, LEV), F32), pltpu.VMEM((PX, PY, LEV), F32)],
        scratch_shapes=[pltpu.VMEM((PX, PY, LEV), F32)],
        compiler_params=params(8),
        cost_estimate=cost(3),
        name="ready",
    )(in_vmem(acc), in_vmem(coef))


def finish_rows(grown, scaled, held, first, count):
    flat = held.reshape(LEV * held.shape[1], BY)
    for i in range(count):
        x = first + i
        value = grown[x] + laplace(scaled, x + 2, 8, BY)
        here = pl.ds(i, LEV, stride=held.shape[1])
        flat[here, :] = jnp.transpose(value) + flat[here, :]


def interior_kernel(
    acc, coef, y_low, y_high, _held, _grown, _scaled, out, held, grown, scaled, went
):
    edge = iota((BX, LEV), 0)
    for rows, near, far, side, inner in (
        (y_low, 1, 0, 7, 8),
        (y_high, 0, 1, 8 + BY, 7 + BY),
    ):
        here = rows[near * BX : (near + 1) * BX, :].astype(F32)
        there = rows[far * BX : (far + 1) * BX, :].astype(F32)
        weight = plane(coef, 2, side, BX)
        mine = weight * here
        over = side + (-1 if side < 8 else 1)
        total = jnp.where(edge == BX - 1, 0.0, pltpu.roll(mine, BX - 1, 0))
        total = total + jnp.where(edge == 0, 0.0, pltpu.roll(mine, 1, 0))
        touching = acc[pl.ds(inner - 8, BX, stride=BY), :]
        inside = plane(coef, 2, inner, BX)
        total = total + inside * touching + plane(coef, 2, over, BX) * there
        set_plane(scaled, 2, side, BX, weight * (here + (total - 4.0 * mine)))
        flat = grown.reshape(CELLS, LEV)
        at = pl.ds(inner - 8, BX, stride=BY)
        fixed = flat[at, :] + mine
        flat[at, :] = fixed
        set_plane(scaled, 2, inner, BX, inside * fixed)

    def leave(part):
        return pltpu.make_async_copy(
            held.at[:, pl.ds(part * TALL, TALL)],
            out.at[:, pl.ds(CHUNK + part * TALL, TALL)],
            went.at[part],
        )

    for part in range(INNER // TALL):
        first = part * TALL

        def some(step, carry):
            flat = held.reshape(LEV * INNER, BY)
            for i in range(4):
                at = first + step * 4 + i
                value = grown[CHUNK + at] + laplace(scaled, CHUNK + at + 2, 8, BY)
                here = pl.ds(at, LEV, stride=INNER)
                flat[here, :] = jnp.transpose(value) + flat[here, :]
            return carry

        lax.fori_loop(0, TALL // 4, some, 0)
        leave(part).start()
    for part in range(INNER // TALL):
        leave(part).wait()


def interior(acc, coef, rims, held, grown, scaled):
    whole = pl.BlockSpec(memory_space=pltpu.VMEM)
    hbm = pl.BlockSpec(memory_space=pltpu.HBM)
    return pl.pallas_call(
        interior_kernel,
        in_specs=[whole] * 7,
        out_specs=[hbm] + [whole] * 3,
        out_shape=[
            pltpu.HBM((LEV, BX, BY), F32),
            pltpu.VMEM((LEV, INNER, BY), F32),
            pltpu.VMEM((BX, BY, LEV), F32),
            pltpu.VMEM((PX, PY, LEV), F32),
        ],
        input_output_aliases={4: 1, 5: 2, 6: 3},
        scratch_shapes=[pltpu.SemaphoreType.DMA((INNER // TALL,))],
        compiler_params=params(4),
        cost_estimate=cost(5),
        name="interior",
    )(in_vmem(acc), in_vmem(coef), *rims, in_vmem(held), in_vmem(grown), in_vmem(scaled))


def edges_kernel(
    acc, coef, x_low, x_high, _out, _grown, _scaled, _low, _high,
    out, grown, scaled, low, high, line, went,
):
    held = (low, high)

    def leave(n):
        at = pl.ds(n * (BX - CHUNK), CHUNK)
        return pltpu.make_async_copy(held[n], out.at[:, at], went.at[n])

    main = pl.ds(8, BY)
    for rows, near, side, inner in ((x_low, 1, 1, 2), (x_high, 0, BX + 2, BX + 1)):
        here = rows[near * BY : (near + 1) * BY, :].astype(F32)
        there = rows[(1 - near) * BY : (2 - near) * BY, :].astype(F32)
        pair = rows[2 * BY : 2 * BY + 16, :].astype(F32)
        weight = coef[side, main, :]
        mine = weight * here
        line[main, :] = mine
        for n, y in enumerate((7, 8 + BY)):
            corner = coef[side, y : y + 1, :] * pair[n : n + 1]
            line[y : y + 1, :] = corner
            scaled[inner, y : y + 1, :] = (
                scaled[inner, y : y + 1, :] + coef[inner, y : y + 1, :] * corner
            )
        inside = coef[inner, main, :]
        total = inside * acc[(inner - 2) * BY : (inner - 1) * BY, :]
        total = total + coef[side + (-1 if side < 8 else 1), main, :] * there
        total = total + line[9 : 9 + BY, :] + line[7 : 7 + BY, :]
        scaled[side, main, :] = weight * (here + (total - 4.0 * mine))
        fixed = grown[inner - 2] + mine
        grown[inner - 2] = fixed
        scaled[inner, main, :] = inside * fixed
    for n in range(2):
        finish_rows(grown, scaled, held[n], n * (BX - CHUNK), CHUNK)
        leave(n).start()
    for n in range(2):
        leave(n).wait()


def edges(acc, coef, rims, so_far, grown, scaled, low, high):
    whole = pl.BlockSpec(memory_space=pltpu.VMEM)
    hbm = pl.BlockSpec(memory_space=pltpu.HBM)
    return pl.pallas_call(
        edges_kernel,
        in_specs=[whole] * 4 + [hbm] + [whole] * 4,
        out_specs=[hbm] + [whole] * 4,
        out_shape=[
            pltpu.HBM((LEV, BX, BY), F32),
            pltpu.VMEM((BX, BY, LEV), F32),
            pltpu.VMEM((PX, PY, LEV), F32),
            pltpu.VMEM((LEV, CHUNK, BY), F32),
            pltpu.VMEM((LEV, CHUNK, BY), F32),
        ],
        input_output_aliases={4: 0, 5: 1, 6: 2, 7: 3, 8: 4},
        scratch_shapes=[pltpu.VMEM((PY, LEV), F32), pltpu.SemaphoreType.DMA((2,))],
        compiler_params=params(4),
        cost_estimate=cost(2),
        name="edges",
    )(
        in_vmem(acc), in_vmem(coef), *rims, in_hbm(so_far),
        in_vmem(grown), in_vmem(scaled), in_vmem(low), in_vmem(high),
    )[0]


def exchange(array):
    return lax.all_to_all(array, ("tile", "obs"), split_axis=0, concat_axis=0, tiled=True)


def per_device(
    control,
    background,
    spread,
    obs_holder,
    obs_anchor,
    obs_frac,
    innovation,
    inverse_var,
    w_first,
    b_first,
    w_second,
    b_second,
    w_third,
):
    b_one = b_first.reshape(1, HID)
    b_two = b_second.reshape(1, HID)
    holder = obs_holder.reshape(1, OWN)
    innov = innovation.T
    w_last = w_third.T
    asked = requests(holder, obs_anchor.reshape(1, OWN), obs_frac, innov, inverse_var, w_last)
    got = exchange(asked.reshape(DEV, ROWS, HID))
    field, bgt, x_up, x_down, y_up, y_down = to_columns(control, background, spread)
    ay_low, ay_high = shift(y_up, "obs", 1), shift(y_down, "obs", -1)
    wide, first = early(spread, field)
    x_up, x_down = compose(x_up, x_down, ay_low, ay_high)
    ax_low, ax_high = shift(x_up, "tile", 1), shift(x_down, "tile", -1)
    before = (ax_low, ax_high, ay_low, ay_high)
    inct, kept = increments(field, wide, first, before)
    reply, slots = gathered(got, bgt.reshape(CELLS, LEV), inct.reshape(CELLS, LEV))
    reply = exchange(reply.reshape(DEV, ROWS, 2 * LEV))
    acc, x_up, x_down, y_up, y_down, coef, *held = adjoint(
        got, slots, w_first, b_one, w_second, b_two, w_last, inverse_var, kept, control
    )
    y_low, y_high = shift(y_up, "obs", 1), shift(y_down, "obs", -1)
    grown, scaled = ready(acc, coef)
    x_up, x_down = compose(x_up, x_down, y_low, y_high)
    x_low, x_high = shift(x_up, "tile", 1), shift(x_down, "tile", -1)
    gradient, _, grown, scaled = interior(acc, coef, (y_low, y_high), held[0], grown, scaled)
    gradient = edges(
        acc, coef, (x_low, x_high), gradient, grown, scaled, held[1], held[2]
    )
    departures = departures_of(
        reply.reshape(DEV * ROWS, 2 * LEV), holder, innov,
        w_first, b_one, w_second, b_two, w_last, inverse_var,
    ).T
    return departures, gradient


def solution(mesh):
    return jax.shard_map(
        per_device,
        mesh=mesh,
        in_specs=(
            P(None, "tile", "obs"),
            P(None, "tile", "obs"),
            P("tile", "obs"),
            P(("tile", "obs"), None),
            P(("tile", "obs")),
            P(None, ("tile", "obs")),
            P(("tile", "obs"), None),
            P(),
            P(),
            P(),
            P(),
            P(),
            P(),
        ),
        out_specs=(P(("tile", "obs"), None), P(None, "tile", "obs")),
        check_vma=False,
    )
```

```python
import functools

import jax
import jax.numpy as jnp
from jax import lax
from jax.experimental import pallas as pl
from jax.experimental.pallas import tpu as pltpu
from jax.sharding import PartitionSpec as P


F32 = jnp.float32
BF16 = jnp.bfloat16
LEV = 128
BX = 64
BY = 128
CELLS = BX * BY
OWN = 256
DEV = 128
CAP = 6
ROWS = 8
SLOTS = CAP * DEV
HID = 512
CH = 616
PX = BX + 4
PY = BY + 16
CHUNK = 8
TALL = 16


def params(mib, **extra):
    return pltpu.CompilerParams(vmem_limit_bytes=mib * 1024 * 1024, **extra)


def cost(us):
    return pl.CostEstimate(flops=int(us * 1.0e9), bytes_accessed=0, transcendentals=0)


def tn(a, b):
    return lax.dot_general(a, b, (((0,), (0,)), ((), ())), preferred_element_type=F32)


def down(row):
    return jnp.transpose(jnp.broadcast_to(row, (LEV, row.shape[1])))


def in_vmem(array):
    return pltpu.with_memory_space_constraint(array, pltpu.VMEM)


def in_hbm(array):
    return pltpu.with_memory_space_constraint(array, pltpu.HBM)


def nn(a, b):
    return jnp.dot(a, b, preferred_element_type=F32)


def nt(a, b):
    return lax.dot_general(a, b, (((1,), (1,)), ((), ())), preferred_element_type=F32)


def iota(shape, dim):
    return lax.broadcasted_iota(jnp.int32, shape, dim)


def split_two(a):
    high = a.astype(BF16)
    return high, (a - high.astype(F32)).astype(BF16)


def ranks(held):
    marks = (iota((DEV, OWN), 0) == held).astype(BF16)
    before = (iota((OWN, OWN), 0) < iota((OWN, OWN), 1)).astype(BF16)
    return jnp.sum(marks.astype(F32) * nn(marks, before), axis=0, keepdims=True).astype(jnp.int32)


def request_kernel(holder, anchor, frac, ivar, innov, w_third, out):
    held = holder[...]
    rank = ranks(held)
    at = anchor[...].astype(F32)
    x = jnp.floor((at + 0.5) * (1.0 / (BY - 1)))
    y = at - (BY - 1) * x
    fields = [x + 1.0, y]
    for dim in range(2):
        value = frac[dim : dim + 1, :]
        for _ in range(3):
            piece = value.astype(BF16).astype(F32)
            fields.append(piece)
            value = value - piece
    fields = jnp.concatenate(fields, axis=0)
    fields = jnp.concatenate([fields] * (LEV // 8), axis=0)
    fields = jnp.where((iota((LEV, OWN), 0) >> 3) == rank, fields, 0.0).astype(BF16)
    each = down(ivar[...].reshape(1, CH))
    row = iota((DEV * ROWS, OWN), 0)
    to_slot = (row == held * ROWS + rank).astype(BF16)
    to_fields = (row == held * ROWS + CAP).astype(BF16)
    scaled = (innov[...] * jnp.concatenate([each, each], axis=1)).astype(BF16)
    pulled = tn(scaled, w_third[...]).astype(BF16)
    out[:, :LEV] = (nn(to_slot, pulled[:, :LEV]) + nt(to_fields, fields)).astype(BF16)
    out[:, LEV:] = nn(to_slot, pulled[:, LEV:]).astype(BF16)


def requests(holder, anchor, frac, innov, ivar, w_third):
    return pl.pallas_call(
        request_kernel,
        out_shape=jax.ShapeDtypeStruct((DEV * ROWS, HID), BF16),
        compiler_params=params(12),
        cost_estimate=cost(4),
        name="requests",
    )(*map(in_hbm, (holder, anchor, frac, ivar, innov, w_third)))


def columns_kernel(
    control, background, spread, field, bgt, x_up, x_down, y_up, y_down,
    held, back_held, wide, turned_back, planes, came, back_came, went,
):
    tall = BX // TALL

    def bring(part):
        at = pl.ds(part * TALL, TALL)
        return pltpu.make_async_copy(control.at[:, at], held.at[part], came.at[part])

    def leave(part):
        at = pl.ds(part * TALL, TALL)
        return pltpu.make_async_copy(turned_back.at[at], bgt.at[at], went.at[part])

    fetch = pltpu.make_async_copy(background, back_held, back_came)
    bring(0).start()
    fetch.start()
    for part in range(1, tall):
        bring(part).start()
    fetch.wait()

    def turn(part, carry):
        first = pl.multiple_of(part * TALL, TALL)
        wide[...] = back_held[:, pl.ds(first, TALL), :].astype(F32).reshape(LEV * TALL, BY)
        bring(part).wait()
        flat = held.at[part].reshape(LEV * TALL, BY)
        for i in range(TALL):
            here = pl.ds(i, LEV, stride=TALL)
            turned = jnp.transpose(flat[here, :])
            field[first + i + 2, 8 : 8 + BY, :] = turned
            turned_back[first + i] = jnp.transpose(wide[here, :]).astype(BF16)
            for n, y in enumerate((0, 1, BY - 2, BY - 1)):
                planes[n, pl.ds(first + i, 1), :] = turned[y : y + 1, :LEV]
        leave(part).start()
        return carry

    lax.fori_loop(0, tall, turn, 0)
    x_down[:BY, :] = field[2, 8 : 8 + BY, :].astype(BF16)
    x_down[BY : 2 * BY, :] = field[3, 8 : 8 + BY, :].astype(BF16)
    x_up[:BY, :] = field[BX, 8 : 8 + BY, :].astype(BF16)
    x_up[BY : 2 * BY, :] = field[BX + 1, 8 : 8 + BY, :].astype(BF16)
    s = spread[...]
    turned = jnp.transpose(jnp.concatenate([s, s], axis=0))

    def rows(two):
        high, low = split_two(two)
        zero = jnp.zeros((12, BY), F32)
        return jnp.concatenate([high.astype(F32), low.astype(F32), zero], axis=0).astype(BF16)

    x_down[2 * BY :, :] = rows(s[0:2, :])
    x_up[2 * BY :, :] = rows(s[BX - 2 : BX, :])
    y_down[: 2 * BX, :] = planes[0:2].reshape(2 * BX, LEV).astype(BF16)
    y_up[: 2 * BX, :] = planes[2:4].reshape(2 * BX, LEV).astype(BF16)
    y_down[2 * BX :, :] = rows(turned[0:2, :])
    y_up[2 * BX :, :] = rows(turned[BY - 2 : BY, :])
    for part in range(tall):
        leave(part).wait()


def to_columns(control, background, spread):
    hbm = pl.BlockSpec(memory_space=pltpu.HBM)
    whole = pl.BlockSpec(memory_space=pltpu.VMEM)
    return pl.pallas_call(
        columns_kernel,
        in_specs=[hbm, hbm, whole],
        out_specs=[whole, hbm] + [whole] * 4,
        out_shape=[
            pltpu.VMEM((PX, PY, LEV), F32),
            pltpu.HBM((BX, BY, LEV), BF16),
            jax.ShapeDtypeStruct((2 * BY + 16, LEV), BF16),
            jax.ShapeDtypeStruct((2 * BY + 16, LEV), BF16),
            jax.ShapeDtypeStruct((2 * BX + 16, LEV), BF16),
            jax.ShapeDtypeStruct((2 * BX + 16, LEV), BF16),
        ],
        scratch_shapes=[
            pltpu.VMEM((BX // TALL, LEV, TALL, BY), F32),
            pltpu.VMEM((LEV, BX, BY), BF16),
            pltpu.VMEM((LEV * TALL, BY), F32),
            pltpu.VMEM((BX, BY, LEV), BF16),
            pltpu.VMEM((4, BX, LEV), F32),
            pltpu.SemaphoreType.DMA((BX // TALL,)),
            pltpu.SemaphoreType.DMA,
            pltpu.SemaphoreType.DMA((BX // TALL,)),
        ],
        compiler_params=params(16),
        cost_estimate=cost(6),
        name="columns",
    )(in_hbm(control), in_hbm(background), spread)


def shift(array, axis, by):
    count = lax.axis_size(axis)
    return lax.ppermute(array, axis, [(i, (i + by) % count) for i in range(count)])


def compose_kernel(count, first_up, first_down, low, high, up, down):
    rows = first_up.shape[0]
    up[:rows, :] = first_up[...]
    down[:rows, :] = first_down[...]
    low = low[...].astype(F32)
    high = high[...].astype(F32)
    fields = [low[2 * count :], high[2 * count :]] if low.shape[0] > 2 * count else []
    for out, row in ((up, count - 1), (down, 0)):
        pair = [low[count + row : count + row + 1], high[row : row + 1], jnp.zeros((14, LEV), F32)]
        out[rows:, :] = jnp.concatenate(pair + fields, axis=0).astype(BF16)


def compose(count, first_up, first_down, low, high):
    rows = first_up.shape[0] + 16 + 2 * (low.shape[0] - 2 * count)
    return pl.pallas_call(
        functools.partial(compose_kernel, count),
        out_shape=[jax.ShapeDtypeStruct((rows, LEV), BF16)] * 2,
        compiler_params=params(2),
        name="compose",
    )(first_up, first_down, low, high)


def laplace(field, x, first, count):
    total = field[x + 1, pl.ds(first, count), :] + field[x - 1, pl.ds(first, count), :]
    total = total + field[x, pl.ds(first + 1, count), :]
    total = total + field[x, pl.ds(first - 1, count), :]
    return total - 4.0 * field[x, pl.ds(first, count), :]


def plane(field, x, y, count):
    flat = field.reshape(PX * PY, LEV)
    return flat[pl.ds(x * PY + y, count, stride=PY), :]


def set_plane(field, x, y, count, value):
    flat = field.reshape(PX * PY, LEV)
    flat[pl.ds(x * PY + y, count, stride=PY), :] = value


def plane_laplace(field, y):
    total = plane(field, 3, y, BX) + plane(field, 1, y, BX)
    total = total + plane(field, 2, y + 1, BX) + plane(field, 2, y - 1, BX)
    return total - 4.0 * plane(field, 2, y, BX)


def lanes(column):
    return jnp.broadcast_to(column, (column.shape[0], LEV))


def joined(rows, at):
    block = rows[at : at + 16, :].astype(F32)
    return block[0:2] + block[2:4]


def fill_y(field, y_low, y_high):
    for n in range(2):
        set_plane(field, 2, 6 + n, BX, y_low[n * BX : (n + 1) * BX, :].astype(F32))
        set_plane(field, 2, 8 + BY + n, BX, y_high[n * BX : (n + 1) * BX, :].astype(F32))


def fill_x(field, x_low, x_high):
    for n in range(2):
        field[n, 8 : 8 + BY, :] = x_low[n * BY : (n + 1) * BY, :].astype(F32)
        field[BX + 2 + n, 8 : 8 + BY, :] = x_high[n * BY : (n + 1) * BY, :].astype(F32)


def fill_corners(field, y_low, y_high):
    for rows, y in ((y_low, 7), (y_high, 8 + BY)):
        pair = rows[2 * BX + 16 : 2 * BX + 32, :].astype(F32)
        field[1, y : y + 1, :] = pair[0:1]
        field[BX + 2, y : y + 1, :] = pair[1:2]


def main_coefficients(coef, spread):
    square = jnp.concatenate([spread[...], jnp.zeros((BY - BX, BY), F32)], axis=0)
    turned = jnp.transpose(square)
    for x in range(BX):
        coef[x + 2, 8 : 8 + BY, :] = lanes(turned[:, x : x + 1])


def rim_coefficients(coef, x_low, x_high, y_low, y_high):
    ends = jnp.concatenate(
        [joined(x_low, 2 * BY), joined(x_high, 2 * BY), jnp.zeros((BY - 4, BY), F32)], axis=0
    )
    ends = jnp.transpose(ends)
    for n, x in enumerate((0, 1, BX + 2, BX + 3)):
        coef[x, 8 : 8 + BY, :] = lanes(ends[:, n : n + 1])
    sides = jnp.concatenate(
        [joined(y_low, 2 * BX), joined(y_high, 2 * BX), jnp.zeros((BY - 4, BY), F32)], axis=0
    )
    sides = jnp.transpose(sides)[:BX, :]
    for n in range(2):
        set_plane(coef, 2, 6 + n, BX, lanes(sides[:, n : n + 1]))
        set_plane(coef, 2, 8 + BY + n, BX, lanes(sides[:, 2 + n : 3 + n]))
    for block, y, lane in ((y_low, 7, BY - 1), (y_high, 8 + BY, 0)):
        left = joined(block, 2 * BX + 32)
        right = joined(block, 2 * BX + 48)
        coef[1, y : y + 1, :] = lanes(left[1:2, lane : lane + 1])
        coef[BX + 2, y : y + 1, :] = lanes(right[0:1, lane : lane + 1])


def sweep(to, field, coef, x):
    middle = field[x, 8 : 8 + BY, :]
    to[x, 8 : 8 + BY, :] = middle + coef[x, 8 : 8 + BY, :] * laplace(field, x, 8, BY)


def early_kernel(spread, field, coef, first):
    main_coefficients(coef, spread)

    def one(x, carry):
        sweep(first, field, coef, x)
        return carry

    lax.fori_loop(3, PX - 3, one, 0)


def early(spread, field):
    return pl.pallas_call(
        early_kernel,
        out_shape=[pltpu.VMEM((PX, PY, LEV), F32), pltpu.VMEM((PX, PY, LEV), F32)],
        compiler_params=params(2),
        cost_estimate=cost(2),
        name="early",
    )(spread, in_vmem(field))


def joined(rows, at):
    block = rows[at : at + 16, :].astype(F32)
    return block[0:2] + block[2:4]


PARTS = BX // CHUNK


def increment_kernel(
    _field, _coef, _first, x_low, x_high, y_low, y_high,
    inc, kept, field, coef, first, done, went, kept_went,
):
    def leave(part):
        at = pl.ds(part * CHUNK, CHUNK)
        return pltpu.make_async_copy(done.at[at], inc.at[at], went.at[part])

    rim_coefficients(coef, x_low, x_high, y_low, y_high)
    keep = pltpu.make_async_copy(coef, kept, kept_went)
    keep.start()
    fill_x(field, x_low, x_high)
    fill_corners(field, y_low, y_high)
    fill_y(field, y_low, y_high)

    for x in (1, 2, BX + 1, BX + 2):
        sweep(first, field, coef, x)
    for y in (7, 8, 7 + BY, 8 + BY):
        moved = plane(field, 2, y, BX) + plane(coef, 2, y, BX) * plane_laplace(field, y)
        set_plane(first, 2, y, BX, moved)

    def sweep_two(x, carry):
        middle = first[x, 8 : 8 + BY, :]
        result = middle + coef[x, 8 : 8 + BY, :] * laplace(first, x, 8, BY)
        done[x - 2] = result.astype(BF16)
        return carry

    for part in range(PARTS):
        lax.fori_loop(2 + CHUNK * part, 2 + CHUNK * (part + 1), sweep_two, 0)
        leave(part).start()
    for part in range(PARTS):
        leave(part).wait()
    keep.wait()


def increments(field, coef, first, rims):
    whole = pl.BlockSpec(memory_space=pltpu.VMEM)
    padded = pltpu.VMEM((PX, PY, LEV), F32)
    return pl.pallas_call(
        increment_kernel,
        in_specs=[whole] * 7,
        out_specs=[pl.BlockSpec(memory_space=pltpu.HBM)] * 2 + [whole] * 3,
        out_shape=[
            pltpu.HBM((BX, BY, LEV), BF16),
            pltpu.HBM((PX, PY, LEV), F32),
            padded,
            padded,
            padded,
        ],
        input_output_aliases={0: 2, 1: 3, 2: 4},
        scratch_shapes=[
            pltpu.VMEM((BX, BY, LEV), BF16),
            pltpu.SemaphoreType.DMA((PARTS,)),
            pltpu.SemaphoreType.DMA,
        ],
        compiler_params=params(8),
        cost_estimate=cost(6),
        name="increment",
    )(in_vmem(field), in_vmem(coef), in_vmem(first), *rims)[:2]


def decode(rows):
    back = lambda n: pltpu.roll(rows, LEV - n, 1)
    frac_x = back(2) + back(3) + back(4)
    frac_y = back(5) + back(6) + back(7)
    valid = rows > 0.5
    cell = jnp.where(valid, ((rows - 1.0) * BY + back(1)).astype(jnp.int32), 2 * iota(rows.shape, 0))
    off = lambda w: jnp.where(valid, w, 0.0)
    return cell, (
        off((1.0 - frac_x) * (1.0 - frac_y)),
        off(frac_x * (1.0 - frac_y)),
        off((1.0 - frac_x) * frac_y),
        off(frac_x * frac_y),
    )


def to_table(cell, cells, table, arrived):
    across = jnp.transpose(cell)
    for k in range(CAP):
        cells[k : k + 1, :] = across[8 * k : 8 * k + 1, :]
    copy = pltpu.make_async_copy(cells, table, arrived)
    copy.start()
    return copy


def gather_kernel(
    got, background, increment, reply, slots,
    wide, cells, table, ga, gb, spaced, both, packed, came, arrived,
):
    part = CELLS // PARTS

    def bring(n, i):
        at = pl.ds(i * part, part)
        source = (background, increment)[n]
        return pltpu.make_async_copy(source.at[at], packed.at[n, at], came.at[n, i])

    for i in range(PARTS):
        bring(0, i).start()
        bring(1, i).start()
    wide[...] = got[...].astype(F32).reshape(DEV * ROWS, LEV)
    cell, weights = decode(wide[pl.ds(CAP, DEV, stride=ROWS), :])
    placed = to_table(cell, cells, table, arrived)
    for i in range(PARTS):
        for n in range(2):
            bring(n, i).wait()

            def widen(j, carry):
                first = pl.multiple_of(i * part + j * BY, BY)
                both[pl.ds(2 * first + n, BY, stride=2), :] = packed[n, pl.ds(first, BY), :].astype(F32)
                return carry

            lax.fori_loop(0, part // BY, widen, 0)
    placed.wait()
    for k in range(CAP):

        def fetch(step, carry):
            for n in range(8):
                owner = step * 8 + n
                at = table[k, owner]
                to = pl.ds(4 * (k * DEV + owner), 4)
                ga[to, :] = both[pl.ds(2 * at, 4), :]
                gb[to, :] = both[pl.ds(2 * (at + BY), 4), :]
            return carry

        lax.fori_loop(0, DEV // 8, fetch, 0)
    spaced[...] = jnp.zeros_like(spaced)
    for k in range(CAP):
        w = [lanes(weight[:, 8 * k : 8 * k + 1]) for weight in weights]
        for n in range(2):
            here = pl.ds(4 * DEV * k + n, DEV, stride=4)
            next_to = pl.ds(4 * DEV * k + 2 + n, DEV, stride=4)
            mixed = w[0] * ga[here, :] + w[1] * gb[here, :]
            mixed = mixed + w[2] * ga[next_to, :]
            mixed = mixed + w[3] * gb[next_to, :]
            slots[k * DEV : (k + 1) * DEV, n * LEV : (n + 1) * LEV] = mixed.astype(BF16)
            spaced[n, pl.ds(k, DEV, stride=ROWS), :] = mixed
    reply[:, :LEV] = spaced[0].astype(BF16)
    reply[:, LEV:] = spaced[1].astype(BF16)


def gathered(got, bgt, inct):
    rows = pltpu.VMEM((4 * SLOTS, LEV), F32)
    whole = pl.BlockSpec(memory_space=pltpu.VMEM)
    return pl.pallas_call(
        gather_kernel,
        grid=(1,),
        in_specs=[pl.BlockSpec((DEV, ROWS, LEV), lambda i: (0, 0, 0))]
        + [pl.BlockSpec(memory_space=pltpu.HBM)] * 2,
        out_specs=[whole, whole],
        out_shape=[
            jax.ShapeDtypeStruct((DEV * ROWS, 2 * LEV), BF16),
            jax.ShapeDtypeStruct((SLOTS, 2 * LEV), BF16),
        ],
        scratch_shapes=[
            pltpu.VMEM((DEV * ROWS, LEV), F32),
            pltpu.VMEM((8, LEV), jnp.int32),
            pltpu.SMEM((8, LEV), jnp.int32),
            rows,
            rows,
            pltpu.VMEM((2, DEV * ROWS, LEV), F32),
            pltpu.VMEM((2 * CELLS, LEV), F32),
            pltpu.VMEM((2, CELLS, LEV), BF16),
            pltpu.SemaphoreType.DMA((2, PARTS)),
            pltpu.SemaphoreType.DMA,
        ],
        compiler_params=params(26),
        cost_estimate=cost(5),
        name="gather",
    )(got, in_hbm(bgt), in_hbm(inct))


def tangent(base, delta, w_first, b_first, w_second, b_second):
    h_one = jnp.tanh(nn(base, w_first) + b_first)
    d_one = 1.0 - h_one * h_one
    h_two = jnp.tanh(nn(h_one.astype(BF16), w_second) + b_second)
    d_two = 1.0 - h_two * h_two
    t_one = (d_one * nn(delta, w_first)).astype(BF16)
    t_two = (d_two * nn(t_one, w_second)).astype(BF16)
    return d_one, d_two, t_two


BLOCK = 768


def adjoint_kernel(
    got, slots, w_first, b_first, w_second, b_second, w_third, ivar, kept, control,
    acc, x_up, x_down, y_up, y_down, coef, held, low, high,
    wide, pulled, profile, cells, table, ca, cb, came, arrived,
):
    copies = [pltpu.make_async_copy(kept, coef, came.at[3])] + [
        pltpu.make_async_copy(control.at[:, pl.ds(at, to.shape[1])], to, came.at[n])
        for n, (to, at) in enumerate(((held, CHUNK), (low, 0), (high, BX - CHUNK)))
    ]
    for copy in copies:
        copy.start()
    for n in range(HID // LEV):
        at = slice(n * LEV, (n + 1) * LEV)
        wide[...] = got[:, :, at].astype(F32).reshape(DEV * ROWS, LEV)
        for k in range(CAP):
            pulled[k * DEV : (k + 1) * DEV, at] = wide[pl.ds(k, DEV, stride=ROWS), :]
        if n == 0:
            cell, weights = decode(wide[pl.ds(CAP, DEV, stride=ROWS), :])
    placed = to_table(cell, cells, table, arrived)

    def block(i, carry):
        here = pl.ds(pl.multiple_of(i * BLOCK, BLOCK), BLOCK)
        d_one, d_two, t_two = tangent(
            slots[here, :LEV], slots[here, LEV:],
            w_first[...], b_first[...], w_second[...], b_second[...],
        )
        change = nt(t_two, w_third[...]) * ivar[...].reshape(1, CH)
        s_two = (d_two * (nn(change.astype(BF16), w_third[...]) - pulled[here, :])).astype(BF16)
        s_one = (d_one * nt(s_two, w_second[...])).astype(BF16)
        profile[here, :] = nt(s_one, w_first[...])
        return carry

    lax.fori_loop(0, SLOTS // BLOCK, block, 0)
    acc[...] = jnp.zeros_like(acc)
    for k in range(CAP):
        grad = profile[k * DEV : (k + 1) * DEV, :]
        w = [lanes(weight[:, 8 * k : 8 * k + 1]) for weight in weights]
        even = pl.ds(2 * DEV * k, DEV, stride=2)
        odd = pl.ds(2 * DEV * k + 1, DEV, stride=2)
        ca[even, :] = w[0] * grad
        cb[even, :] = w[1] * grad
        ca[odd, :] = w[2] * grad
        cb[odd, :] = w[3] * grad
    placed.wait()
    for k in range(CAP):

        def add(step, carry):
            for n in range(8):
                owner = step * 8 + n
                at = table[k, owner]
                there = pl.ds(2 * (k * DEV + owner), 2)
                one = acc[pl.ds(at, 2), :] + ca[there, :]
                two = acc[pl.ds(at + BY, 2), :] + cb[there, :]
                acc[pl.ds(at, 2), :] = one
                acc[pl.ds(at + BY, 2), :] = two
            return carry

        lax.fori_loop(0, DEV // 8, add, 0)
    x_down[...] = acc[: 2 * BY, :].astype(BF16)
    x_up[...] = acc[CELLS - 2 * BY :, :].astype(BF16)
    for n in range(2):
        y_down[n * BX : (n + 1) * BX, :] = acc[pl.ds(n, BX, stride=BY), :].astype(BF16)
        y_up[n * BX : (n + 1) * BX, :] = acc[pl.ds(BY - 2 + n, BX, stride=BY), :].astype(BF16)
    for copy in copies:
        copy.wait()


INNER = BX - 2 * CHUNK


def adjoint(got, slots, w_first, b_first, w_second, b_second, w_third, ivar, kept, control):
    whole = pl.BlockSpec(memory_space=pltpu.VMEM)
    return pl.pallas_call(
        adjoint_kernel,
        in_specs=[whole] * 8 + [pl.BlockSpec(memory_space=pltpu.HBM)] * 2,
        out_specs=[whole] * 9,
        out_shape=[
            pltpu.VMEM((CELLS, LEV), F32),
            jax.ShapeDtypeStruct((2 * BY, LEV), BF16),
            jax.ShapeDtypeStruct((2 * BY, LEV), BF16),
            jax.ShapeDtypeStruct((2 * BX, LEV), BF16),
            jax.ShapeDtypeStruct((2 * BX, LEV), BF16),
            pltpu.VMEM((PX, PY, LEV), F32),
            pltpu.VMEM((LEV, INNER, BY), F32),
            pltpu.VMEM((LEV, CHUNK, BY), F32),
            pltpu.VMEM((LEV, CHUNK, BY), F32),
        ],
        scratch_shapes=[
            pltpu.VMEM((DEV * ROWS, LEV), F32),
            pltpu.VMEM((SLOTS, HID), F32),
            pltpu.VMEM((SLOTS, LEV), F32),
            pltpu.VMEM((8, LEV), jnp.int32),
            pltpu.SMEM((8, LEV), jnp.int32),
            pltpu.VMEM((2 * SLOTS, LEV), F32),
            pltpu.VMEM((2 * SLOTS, LEV), F32),
            pltpu.SemaphoreType.DMA((4,)),
            pltpu.SemaphoreType.DMA,
        ],
        compiler_params=params(32),
        cost_estimate=cost(10),
        name="adjoint",
    )(
        got, slots, w_first, b_first, w_second, b_second, w_third, ivar,
        in_hbm(kept), in_hbm(control),
    )


def departure_kernel(
    reply, holder, innov, w_first, b_first, w_second, b_second, w_third, ivar, out
):
    held = holder[...]
    pick = (iota((OWN, DEV * ROWS), 1) == down(held * ROWS + ranks(held)).astype(jnp.int32)[:, 0:1]).astype(BF16)
    own = nn(pick, reply[...]).astype(BF16)
    _, _, t_two = tangent(
        own[:, :LEV], own[:, LEV:], w_first[...], b_first[...], w_second[...], b_second[...]
    )
    each = down(ivar[...].reshape(1, CH))
    out[...] = (nt(w_third[...], t_two) - innov[...]) * jnp.concatenate([each, each], axis=1)


def departures_of(reply, holder, innov, w_first, b_first, w_second, b_second, w_third, ivar):
    return pl.pallas_call(
        departure_kernel,
        out_shape=jax.ShapeDtypeStruct((CH, OWN), F32),
        compiler_params=params(12),
        cost_estimate=cost(4),
        name="departures",
    )(reply, holder, innov, w_first, b_first, w_second, b_second, w_third, ivar)


def ready_kernel(acc, coef, grown, scaled, field):
    for x in (1, BX + 2):
        field[x] = jnp.zeros((PY, LEV), F32)
    for y in (7, 8 + BY):
        set_plane(field, 2, y, BX, jnp.zeros((BX, LEV), F32))

    def scale(x, carry):
        at = pl.ds(pl.multiple_of((x - 2) * BY, BY), BY)
        field[x, 8 : 8 + BY, :] = coef[x, 8 : 8 + BY, :] * acc[at, :]
        return carry

    lax.fori_loop(2, PX - 2, scale, 0)

    def sweep_one(x, carry):
        at = pl.ds(pl.multiple_of((x - 2) * BY, BY), BY)
        value = acc[at, :] + laplace(field, x, 8, BY)
        grown[x - 2] = value
        scaled[x, 8 : 8 + BY, :] = coef[x, 8 : 8 + BY, :] * value
        return carry

    lax.fori_loop(2, PX - 2, sweep_one, 0)


def ready(acc, coef):
    return pl.pallas_call(
        ready_kernel,
        out_shape=[pltpu.VMEM((BX, BY, LEV), F32), pltpu.VMEM((PX, PY, LEV), F32)],
        scratch_shapes=[pltpu.VMEM((PX, PY, LEV), F32)],
        compiler_params=params(8),
        cost_estimate=cost(3),
        name="ready",
    )(in_vmem(acc), in_vmem(coef))


def finish_rows(grown, scaled, held, first, count):
    flat = held.reshape(LEV * held.shape[1], BY)
    for i in range(count):
        x = first + i
        value = grown[x] + laplace(scaled, x + 2, 8, BY)
        here = pl.ds(i, LEV, stride=held.shape[1])
        flat[here, :] = jnp.transpose(value) + flat[here, :]


def interior_kernel(
    acc, coef, y_low, y_high, _held, _grown, _scaled, out, held, grown, scaled, went
):
    edge = iota((BX, LEV), 0)
    for rows, near, far, side, inner in (
        (y_low, 1, 0, 7, 8),
        (y_high, 0, 1, 8 + BY, 7 + BY),
    ):
        here = rows[near * BX : (near + 1) * BX, :].astype(F32)
        there = rows[far * BX : (far + 1) * BX, :].astype(F32)
        weight = plane(coef, 2, side, BX)
        mine = weight * here
        over = side + (-1 if side < 8 else 1)
        total = jnp.where(edge == BX - 1, 0.0, pltpu.roll(mine, BX - 1, 0))
        total = total + jnp.where(edge == 0, 0.0, pltpu.roll(mine, 1, 0))
        touching = acc[pl.ds(inner - 8, BX, stride=BY), :]
        inside = plane(coef, 2, inner, BX)
        total = total + inside * touching + plane(coef, 2, over, BX) * there
        set_plane(scaled, 2, side, BX, weight * (here + (total - 4.0 * mine)))
        flat = grown.reshape(CELLS, LEV)
        at = pl.ds(inner - 8, BX, stride=BY)
        fixed = flat[at, :] + mine
        flat[at, :] = fixed
        set_plane(scaled, 2, inner, BX, inside * fixed)

    def leave(part):
        return pltpu.make_async_copy(
            held.at[:, pl.ds(part * TALL, TALL)],
            out.at[:, pl.ds(CHUNK + part * TALL, TALL)],
            went.at[part],
        )

    for part in range(INNER // TALL):
        first = part * TALL

        def some(step, carry):
            flat = held.reshape(LEV * INNER, BY)
            for i in range(4):
                at = first + step * 4 + i
                value = grown[CHUNK + at] + laplace(scaled, CHUNK + at + 2, 8, BY)
                here = pl.ds(at, LEV, stride=INNER)
                flat[here, :] = jnp.transpose(value) + flat[here, :]
            return carry

        lax.fori_loop(0, TALL // 4, some, 0)
        leave(part).start()
    for part in range(INNER // TALL):
        leave(part).wait()


def interior(acc, coef, rims, held, grown, scaled):
    whole = pl.BlockSpec(memory_space=pltpu.VMEM)
    hbm = pl.BlockSpec(memory_space=pltpu.HBM)
    return pl.pallas_call(
        interior_kernel,
        in_specs=[whole] * 7,
        out_specs=[hbm] + [whole] * 3,
        out_shape=[
            pltpu.HBM((LEV, BX, BY), F32),
            pltpu.VMEM((LEV, INNER, BY), F32),
            pltpu.VMEM((BX, BY, LEV), F32),
            pltpu.VMEM((PX, PY, LEV), F32),
        ],
        input_output_aliases={4: 1, 5: 2, 6: 3},
        scratch_shapes=[pltpu.SemaphoreType.DMA((INNER // TALL,))],
        compiler_params=params(4),
        cost_estimate=cost(5),
        name="interior",
    )(in_vmem(acc), in_vmem(coef), *rims, in_vmem(held), in_vmem(grown), in_vmem(scaled))


def edges_kernel(
    acc, coef, x_low, x_high, _out, _grown, _scaled, _low, _high,
    out, grown, scaled, low, high, line, went,
):
    held = (low, high)

    def leave(n):
        at = pl.ds(n * (BX - CHUNK), CHUNK)
        return pltpu.make_async_copy(held[n], out.at[:, at], went.at[n])

    main = pl.ds(8, BY)
    for rows, near, side, inner in ((x_low, 1, 1, 2), (x_high, 0, BX + 2, BX + 1)):
        here = rows[near * BY : (near + 1) * BY, :].astype(F32)
        there = rows[(1 - near) * BY : (2 - near) * BY, :].astype(F32)
        pair = rows[2 * BY : 2 * BY + 16, :].astype(F32)
        weight = coef[side, main, :]
        mine = weight * here
        line[main, :] = mine
        for n, y in enumerate((7, 8 + BY)):
            corner = coef[side, y : y + 1, :] * pair[n : n + 1]
            line[y : y + 1, :] = corner
            scaled[inner, y : y + 1, :] = (
                scaled[inner, y : y + 1, :] + coef[inner, y : y + 1, :] * corner
            )
        inside = coef[inner, main, :]
        total = inside * acc[(inner - 2) * BY : (inner - 1) * BY, :]
        total = total + coef[side + (-1 if side < 8 else 1), main, :] * there
        total = total + line[9 : 9 + BY, :] + line[7 : 7 + BY, :]
        scaled[side, main, :] = weight * (here + (total - 4.0 * mine))
        fixed = grown[inner - 2] + mine
        grown[inner - 2] = fixed
        scaled[inner, main, :] = inside * fixed
    for n in range(2):
        finish_rows(grown, scaled, held[n], n * (BX - CHUNK), CHUNK)
        leave(n).start()
    for n in range(2):
        leave(n).wait()


def edges(acc, coef, rims, so_far, grown, scaled, low, high):
    whole = pl.BlockSpec(memory_space=pltpu.VMEM)
    hbm = pl.BlockSpec(memory_space=pltpu.HBM)
    return pl.pallas_call(
        edges_kernel,
        in_specs=[whole] * 4 + [hbm] + [whole] * 4,
        out_specs=[hbm] + [whole] * 4,
        out_shape=[
            pltpu.HBM((LEV, BX, BY), F32),
            pltpu.VMEM((BX, BY, LEV), F32),
            pltpu.VMEM((PX, PY, LEV), F32),
            pltpu.VMEM((LEV, CHUNK, BY), F32),
            pltpu.VMEM((LEV, CHUNK, BY), F32),
        ],
        input_output_aliases={4: 0, 5: 1, 6: 2, 7: 3, 8: 4},
        scratch_shapes=[pltpu.VMEM((PY, LEV), F32), pltpu.SemaphoreType.DMA((2,))],
        compiler_params=params(4),
        cost_estimate=cost(2),
        name="edges",
    )(
        in_vmem(acc), in_vmem(coef), *rims, in_hbm(so_far),
        in_vmem(grown), in_vmem(scaled), in_vmem(low), in_vmem(high),
    )[0]


def exchange(array):
    return lax.all_to_all(array, ("tile", "obs"), split_axis=0, concat_axis=0, tiled=True)


def per_device(
    control,
    background,
    spread,
    obs_holder,
    obs_anchor,
    obs_frac,
    innovation,
    inverse_var,
    w_first,
    b_first,
    w_second,
    b_second,
    w_third,
):
    b_one = b_first.reshape(1, HID)
    b_two = b_second.reshape(1, HID)
    holder = obs_holder.reshape(1, OWN)
    innov = innovation.T
    w_last = w_third.T
    asked = requests(holder, obs_anchor.reshape(1, OWN), obs_frac, innov, inverse_var, w_last)
    got = exchange(asked.reshape(DEV, ROWS, HID))
    field, bgt, x_up, x_down, y_up, y_down = to_columns(control, background, spread)
    ax_low, ax_high = shift(x_up, "tile", 1), shift(x_down, "tile", -1)
    wide, first = early(spread, field)
    y_up, y_down = compose(BY, y_up, y_down, ax_low, ax_high)
    ay_low, ay_high = shift(y_up, "obs", 1), shift(y_down, "obs", -1)
    before = (ax_low, ax_high, ay_low, ay_high)
    inct, kept = increments(field, wide, first, before)
    reply, slots = gathered(got, bgt.reshape(CELLS, LEV), inct.reshape(CELLS, LEV))
    reply = exchange(reply.reshape(DEV, ROWS, 2 * LEV))
    acc, x_up, x_down, y_up, y_down, coef, *held = adjoint(
        got, slots, w_first, b_one, w_second, b_two, w_last, inverse_var, kept, control
    )
    y_low, y_high = shift(y_up, "obs", 1), shift(y_down, "obs", -1)
    grown, scaled = ready(acc, coef)
    x_up, x_down = compose(BX, x_up, x_down, y_low, y_high)
    x_low, x_high = shift(x_up, "tile", 1), shift(x_down, "tile", -1)
    gradient, _, grown, scaled = interior(acc, coef, (y_low, y_high), held[0], grown, scaled)
    gradient = edges(
        acc, coef, (x_low, x_high), gradient, grown, scaled, held[1], held[2]
    )
    departures = departures_of(
        reply.reshape(DEV * ROWS, 2 * LEV), holder, innov,
        w_first, b_one, w_second, b_two, w_last, inverse_var,
    ).T
    return departures, gradient


def solution(mesh):
    return jax.shard_map(
        per_device,
        mesh=mesh,
        in_specs=(
            P(None, "tile", "obs"),
            P(None, "tile", "obs"),
            P("tile", "obs"),
            P(("tile", "obs"), None),
            P(("tile", "obs")),
            P(None, ("tile", "obs")),
            P(("tile", "obs"), None),
            P(),
            P(),
            P(),
            P(),
            P(),
            P(),
        ),
        out_specs=(P(("tile", "obs"), None), P(None, "tile", "obs")),
        check_vma=False,
    )
```

```python
import functools

import jax
import jax.numpy as jnp
from jax import lax
from jax.experimental import pallas as pl
from jax.experimental.pallas import tpu as pltpu
from jax.sharding import PartitionSpec as P


F32 = jnp.float32
BF16 = jnp.bfloat16
LEV = 128
BX = 64
BY = 128
CELLS = BX * BY
OWN = 256
DEV = 128
CAP = 6
ROWS = 8
SLOTS = CAP * DEV
HID = 512
CH = 616
PX = BX + 4
PY = BY + 16
CHUNK = 8
TALL = 16


def params(mib, **extra):
    return pltpu.CompilerParams(vmem_limit_bytes=mib * 1024 * 1024, **extra)


def cost(us):
    return pl.CostEstimate(flops=int(us * 1.0e9), bytes_accessed=0, transcendentals=0)


def tn(a, b):
    return lax.dot_general(a, b, (((0,), (0,)), ((), ())), preferred_element_type=F32)


def down(row):
    return jnp.transpose(jnp.broadcast_to(row, (LEV, row.shape[1])))


def in_vmem(array):
    return pltpu.with_memory_space_constraint(array, pltpu.VMEM)


def in_hbm(array):
    return pltpu.with_memory_space_constraint(array, pltpu.HBM)


def nn(a, b):
    return jnp.dot(a, b, preferred_element_type=F32)


def nt(a, b):
    return lax.dot_general(a, b, (((1,), (1,)), ((), ())), preferred_element_type=F32)


def iota(shape, dim):
    return lax.broadcasted_iota(jnp.int32, shape, dim)


def split_two(a):
    high = a.astype(BF16)
    return high, (a - high.astype(F32)).astype(BF16)


def ranks(held):
    marks = (iota((DEV, OWN), 0) == held).astype(BF16)
    before = (iota((OWN, OWN), 0) < iota((OWN, OWN), 1)).astype(BF16)
    return jnp.sum(marks.astype(F32) * nn(marks, before), axis=0, keepdims=True).astype(jnp.int32)


def request_kernel(holder, anchor, frac, ivar, innov, w_third, out):
    held = holder[...]
    rank = ranks(held)
    at = anchor[...].astype(F32)
    x = jnp.floor((at + 0.5) * (1.0 / (BY - 1)))
    y = at - (BY - 1) * x
    fields = [x + 1.0, y]
    for dim in range(2):
        value = frac[dim : dim + 1, :]
        for _ in range(3):
            piece = value.astype(BF16).astype(F32)
            fields.append(piece)
            value = value - piece
    fields = jnp.concatenate(fields, axis=0)
    fields = jnp.concatenate([fields] * (LEV // 8), axis=0)
    fields = jnp.where((iota((LEV, OWN), 0) >> 3) == rank, fields, 0.0).astype(BF16)
    each = down(ivar[...].reshape(1, CH))
    row = iota((DEV * ROWS, OWN), 0)
    to_slot = (row == held * ROWS + rank).astype(BF16)
    to_fields = (row == held * ROWS + CAP).astype(BF16)
    scaled = (innov[...] * jnp.concatenate([each, each], axis=1)).astype(BF16)
    pulled = tn(scaled, w_third[...]).astype(BF16)
    out[:, :LEV] = (nn(to_slot, pulled[:, :LEV]) + nt(to_fields, fields)).astype(BF16)
    out[:, LEV:] = nn(to_slot, pulled[:, LEV:]).astype(BF16)


def requests(holder, anchor, frac, innov, ivar, w_third):
    return pl.pallas_call(
        request_kernel,
        out_shape=jax.ShapeDtypeStruct((DEV * ROWS, HID), BF16),
        compiler_params=params(12),
        cost_estimate=cost(4),
        name="requests",
    )(*map(in_hbm, (holder, anchor, frac, ivar, innov, w_third)))


def columns_kernel(
    control, background, spread, field, bgt, x_up, x_down, y_up, y_down,
    held, back_held, wide, turned_back, planes, came, back_came, went,
):
    tall = BX // TALL

    def bring(part):
        at = pl.ds(part * TALL, TALL)
        return pltpu.make_async_copy(control.at[:, at], held.at[part], came.at[part])

    def leave(part):
        at = pl.ds(part * TALL, TALL)
        return pltpu.make_async_copy(turned_back.at[at], bgt.at[at], went.at[part])

    fetch = pltpu.make_async_copy(background, back_held, back_came)
    bring(0).start()
    fetch.start()
    for part in range(1, tall):
        bring(part).start()
    fetch.wait()

    def turn(part, carry):
        first = pl.multiple_of(part * TALL, TALL)
        wide[...] = back_held[:, pl.ds(first, TALL), :].astype(F32).reshape(LEV * TALL, BY)
        bring(part).wait()
        flat = held.at[part].reshape(LEV * TALL, BY)
        for i in range(TALL):
            here = pl.ds(i, LEV, stride=TALL)
            turned = jnp.transpose(flat[here, :])
            field[first + i + 2, 8 : 8 + BY, :] = turned
            turned_back[first + i] = jnp.transpose(wide[here, :]).astype(BF16)
            for n, y in enumerate((0, 1, BY - 2, BY - 1)):
                planes[n, pl.ds(first + i, 1), :] = turned[y : y + 1, :LEV]
        leave(part).start()
        return carry

    lax.fori_loop(0, tall, turn, 0)
    x_down[:BY, :] = field[2, 8 : 8 + BY, :].astype(BF16)
    x_down[BY : 2 * BY, :] = field[3, 8 : 8 + BY, :].astype(BF16)
    x_up[:BY, :] = field[BX, 8 : 8 + BY, :].astype(BF16)
    x_up[BY : 2 * BY, :] = field[BX + 1, 8 : 8 + BY, :].astype(BF16)
    s = spread[...]
    turned = jnp.transpose(jnp.concatenate([s, s], axis=0))

    def rows(two):
        high, low = split_two(two)
        zero = jnp.zeros((12, BY), F32)
        return jnp.concatenate([high.astype(F32), low.astype(F32), zero], axis=0).astype(BF16)

    x_down[2 * BY :, :] = rows(s[0:2, :])
    x_up[2 * BY :, :] = rows(s[BX - 2 : BX, :])
    y_down[: 2 * BX, :] = planes[0:2].reshape(2 * BX, LEV).astype(BF16)
    y_up[: 2 * BX, :] = planes[2:4].reshape(2 * BX, LEV).astype(BF16)
    y_down[2 * BX :, :] = rows(turned[0:2, :])
    y_up[2 * BX :, :] = rows(turned[BY - 2 : BY, :])
    for part in range(tall):
        leave(part).wait()


def to_columns(control, background, spread):
    hbm = pl.BlockSpec(memory_space=pltpu.HBM)
    whole = pl.BlockSpec(memory_space=pltpu.VMEM)
    return pl.pallas_call(
        columns_kernel,
        in_specs=[hbm, hbm, whole],
        out_specs=[whole, hbm] + [whole] * 4,
        out_shape=[
            pltpu.VMEM((PX, PY, LEV), F32),
            pltpu.HBM((BX, BY, LEV), BF16),
            jax.ShapeDtypeStruct((2 * BY + 16, LEV), BF16),
            jax.ShapeDtypeStruct((2 * BY + 16, LEV), BF16),
            jax.ShapeDtypeStruct((2 * BX + 16, LEV), BF16),
            jax.ShapeDtypeStruct((2 * BX + 16, LEV), BF16),
        ],
        scratch_shapes=[
            pltpu.VMEM((BX // TALL, LEV, TALL, BY), F32),
            pltpu.VMEM((LEV, BX, BY), BF16),
            pltpu.VMEM((LEV * TALL, BY), F32),
            pltpu.VMEM((BX, BY, LEV), BF16),
            pltpu.VMEM((4, BX, LEV), F32),
            pltpu.SemaphoreType.DMA((BX // TALL,)),
            pltpu.SemaphoreType.DMA,
            pltpu.SemaphoreType.DMA((BX // TALL,)),
        ],
        compiler_params=params(16),
        cost_estimate=cost(6),
        name="columns",
    )(in_hbm(control), in_hbm(background), spread)


def shift(array, axis, by):
    count = lax.axis_size(axis)
    return lax.ppermute(array, axis, [(i, (i + by) % count) for i in range(count)])


def compose_kernel(count, first_up, first_down, low, high, up, down):
    rows = first_up.shape[0]
    up[:rows, :] = first_up[...]
    down[:rows, :] = first_down[...]
    low = low[...].astype(F32)
    high = high[...].astype(F32)
    fields = [low[2 * count :], high[2 * count :]] if low.shape[0] > 2 * count else []
    for out, row in ((up, count - 1), (down, 0)):
        pair = [low[count + row : count + row + 1], high[row : row + 1], jnp.zeros((14, LEV), F32)]
        out[rows:, :] = jnp.concatenate(pair + fields, axis=0).astype(BF16)


def compose(count, first_up, first_down, low, high):
    rows = first_up.shape[0] + 16 + 2 * (low.shape[0] - 2 * count)
    return pl.pallas_call(
        functools.partial(compose_kernel, count),
        out_shape=[jax.ShapeDtypeStruct((rows, LEV), BF16)] * 2,
        compiler_params=params(2),
        name="compose",
    )(first_up, first_down, low, high)


def laplace(field, x, first, count):
    total = field[x + 1, pl.ds(first, count), :] + field[x - 1, pl.ds(first, count), :]
    total = total + field[x, pl.ds(first + 1, count), :]
    total = total + field[x, pl.ds(first - 1, count), :]
    return total - 4.0 * field[x, pl.ds(first, count), :]


def plane(field, x, y, count):
    flat = field.reshape(PX * PY, LEV)
    return flat[pl.ds(x * PY + y, count, stride=PY), :]


def set_plane(field, x, y, count, value):
    flat = field.reshape(PX * PY, LEV)
    flat[pl.ds(x * PY + y, count, stride=PY), :] = value


def plane_laplace(field, y):
    total = plane(field, 3, y, BX) + plane(field, 1, y, BX)
    total = total + plane(field, 2, y + 1, BX) + plane(field, 2, y - 1, BX)
    return total - 4.0 * plane(field, 2, y, BX)


def lanes(column):
    return jnp.broadcast_to(column, (column.shape[0], LEV))


def joined(rows, at):
    block = rows[at : at + 16, :].astype(F32)
    return block[0:2] + block[2:4]


def fill_y(field, y_low, y_high):
    for n in range(2):
        set_plane(field, 2, 6 + n, BX, y_low[n * BX : (n + 1) * BX, :].astype(F32))
        set_plane(field, 2, 8 + BY + n, BX, y_high[n * BX : (n + 1) * BX, :].astype(F32))


def fill_x(field, x_low, x_high):
    for n in range(2):
        field[n, 8 : 8 + BY, :] = x_low[n * BY : (n + 1) * BY, :].astype(F32)
        field[BX + 2 + n, 8 : 8 + BY, :] = x_high[n * BY : (n + 1) * BY, :].astype(F32)


def fill_corners(field, y_low, y_high):
    for rows, y in ((y_low, 7), (y_high, 8 + BY)):
        pair = rows[2 * BX + 16 : 2 * BX + 32, :].astype(F32)
        field[1, y : y + 1, :] = pair[0:1]
        field[BX + 2, y : y + 1, :] = pair[1:2]


def main_coefficients(coef, spread):
    square = jnp.concatenate([spread[...], jnp.zeros((BY - BX, BY), F32)], axis=0)
    turned = jnp.transpose(square)
    for x in range(BX):
        coef[x + 2, 8 : 8 + BY, :] = lanes(turned[:, x : x + 1])


def rim_coefficients(coef, x_low, x_high, y_low, y_high):
    ends = jnp.concatenate(
        [joined(x_low, 2 * BY), joined(x_high, 2 * BY), jnp.zeros((BY - 4, BY), F32)], axis=0
    )
    ends = jnp.transpose(ends)
    for n, x in enumerate((0, 1, BX + 2, BX + 3)):
        coef[x, 8 : 8 + BY, :] = lanes(ends[:, n : n + 1])
    sides = jnp.concatenate(
        [joined(y_low, 2 * BX), joined(y_high, 2 * BX), jnp.zeros((BY - 4, BY), F32)], axis=0
    )
    sides = jnp.transpose(sides)[:BX, :]
    for n in range(2):
        set_plane(coef, 2, 6 + n, BX, lanes(sides[:, n : n + 1]))
        set_plane(coef, 2, 8 + BY + n, BX, lanes(sides[:, 2 + n : 3 + n]))
    for block, y, lane in ((y_low, 7, BY - 1), (y_high, 8 + BY, 0)):
        left = joined(block, 2 * BX + 32)
        right = joined(block, 2 * BX + 48)
        coef[1, y : y + 1, :] = lanes(left[1:2, lane : lane + 1])
        coef[BX + 2, y : y + 1, :] = lanes(right[0:1, lane : lane + 1])


def sweep(to, field, coef, x):
    middle = field[x, 8 : 8 + BY, :]
    to[x, 8 : 8 + BY, :] = middle + coef[x, 8 : 8 + BY, :] * laplace(field, x, 8, BY)


def early_kernel(spread, field, coef, first):
    main_coefficients(coef, spread)

    def one(x, carry):
        sweep(first, field, coef, x)
        return carry

    lax.fori_loop(3, PX - 3, one, 0)


def early(spread, field):
    return pl.pallas_call(
        early_kernel,
        out_shape=[pltpu.VMEM((PX, PY, LEV), F32), pltpu.VMEM((PX, PY, LEV), F32)],
        compiler_params=params(2),
        cost_estimate=cost(2),
        name="early",
    )(spread, in_vmem(field))


def joined(rows, at):
    block = rows[at : at + 16, :].astype(F32)
    return block[0:2] + block[2:4]


PARTS = BX // CHUNK


def increment_kernel(
    _field, _coef, _first, x_low, x_high, y_low, y_high,
    inc, kept, field, coef, first, done, went, kept_went,
):
    def leave(part):
        at = pl.ds(part * CHUNK, CHUNK)
        return pltpu.make_async_copy(done.at[at], inc.at[at], went.at[part])

    rim_coefficients(coef, x_low, x_high, y_low, y_high)
    keep = pltpu.make_async_copy(coef, kept, kept_went)
    keep.start()
    fill_x(field, x_low, x_high)
    fill_corners(field, y_low, y_high)
    fill_y(field, y_low, y_high)

    for x in (1, 2, BX + 1, BX + 2):
        sweep(first, field, coef, x)
    for y in (7, 8, 7 + BY, 8 + BY):
        moved = plane(field, 2, y, BX) + plane(coef, 2, y, BX) * plane_laplace(field, y)
        set_plane(first, 2, y, BX, moved)

    def sweep_two(x, carry):
        middle = first[x, 8 : 8 + BY, :]
        result = middle + coef[x, 8 : 8 + BY, :] * laplace(first, x, 8, BY)
        done[x - 2] = result.astype(BF16)
        return carry

    for part in range(PARTS):
        lax.fori_loop(2 + CHUNK * part, 2 + CHUNK * (part + 1), sweep_two, 0)
        leave(part).start()
    for part in range(PARTS):
        leave(part).wait()
    keep.wait()


def increments(field, coef, first, rims):
    whole = pl.BlockSpec(memory_space=pltpu.VMEM)
    padded = pltpu.VMEM((PX, PY, LEV), F32)
    return pl.pallas_call(
        increment_kernel,
        in_specs=[whole] * 7,
        out_specs=[pl.BlockSpec(memory_space=pltpu.HBM)] * 2 + [whole] * 3,
        out_shape=[
            pltpu.HBM((BX, BY, LEV), BF16),
            pltpu.HBM((PX, PY, LEV), F32),
            padded,
            padded,
            padded,
        ],
        input_output_aliases={0: 2, 1: 3, 2: 4},
        scratch_shapes=[
            pltpu.VMEM((BX, BY, LEV), BF16),
            pltpu.SemaphoreType.DMA((PARTS,)),
            pltpu.SemaphoreType.DMA,
        ],
        compiler_params=params(8),
        cost_estimate=cost(6),
        name="increment",
    )(in_vmem(field), in_vmem(coef), in_vmem(first), *rims)[:2]


def decode(rows):
    back = lambda n: pltpu.roll(rows, LEV - n, 1)
    frac_x = back(2) + back(3) + back(4)
    frac_y = back(5) + back(6) + back(7)
    valid = rows > 0.5
    cell = jnp.where(valid, ((rows - 1.0) * BY + back(1)).astype(jnp.int32), 2 * iota(rows.shape, 0))
    off = lambda w: jnp.where(valid, w, 0.0)
    return cell, (
        off((1.0 - frac_x) * (1.0 - frac_y)),
        off(frac_x * (1.0 - frac_y)),
        off((1.0 - frac_x) * frac_y),
        off(frac_x * frac_y),
    )


def to_table(cell, cells, table, arrived):
    across = jnp.transpose(cell)
    for k in range(CAP):
        cells[k : k + 1, :] = across[8 * k : 8 * k + 1, :]
    copy = pltpu.make_async_copy(cells, table, arrived)
    copy.start()
    return copy


def gather_kernel(
    got, background, increment, reply, slots,
    wide, cells, table, ga, gb, spaced, both, packed, came, arrived,
):
    part = CELLS // PARTS

    def bring(n, i):
        at = pl.ds(i * part, part)
        source = (background, increment)[n]
        return pltpu.make_async_copy(source.at[at], packed.at[n, at], came.at[n, i])

    for i in range(PARTS):
        bring(0, i).start()
        bring(1, i).start()
    wide[...] = got[...].astype(F32).reshape(DEV * ROWS, LEV)
    cell, weights = decode(wide[pl.ds(CAP, DEV, stride=ROWS), :])
    placed = to_table(cell, cells, table, arrived)
    for i in range(PARTS):
        for n in range(2):
            bring(n, i).wait()

            def widen(j, carry):
                first = pl.multiple_of(i * part + j * BY, BY)
                both[pl.ds(2 * first + n, BY, stride=2), :] = packed[n, pl.ds(first, BY), :].astype(F32)
                return carry

            lax.fori_loop(0, part // BY, widen, 0)
    placed.wait()
    for k in range(CAP):

        def fetch(step, carry):
            for n in range(16):
                owner = step * 16 + n
                at = table[k, owner]
                to = pl.ds(4 * (k * DEV + owner), 4)
                ga[to, :] = both[pl.ds(2 * at, 4), :]
                gb[to, :] = both[pl.ds(2 * (at + BY), 4), :]
            return carry

        lax.fori_loop(0, DEV // 16, fetch, 0)
    spaced[...] = jnp.zeros_like(spaced)
    for k in range(CAP):
        w = [lanes(weight[:, 8 * k : 8 * k + 1]) for weight in weights]
        for n in range(2):
            here = pl.ds(4 * DEV * k + n, DEV, stride=4)
            next_to = pl.ds(4 * DEV * k + 2 + n, DEV, stride=4)
            mixed = w[0] * ga[here, :] + w[1] * gb[here, :]
            mixed = mixed + w[2] * ga[next_to, :]
            mixed = mixed + w[3] * gb[next_to, :]
            slots[k * DEV : (k + 1) * DEV, n * LEV : (n + 1) * LEV] = mixed.astype(BF16)
            spaced[n, pl.ds(k, DEV, stride=ROWS), :] = mixed
    reply[:, :LEV] = spaced[0].astype(BF16)
    reply[:, LEV:] = spaced[1].astype(BF16)


def gathered(got, bgt, inct):
    rows = pltpu.VMEM((4 * SLOTS, LEV), F32)
    whole = pl.BlockSpec(memory_space=pltpu.VMEM)
    return pl.pallas_call(
        gather_kernel,
        grid=(1,),
        in_specs=[pl.BlockSpec((DEV, ROWS, LEV), lambda i: (0, 0, 0))]
        + [pl.BlockSpec(memory_space=pltpu.HBM)] * 2,
        out_specs=[whole, whole],
        out_shape=[
            jax.ShapeDtypeStruct((DEV * ROWS, 2 * LEV), BF16),
            jax.ShapeDtypeStruct((SLOTS, 2 * LEV), BF16),
        ],
        scratch_shapes=[
            pltpu.VMEM((DEV * ROWS, LEV), F32),
            pltpu.VMEM((8, LEV), jnp.int32),
            pltpu.SMEM((8, LEV), jnp.int32),
            rows,
            rows,
            pltpu.VMEM((2, DEV * ROWS, LEV), F32),
            pltpu.VMEM((2 * CELLS, LEV), F32),
            pltpu.VMEM((2, CELLS, LEV), BF16),
            pltpu.SemaphoreType.DMA((2, PARTS)),
            pltpu.SemaphoreType.DMA,
        ],
        compiler_params=params(26),
        cost_estimate=cost(5),
        name="gather",
    )(got, in_hbm(bgt), in_hbm(inct))


def tangent(base, delta, w_first, b_first, w_second, b_second):
    h_one = jnp.tanh(nn(base, w_first) + b_first)
    d_one = 1.0 - h_one * h_one
    h_two = jnp.tanh(nn(h_one.astype(BF16), w_second) + b_second)
    d_two = 1.0 - h_two * h_two
    t_one = (d_one * nn(delta, w_first)).astype(BF16)
    t_two = (d_two * nn(t_one, w_second)).astype(BF16)
    return d_one, d_two, t_two


BLOCK = 768


def adjoint_kernel(
    got, slots, w_first, b_first, w_second, b_second, w_third, ivar, kept, control,
    acc, x_up, x_down, y_up, y_down, coef, held, low, high,
    wide, pulled, profile, cells, table, ca, cb, came, arrived,
):
    copies = [pltpu.make_async_copy(kept, coef, came.at[3])] + [
        pltpu.make_async_copy(control.at[:, pl.ds(at, to.shape[1])], to, came.at[n])
        for n, (to, at) in enumerate(((held, CHUNK), (low, 0), (high, BX - CHUNK)))
    ]
    for copy in copies:
        copy.start()
    for n in range(HID // LEV):
        at = slice(n * LEV, (n + 1) * LEV)
        wide[...] = got[:, :, at].astype(F32).reshape(DEV * ROWS, LEV)
        for k in range(CAP):
            pulled[k * DEV : (k + 1) * DEV, at] = wide[pl.ds(k, DEV, stride=ROWS), :]
        if n == 0:
            cell, weights = decode(wide[pl.ds(CAP, DEV, stride=ROWS), :])
    placed = to_table(cell, cells, table, arrived)

    def block(i, carry):
        here = pl.ds(pl.multiple_of(i * BLOCK, BLOCK), BLOCK)
        d_one, d_two, t_two = tangent(
            slots[here, :LEV], slots[here, LEV:],
            w_first[...], b_first[...], w_second[...], b_second[...],
        )
        change = nt(t_two, w_third[...]) * ivar[...].reshape(1, CH)
        s_two = (d_two * (nn(change.astype(BF16), w_third[...]) - pulled[here, :])).astype(BF16)
        s_one = (d_one * nt(s_two, w_second[...])).astype(BF16)
        profile[here, :] = nt(s_one, w_first[...])
        return carry

    lax.fori_loop(0, SLOTS // BLOCK, block, 0)
    acc[...] = jnp.zeros_like(acc)
    for k in range(CAP):
        grad = profile[k * DEV : (k + 1) * DEV, :]
        w = [lanes(weight[:, 8 * k : 8 * k + 1]) for weight in weights]
        even = pl.ds(2 * DEV * k, DEV, stride=2)
        odd = pl.ds(2 * DEV * k + 1, DEV, stride=2)
        ca[even, :] = w[0] * grad
        cb[even, :] = w[1] * grad
        ca[odd, :] = w[2] * grad
        cb[odd, :] = w[3] * grad
    placed.wait()
    for k in range(CAP):

        def add(step, carry):
            for n in range(16):
                owner = step * 16 + n
                at = table[k, owner]
                there = pl.ds(2 * (k * DEV + owner), 2)
                one = acc[pl.ds(at, 2), :] + ca[there, :]
                two = acc[pl.ds(at + BY, 2), :] + cb[there, :]
                acc[pl.ds(at, 2), :] = one
                acc[pl.ds(at + BY, 2), :] = two
            return carry

        lax.fori_loop(0, DEV // 16, add, 0)
    x_down[...] = acc[: 2 * BY, :].astype(BF16)
    x_up[...] = acc[CELLS - 2 * BY :, :].astype(BF16)
    for n in range(2):
        y_down[n * BX : (n + 1) * BX, :] = acc[pl.ds(n, BX, stride=BY), :].astype(BF16)
        y_up[n * BX : (n + 1) * BX, :] = acc[pl.ds(BY - 2 + n, BX, stride=BY), :].astype(BF16)
    for copy in copies:
        copy.wait()


INNER = BX - 2 * CHUNK


def adjoint(got, slots, w_first, b_first, w_second, b_second, w_third, ivar, kept, control):
    whole = pl.BlockSpec(memory_space=pltpu.VMEM)
    return pl.pallas_call(
        adjoint_kernel,
        in_specs=[whole] * 8 + [pl.BlockSpec(memory_space=pltpu.HBM)] * 2,
        out_specs=[whole] * 9,
        out_shape=[
            pltpu.VMEM((CELLS, LEV), F32),
            jax.ShapeDtypeStruct((2 * BY, LEV), BF16),
            jax.ShapeDtypeStruct((2 * BY, LEV), BF16),
            jax.ShapeDtypeStruct((2 * BX, LEV), BF16),
            jax.ShapeDtypeStruct((2 * BX, LEV), BF16),
            pltpu.VMEM((PX, PY, LEV), F32),
            pltpu.VMEM((LEV, INNER, BY), F32),
            pltpu.VMEM((LEV, CHUNK, BY), F32),
            pltpu.VMEM((LEV, CHUNK, BY), F32),
        ],
        scratch_shapes=[
            pltpu.VMEM((DEV * ROWS, LEV), F32),
            pltpu.VMEM((SLOTS, HID), F32),
            pltpu.VMEM((SLOTS, LEV), F32),
            pltpu.VMEM((8, LEV), jnp.int32),
            pltpu.SMEM((8, LEV), jnp.int32),
            pltpu.VMEM((2 * SLOTS, LEV), F32),
            pltpu.VMEM((2 * SLOTS, LEV), F32),
            pltpu.SemaphoreType.DMA((4,)),
            pltpu.SemaphoreType.DMA,
        ],
        compiler_params=params(32),
        cost_estimate=cost(10),
        name="adjoint",
    )(
        got, slots, w_first, b_first, w_second, b_second, w_third, ivar,
        in_hbm(kept), in_hbm(control),
    )


def departure_kernel(
    reply, holder, innov, w_first, b_first, w_second, b_second, w_third, ivar, out
):
    held = holder[...]
    pick = (iota((OWN, DEV * ROWS), 1) == down(held * ROWS + ranks(held)).astype(jnp.int32)[:, 0:1]).astype(BF16)
    own = nn(pick, reply[...]).astype(BF16)
    _, _, t_two = tangent(
        own[:, :LEV], own[:, LEV:], w_first[...], b_first[...], w_second[...], b_second[...]
    )
    each = down(ivar[...].reshape(1, CH))
    out[...] = (nt(w_third[...], t_two) - innov[...]) * jnp.concatenate([each, each], axis=1)


def departures_of(reply, holder, innov, w_first, b_first, w_second, b_second, w_third, ivar):
    return pl.pallas_call(
        departure_kernel,
        out_shape=jax.ShapeDtypeStruct((CH, OWN), F32),
        compiler_params=params(12),
        cost_estimate=cost(4),
        name="departures",
    )(reply, holder, innov, w_first, b_first, w_second, b_second, w_third, ivar)


def ready_kernel(acc, coef, grown, scaled, field):
    for x in (1, BX + 2):
        field[x] = jnp.zeros((PY, LEV), F32)
    for y in (7, 8 + BY):
        set_plane(field, 2, y, BX, jnp.zeros((BX, LEV), F32))

    def scale(x, carry):
        at = pl.ds(pl.multiple_of((x - 2) * BY, BY), BY)
        field[x, 8 : 8 + BY, :] = coef[x, 8 : 8 + BY, :] * acc[at, :]
        return carry

    lax.fori_loop(2, PX - 2, scale, 0)

    def sweep_one(x, carry):
        at = pl.ds(pl.multiple_of((x - 2) * BY, BY), BY)
        value = acc[at, :] + laplace(field, x, 8, BY)
        grown[x - 2] = value
        scaled[x, 8 : 8 + BY, :] = coef[x, 8 : 8 + BY, :] * value
        return carry

    lax.fori_loop(2, PX - 2, sweep_one, 0)


def ready(acc, coef):
    return pl.pallas_call(
        ready_kernel,
        out_shape=[pltpu.VMEM((BX, BY, LEV), F32), pltpu.VMEM((PX, PY, LEV), F32)],
        scratch_shapes=[pltpu.VMEM((PX, PY, LEV), F32)],
        compiler_params=params(8),
        cost_estimate=cost(3),
        name="ready",
    )(in_vmem(acc), in_vmem(coef))


def finish_rows(grown, scaled, held, first, count):
    flat = held.reshape(LEV * held.shape[1], BY)
    for i in range(count):
        x = first + i
        value = grown[x] + laplace(scaled, x + 2, 8, BY)
        here = pl.ds(i, LEV, stride=held.shape[1])
        flat[here, :] = jnp.transpose(value) + flat[here, :]


def interior_kernel(
    acc, coef, y_low, y_high, _held, _grown, _scaled, out, held, grown, scaled, went
):
    edge = iota((BX, LEV), 0)
    for rows, near, far, side, inner in (
        (y_low, 1, 0, 7, 8),
        (y_high, 0, 1, 8 + BY, 7 + BY),
    ):
        here = rows[near * BX : (near + 1) * BX, :].astype(F32)
        there = rows[far * BX : (far + 1) * BX, :].astype(F32)
        weight = plane(coef, 2, side, BX)
        mine = weight * here
        over = side + (-1 if side < 8 else 1)
        total = jnp.where(edge == BX - 1, 0.0, pltpu.roll(mine, BX - 1, 0))
        total = total + jnp.where(edge == 0, 0.0, pltpu.roll(mine, 1, 0))
        touching = acc[pl.ds(inner - 8, BX, stride=BY), :]
        inside = plane(coef, 2, inner, BX)
        total = total + inside * touching + plane(coef, 2, over, BX) * there
        set_plane(scaled, 2, side, BX, weight * (here + (total - 4.0 * mine)))
        flat = grown.reshape(CELLS, LEV)
        at = pl.ds(inner - 8, BX, stride=BY)
        fixed = flat[at, :] + mine
        flat[at, :] = fixed
        set_plane(scaled, 2, inner, BX, inside * fixed)

    def leave(part):
        return pltpu.make_async_copy(
            held.at[:, pl.ds(part * TALL, TALL)],
            out.at[:, pl.ds(CHUNK + part * TALL, TALL)],
            went.at[part],
        )

    for part in range(INNER // TALL):
        first = part * TALL

        def some(step, carry):
            flat = held.reshape(LEV * INNER, BY)
            for i in range(4):
                at = first + step * 4 + i
                value = grown[CHUNK + at] + laplace(scaled, CHUNK + at + 2, 8, BY)
                here = pl.ds(at, LEV, stride=INNER)
                flat[here, :] = jnp.transpose(value) + flat[here, :]
            return carry

        lax.fori_loop(0, TALL // 4, some, 0)
        leave(part).start()
    for part in range(INNER // TALL):
        leave(part).wait()


def interior(acc, coef, rims, held, grown, scaled):
    whole = pl.BlockSpec(memory_space=pltpu.VMEM)
    hbm = pl.BlockSpec(memory_space=pltpu.HBM)
    return pl.pallas_call(
        interior_kernel,
        in_specs=[whole] * 7,
        out_specs=[hbm] + [whole] * 3,
        out_shape=[
            pltpu.HBM((LEV, BX, BY), F32),
            pltpu.VMEM((LEV, INNER, BY), F32),
            pltpu.VMEM((BX, BY, LEV), F32),
            pltpu.VMEM((PX, PY, LEV), F32),
        ],
        input_output_aliases={4: 1, 5: 2, 6: 3},
        scratch_shapes=[pltpu.SemaphoreType.DMA((INNER // TALL,))],
        compiler_params=params(4),
        cost_estimate=cost(5),
        name="interior",
    )(in_vmem(acc), in_vmem(coef), *rims, in_vmem(held), in_vmem(grown), in_vmem(scaled))


def edges_kernel(
    acc, coef, x_low, x_high, _out, _grown, _scaled, _low, _high,
    out, grown, scaled, low, high, line, went,
):
    held = (low, high)

    def leave(n):
        at = pl.ds(n * (BX - CHUNK), CHUNK)
        return pltpu.make_async_copy(held[n], out.at[:, at], went.at[n])

    main = pl.ds(8, BY)
    for rows, near, side, inner in ((x_low, 1, 1, 2), (x_high, 0, BX + 2, BX + 1)):
        here = rows[near * BY : (near + 1) * BY, :].astype(F32)
        there = rows[(1 - near) * BY : (2 - near) * BY, :].astype(F32)
        pair = rows[2 * BY : 2 * BY + 16, :].astype(F32)
        weight = coef[side, main, :]
        mine = weight * here
        line[main, :] = mine
        for n, y in enumerate((7, 8 + BY)):
            corner = coef[side, y : y + 1, :] * pair[n : n + 1]
            line[y : y + 1, :] = corner
            scaled[inner, y : y + 1, :] = (
                scaled[inner, y : y + 1, :] + coef[inner, y : y + 1, :] * corner
            )
        inside = coef[inner, main, :]
        total = inside * acc[(inner - 2) * BY : (inner - 1) * BY, :]
        total = total + coef[side + (-1 if side < 8 else 1), main, :] * there
        total = total + line[9 : 9 + BY, :] + line[7 : 7 + BY, :]
        scaled[side, main, :] = weight * (here + (total - 4.0 * mine))
        fixed = grown[inner - 2] + mine
        grown[inner - 2] = fixed
        scaled[inner, main, :] = inside * fixed
    for n in range(2):
        finish_rows(grown, scaled, held[n], n * (BX - CHUNK), CHUNK)
        leave(n).start()
    for n in range(2):
        leave(n).wait()


def edges(acc, coef, rims, so_far, grown, scaled, low, high):
    whole = pl.BlockSpec(memory_space=pltpu.VMEM)
    hbm = pl.BlockSpec(memory_space=pltpu.HBM)
    return pl.pallas_call(
        edges_kernel,
        in_specs=[whole] * 4 + [hbm] + [whole] * 4,
        out_specs=[hbm] + [whole] * 4,
        out_shape=[
            pltpu.HBM((LEV, BX, BY), F32),
            pltpu.VMEM((BX, BY, LEV), F32),
            pltpu.VMEM((PX, PY, LEV), F32),
            pltpu.VMEM((LEV, CHUNK, BY), F32),
            pltpu.VMEM((LEV, CHUNK, BY), F32),
        ],
        input_output_aliases={4: 0, 5: 1, 6: 2, 7: 3, 8: 4},
        scratch_shapes=[pltpu.VMEM((PY, LEV), F32), pltpu.SemaphoreType.DMA((2,))],
        compiler_params=params(4),
        cost_estimate=cost(2),
        name="edges",
    )(
        in_vmem(acc), in_vmem(coef), *rims, in_hbm(so_far),
        in_vmem(grown), in_vmem(scaled), in_vmem(low), in_vmem(high),
    )[0]


def exchange(array):
    return lax.all_to_all(array, ("tile", "obs"), split_axis=0, concat_axis=0, tiled=True)


def per_device(
    control,
    background,
    spread,
    obs_holder,
    obs_anchor,
    obs_frac,
    innovation,
    inverse_var,
    w_first,
    b_first,
    w_second,
    b_second,
    w_third,
):
    b_one = b_first.reshape(1, HID)
    b_two = b_second.reshape(1, HID)
    holder = obs_holder.reshape(1, OWN)
    innov = innovation.T
    w_last = w_third.T
    asked = requests(holder, obs_anchor.reshape(1, OWN), obs_frac, innov, inverse_var, w_last)
    got = exchange(asked.reshape(DEV, ROWS, HID))
    field, bgt, x_up, x_down, y_up, y_down = to_columns(control, background, spread)
    ax_low, ax_high = shift(x_up, "tile", 1), shift(x_down, "tile", -1)
    wide, first = early(spread, field)
    y_up, y_down = compose(BY, y_up, y_down, ax_low, ax_high)
    ay_low, ay_high = shift(y_up, "obs", 1), shift(y_down, "obs", -1)
    before = (ax_low, ax_high, ay_low, ay_high)
    inct, kept = increments(field, wide, first, before)
    reply, slots = gathered(got, bgt.reshape(CELLS, LEV), inct.reshape(CELLS, LEV))
    reply = exchange(reply.reshape(DEV, ROWS, 2 * LEV))
    acc, x_up, x_down, y_up, y_down, coef, *held = adjoint(
        got, slots, w_first, b_one, w_second, b_two, w_last, inverse_var, kept, control
    )
    y_low, y_high = shift(y_up, "obs", 1), shift(y_down, "obs", -1)
    grown, scaled = ready(acc, coef)
    x_up, x_down = compose(BX, x_up, x_down, y_low, y_high)
    x_low, x_high = shift(x_up, "tile", 1), shift(x_down, "tile", -1)
    gradient, _, grown, scaled = interior(acc, coef, (y_low, y_high), held[0], grown, scaled)
    gradient = edges(
        acc, coef, (x_low, x_high), gradient, grown, scaled, held[1], held[2]
    )
    departures = departures_of(
        reply.reshape(DEV * ROWS, 2 * LEV), holder, innov,
        w_first, b_one, w_second, b_two, w_last, inverse_var,
    ).T
    return departures, gradient


def solution(mesh):
    return jax.shard_map(
        per_device,
        mesh=mesh,
        in_specs=(
            P(None, "tile", "obs"),
            P(None, "tile", "obs"),
            P("tile", "obs"),
            P(("tile", "obs"), None),
            P(("tile", "obs")),
            P(None, ("tile", "obs")),
            P(("tile", "obs"), None),
            P(),
            P(),
            P(),
            P(),
            P(),
            P(),
        ),
        out_specs=(P(("tile", "obs"), None), P(None, "tile", "obs")),
        check_vma=False,
    )
```
